32 devices in a mesh: dp: 16 (over z, y, core), tensor: 2 (over x).
Axes of the slice: x: 2, y: 2, z: 4, core: 2. Of those that a mesh axis runs over, the one named last changes fastest.
Arguments:
- characters: bfloat16 [16, 1536, 768], P('dp'), may hold values from -8 to 8
- first_gain: bfloat16 [768], replicated, may hold values from 0.5 to 1.5
- first_shift: bfloat16 [768], replicated, may hold values from -1.75 to 1.75
- query_weight: bfloat16 [768, 768], P(None, 'tensor'), may hold values from -0.3125 to 0.3125
- query_bias: bfloat16 [768], P('tensor'), may hold values from -3 to 3
- key_weight: bfloat16 [768, 768], P(None, 'tensor'), may hold values from -0.3125 to 0.3125
- value_weight: bfloat16 [768, 768], P(None, 'tensor'), may hold values from -0.21875 to 0.21875
- value_bias: bfloat16 [768], P('tensor'), may hold values from -1.25 to 1.25
- out_weight: bfloat16 [768, 768], P('tensor'), may hold values from -0.625 to 0.625
- out_bias: bfloat16 [768], replicated, may hold values from -1.75 to 1.75
- second_gain: bfloat16 [768], replicated, may hold values from 0.5 to 1.5
- second_shift: bfloat16 [768], replicated, may hold values from -1.75 to 1.75
- up_weight: bfloat16 [768, 3072], P(None, 'tensor'), may hold values from -0.21875 to 0.21875
- up_bias: bfloat16 [3072], P('tensor'), may hold values from -3 to 3
- down_weight: bfloat16 [3072, 768], P('tensor'), may hold values from -0.109375 to 0.109375
- down_bias: bfloat16 [768], replicated, may hold values from -1.75 to 1.75
- conv_weight: bfloat16 [3072, 768], P(None, 'tensor'), may hold values from -0.109375 to 0.109375
- conv_bias: bfloat16 [768], P('tensor'), may hold values from -3 to 3
- third_gain: bfloat16 [768], P('tensor'), may hold values from 0.099609375 to 1.8984375
- third_shift: bfloat16 [768], P('tensor'), may hold values from -1.75 to 1.75
- cotangent: bfloat16 [16, 384, 768], P('dp'), may hold values from -8 to 8
Outputs:
- molecules: bfloat16 [16, 384, 768], P('dp', None, 'tensor')
- input_grad: float32 [16, 1536, 768], P('dp', 'tensor')
- grad_first_gain: float32 [768], P('dp')
- grad_first_shift: float32 [768], P('dp')
- grad_query_weight: float32 [768, 768], P('dp', 'tensor')
- grad_query_bias: float32 [768], P('tensor')
- grad_key_weight: float32 [768, 768], P('dp', 'tensor')
- grad_value_weight: float32 [768, 768], P('dp', 'tensor')
- grad_value_bias: float32 [768], P('tensor')
- grad_out_weight: float32 [768, 768], P('tensor', 'dp')
- grad_out_bias: float32 [768], P('dp')
- grad_second_gain: float32 [768], P('dp')
- grad_second_shift: float32 [768], P('dp')
- grad_up_weight: float32 [768, 3072], P('dp', 'tensor')
- grad_up_bias: float32 [3072], P('tensor')
- grad_down_weight: float32 [3072, 768], P('tensor', 'dp')
- grad_down_bias: float32 [768], P('dp')
- grad_conv_weight: float32 [3072, 768], P('dp', 'tensor')
- grad_conv_bias: float32 [768], P('tensor')
- grad_third_gain: float32 [768], P('tensor')
- grad_third_shift: float32 [768], P('tensor')
The draws below stay inside these ranges and needn't reach their ends.
All inputs are finite; a program needn't handle non-finite values.
Results may differ from the reference program's by a relative error of at most 0.028.
Values may be sent and summed in bfloat16 or wider, within the bound.
No kernel may reach another device: no remote copies, remote signals or barrier semaphores. Data moves between devices by JAX's collectives and lax.ppermute only.
A program may use at most 192 MiB of HBM per device.

```python
import jax
import jax.numpy as jnp
from jax import lax

D = 768
HEAD_DIM = 64
FF = 3072
BLOCK = 128
STRIDE = 4
SEQ_LEN = 1536
ROWS = 16
MOLS = 384
GROUPS = 2


def draw_cotangent(key, part):
    noise_key, size_key, sign_key = jax.random.split(key, 3)
    noise_part = jnp.clip(jax.random.normal(noise_key, (ROWS, MOLS, D), jnp.float32), -6.0, 6.0)
    magnitude = jax.random.uniform(size_key, (ROWS, MOLS, 1), jnp.float32, 0.5, 1.5)
    sign_part = (2 * jax.random.randint(sign_key, (ROWS, MOLS, 1), 0, 2) - 1).astype(jnp.float32)
    return (noise_part + magnitude * sign_part).astype(jnp.bfloat16)


def strengthened(drawn, key, source, target, shards_of, factor):
    def block_of(dim):
        return (jnp.arange(drawn.shape[dim]) // (drawn.shape[dim] // shards_of)).reshape((-1,) + (1,) * (drawn.ndim - 1 - dim))

    first = jax.random.permutation(key, shards_of)[block_of(target)]
    second = (block_of(target) + shards_of // 2) % shards_of
    return jnp.where((block_of(source) == first) | (block_of(source) == second), factor * drawn, drawn)


def level_of(rng, shape, cuts, low, high):
    def one(position, blocks):
        steps = jax.random.uniform(jax.random.fold_in(jax.random.fold_in(rng, 6), position), (blocks,), jnp.float32, low / len(cuts), high / len(cuts))
        return jnp.repeat(jnp.exp(steps), shape[position] // blocks).reshape((-1,) + (1,) * (len(shape) - position - 1))

    gain = one(*cuts[0])
    for cut in cuts[1:]:
        gain = gain * one(*cut)
    return gain


def normal_values(stream_key, extent, deviation, reach, cuts=(), dtype=jnp.bfloat16):
    drawn = deviation * jax.random.normal(stream_key, extent, jnp.float32)
    if cuts:
        drawn = drawn * level_of(stream_key, extent, cuts, -0.22, 0.18)
    return jnp.clip(drawn, -reach, reach).astype(dtype)


def bell_draw_with(rng, extent, deviation, bound, cuts, heavy, held_as=jnp.bfloat16):
    entries = deviation * jax.random.normal(rng, extent, jnp.float32)
    if cuts:
        entries = entries * level_of(rng, extent, cuts, -0.22, 0.18)
    return jnp.clip(strengthened(entries, jax.random.fold_in(rng, 3), *heavy), -bound, bound).astype(held_as)


def setup_inputs(seed: int = 0) -> dict:
    streams_of = jax.random.split(jax.random.key(seed), 22)
    return {
        "characters": bell_draw_with(streams_of[0], (ROWS, SEQ_LEN, D), 1.0, 8.0, ((0, 16),), (0, 2, 16, 2.0)),
        "first_gain": jnp.clip(1.0 + 0.1 * jax.random.normal(streams_of[1], (D,), jnp.float32), 0.5, 1.5).astype(jnp.bfloat16),
        "first_shift": normal_values(streams_of[2], (D,), 0.3, 1.75),
        "query_weight": normal_values(streams_of[3], (D, D), (D // 2) ** -0.5, 0.3125, ((1, 2),)),
        "query_bias": normal_values(streams_of[4], (D,), 0.5, 3.0, ((0, 2),)),
        "key_weight": normal_values(streams_of[5], (D, D), (D // 2) ** -0.5, 0.3125, ((1, 2),)),
        "value_weight": normal_values(streams_of[6], (D, D), D ** -0.5, 0.21875, ((1, 2),)),
        "value_bias": normal_values(streams_of[7], (D,), 0.2, 1.25, ((0, 2),)),
        "out_weight": normal_values(streams_of[8], (D, D), (D // 8) ** -0.5, 0.625, ((0, 2),)),
        "out_bias": normal_values(streams_of[9], (D,), 0.3, 1.75),
        "second_gain": jnp.clip(1.0 + 0.1 * jax.random.normal(streams_of[10], (D,), jnp.float32), 0.5, 1.5).astype(jnp.bfloat16),
        "second_shift": normal_values(streams_of[11], (D,), 0.3, 1.75),
        "up_weight": normal_values(streams_of[12], (D, FF), D ** -0.5, 0.21875, ((1, 2),)),
        "up_bias": normal_values(streams_of[13], (FF,), 0.5, 3.0, ((0, 2),)),
        "down_weight": normal_values(streams_of[14], (FF, D), FF ** -0.5, 0.109375, ((0, 2),)),
        "down_bias": normal_values(streams_of[15], (D,), 0.3, 1.75),
        "conv_weight": normal_values(streams_of[16], (STRIDE * D, D), (STRIDE * D) ** -0.5, 0.109375, ((1, 2),)),
        "conv_bias": normal_values(streams_of[17], (D,), 0.5, 3.0, ((0, 2),)),
        "third_gain": jnp.clip(1.0 + 0.18 * jax.random.normal(streams_of[18], (D,), jnp.float32), 0.099609375, 1.8984375).astype(jnp.bfloat16),
        "third_shift": normal_values(streams_of[19], (D,), 0.3, 1.75, ((0, 2),)),
        "cotangent": draw_cotangent(jax.random.fold_in(streams_of[21], 71), 0),
    }


@jax.custom_vjp
def low(v):
    return lax.optimization_barrier(v.astype(jnp.bfloat16)).astype(jnp.float32)

@jax.custom_vjp
def low_back(v):
    return v

def low_keep(v):
    return (low(v), None)

def low_pass(kept, grad):
    return (grad,)

def back_keep(v):
    return (v, None)

def back_low(kept, grad):
    return (low(grad),)
low.defvjp(low_keep, low_pass)
low_back.defvjp(back_keep, back_low)
EPSILON = 1e-05
HIGHEST = lax.Precision.HIGHEST

def matmul_hi(left_side, right_side):
    return jnp.dot(left_side, right_side, precision=HIGHEST)

def norm_rows(inputs, scale_by, shift_by):
    row_mean = lax.optimization_barrier(jnp.mean(inputs, -1, keepdims=True))
    centered = inputs - row_mean
    inv_dev = lax.rsqrt(lax.optimization_barrier(jnp.mean(centered * centered, -1, keepdims=True)) + EPSILON)
    return centered * inv_dev * scale_by + shift_by

def row_forward(one_row, params):
    first_gain, first_shift, query_weight, query_bias, key_weight, value_weight, value_bias, out_weight, out_bias, second_gain, second_shift, up_weight, up_bias, down_weight, down_bias, conv_weight, conv_bias, third_gain, third_shift = params
    length = one_row.shape[0]
    width = one_row.shape[1]
    head_cols = width // GROUPS
    unit_cols = up_weight.shape[1] // GROUPS
    block_shape = (length // BLOCK, BLOCK, head_cols // HEAD_DIM, HEAD_DIM)
    attn_in = low(norm_rows(one_row, first_gain, first_shift))
    attn_sum = jnp.zeros((length, width), jnp.float32)
    for group_index in range(GROUPS):
        col_start = group_index * head_cols
        col_end = col_start + head_cols
        group_in = low_back(attn_in)
        queries = low(low_back(matmul_hi(group_in, query_weight[:, col_start:col_end])) + query_bias[col_start:col_end])
        key_rows = low(low_back(matmul_hi(group_in, key_weight[:, col_start:col_end])))
        value_rows = low(low_back(matmul_hi(group_in, value_weight[:, col_start:col_end])) + value_bias[col_start:col_end])
        scores = low_back(jnp.einsum('bqhd,bkhd->bhqk', queries.reshape(block_shape), key_rows.reshape(block_shape), precision=HIGHEST))
        attention = jax.nn.softmax(scores * HEAD_DIM ** (-0.5), axis=-1)
        context = jnp.einsum('bhqk,bkhd->bqhd', low(attention), value_rows.reshape(block_shape), precision=HIGHEST)
        context = low(low_back(context.reshape(length, head_cols)))
        attn_sum = attn_sum + low(matmul_hi(context, out_weight[col_start:col_end, :]))
    middle = one_row + out_bias + low_back(attn_sum)
    ffn_in = low(norm_rows(middle, second_gain, second_shift))
    ffn_sum = jnp.zeros((length, width), jnp.float32)
    for group_index in range(GROUPS):
        unit_start = group_index * unit_cols
        unit_end = unit_start + unit_cols
        group_in = low_back(ffn_in)
        upper_pre = low_back(matmul_hi(group_in, up_weight[:, unit_start:unit_end])) + up_bias[unit_start:unit_end]
        hidden = low(jax.nn.gelu(upper_pre, approximate=False))
        ffn_sum = ffn_sum + low(matmul_hi(hidden, down_weight[unit_start:unit_end, :]))
    result = middle + down_bias + low_back(ffn_sum)
    mols = length // STRIDE
    pieces = []
    for group_index in range(GROUPS):
        col_start = group_index * head_cols
        col_end = col_start + head_cols
        group_rows = low_back(result)
        windows = low(group_rows).reshape(mols, STRIDE * width)
        conv_pre = low_back(matmul_hi(windows, conv_weight[:, col_start:col_end])) + conv_bias[col_start:col_end]
        conv_act = jax.nn.gelu(conv_pre, approximate=False)
        pieces.append(jnp.concatenate([group_rows[0:1, col_start:col_end], conv_act[:mols - 1]], 0))
    gathered = jnp.concatenate(pieces, 1)
    return norm_rows(gathered, third_gain, third_shift)

def reference(characters, first_gain, first_shift, query_weight, query_bias, key_weight, value_weight, value_bias, out_weight, out_bias, second_gain, second_shift, up_weight, up_bias, down_weight, down_bias, conv_weight, conv_bias, third_gain, third_shift, cotangent):
    params = tuple((member.astype(jnp.float32) for member in (first_gain, first_shift, query_weight, query_bias, key_weight, value_weight, value_bias, out_weight, out_bias, second_gain, second_shift, up_weight, up_bias, down_weight, down_bias, conv_weight, conv_bias, third_gain, third_shift)))
    chars_wide = characters.astype(jnp.float32)

    def forward(char_rows, weights):
        row_step = jax.checkpoint(lambda single: row_forward(single, weights))
        return lax.map(row_step, char_rows)
    outputs, pullback = jax.vjp(forward, chars_wide, params)
    char_grad, weight_grads = pullback(cotangent.astype(jnp.float32))
    grad_first_gain, grad_first_shift, grad_query_weight, grad_query_bias, grad_key_weight, grad_value_weight, grad_value_bias, grad_out_weight, grad_out_bias, grad_second_gain, grad_second_shift, grad_up_weight, grad_up_bias, grad_down_weight, grad_down_bias, grad_conv_weight, grad_conv_bias, grad_third_gain, grad_third_shift = weight_grads
    return (outputs.astype(jnp.bfloat16), char_grad, grad_first_gain, grad_first_shift, grad_query_weight, grad_query_bias, grad_key_weight, grad_value_weight, grad_value_bias, grad_out_weight, grad_out_bias, grad_second_gain, grad_second_shift, grad_up_weight, grad_up_bias, grad_down_weight, grad_down_bias, grad_conv_weight, grad_conv_bias, grad_third_gain, grad_third_shift)
```

```python
import functools

import jax
import jax.numpy as jnp
from jax import lax
from jax.experimental import pallas as pl
from jax.experimental.pallas import tpu as pltpu
from jax.sharding import PartitionSpec as P

HEAD_DIM = 64
BLOCK = 128
STRIDE = 4
EPSILON = 1e-05
INV_ROOT_TWO = 0.7071067811865476
INV_ROOT_TWO_PI = 0.3989422804014327
F32 = jnp.float32
BF16 = jnp.bfloat16
PARTS = 8
ROW_TILE = 256


def times(left, right):
    return jnp.dot(left, right, preferred_element_type=F32)


def times_t(left, right):
    return lax.dot_general(left, right, (((1,), (1,)), ((), ())), preferred_element_type=F32)


def t_times(left, right):
    return lax.dot_general(left, right, (((0,), (0,)), ((), ())), preferred_element_type=F32)


def gelu_parts(u):
    phi = 0.5 + 0.5 * lax.erf(u * INV_ROOT_TWO)
    return u * phi, phi + u * (jnp.exp(-0.5 * (u * u)) * INV_ROOT_TWO_PI)


def norm_stats(values):
    mean = jnp.mean(values, -1, keepdims=True)
    centered = values - mean
    inv = lax.rsqrt(jnp.mean(centered * centered, -1, keepdims=True) + EPSILON)
    return centered * inv, inv


def norm_back(scaled, hat, inv):
    return inv * (
        scaled
        - jnp.mean(scaled, -1, keepdims=True)
        - hat * jnp.mean(scaled * hat, -1, keepdims=True)
    )


def column_sum(values):
    return jnp.sum(values, 0, keepdims=True)


def call(body, outs, ins, scratch=(), vmem_mb=32, flops=0, bytes_accessed=0, name=None, spaces=None):
    spaces = spaces or {}
    in_specs = [pl.BlockSpec(memory_space=spaces.get(("in", i), pltpu.VMEM)) for i in range(len(ins))]
    out_specs = [pl.BlockSpec(memory_space=spaces.get(("out", i), pltpu.VMEM)) for i in range(len(outs))]
    return pl.pallas_call(
        body,
        out_shape=[jax.ShapeDtypeStruct(shape, dtype) for shape, dtype in outs],
        in_specs=in_specs,
        out_specs=out_specs,
        scratch_shapes=list(scratch),
        compiler_params=pltpu.CompilerParams(vmem_limit_bytes=vmem_mb << 20),
        cost_estimate=pl.CostEstimate(
            flops=int(flops), bytes_accessed=int(bytes_accessed), transcendentals=0
        ),
        name=name,
    )(*ins)


def rows_at(step, tile=ROW_TILE):
    return pl.ds(pl.multiple_of(step * tile, tile), tile)


def pair_masks():
    lane = lax.broadcasted_iota(jnp.int32, (1, 2 * HEAD_DIM), 1)
    low = (lane < HEAD_DIM).astype(F32).astype(BF16)
    high = (lane >= HEAD_DIM).astype(F32).astype(BF16)
    return low, high


def stacked(pair, masks):
    return jnp.concatenate([pair * masks[0], pair * masks[1]], 0)


def place_parts(part_refs, counts, table, targets, sems):
    copies = []
    slot = 0
    place = 0
    for ref, count in zip(part_refs, counts):
        for item in range(count):
            where = table[place]
            place += 1
            for start, rows, target, columns in targets:
                copies.append(
                    pltpu.make_async_copy(
                        ref.at[item, pl.ds(start, rows), :],
                        target.at[pl.ds(pl.multiple_of(where * rows, 16), rows), columns],
                        sems.at[slot],
                    )
                )
                slot += 1
    return copies


def attention_forward(attn_in, wq, wk, wv, qb, vb, rows, q_ref, k_ref, v_ref, p_ref, ctx_ref, masks):
    queries = (times(attn_in, wq[...]) + qb[...]).astype(BF16)
    keys = times(attn_in, wk[...]).astype(BF16)
    values = (times(attn_in, wv[...]) + vb[...]).astype(BF16)
    q_ref[rows, :] = queries
    k_ref[rows, :] = keys
    v_ref[rows, :] = values
    pairs = queries.shape[1] // (2 * HEAD_DIM)
    for block in range(attn_in.shape[0] // BLOCK):
        chars = slice(block * BLOCK, (block + 1) * BLOCK)
        here = pl.ds(rows.start + block * BLOCK, BLOCK)
        for pair in range(pairs):
            lanes = slice(pair * 2 * HEAD_DIM, (pair + 1) * 2 * HEAD_DIM)
            scores = times_t(queries[chars, lanes], stacked(keys[chars, lanes], masks))
            scores = scores * HEAD_DIM ** (-0.5)
            probs = []
            for head in range(2):
                part = scores[:, head * BLOCK : (head + 1) * BLOCK]
                expo = jnp.exp(part - jnp.max(part, -1, keepdims=True))
                probs.append(expo * (1.0 / jnp.sum(expo, -1, keepdims=True)))
            both = jnp.concatenate(probs, 1).astype(BF16)
            p_ref[here, pair * 2 * BLOCK : (pair + 1) * 2 * BLOCK] = both
            ctx_ref[here, lanes] = times(both, stacked(values[chars, lanes], masks)).astype(BF16)


def own_attention(x, gain, shift, wq, wk, wv, qb, vb):
    span, width = x.shape
    half = wq.shape[1]

    def body(x_ref, g, s, wq, wk, wv, qb, vb, a_ref, q_ref, k_ref, v_ref, p_ref, ctx_ref):
        masks = pair_masks()

        def step(i, carry):
            rows = rows_at(i)
            hat, _ = norm_stats(x_ref[rows, :].astype(F32))
            attn_in = (hat * g[...] + s[...]).astype(BF16)
            a_ref[rows, :] = attn_in
            attention_forward(attn_in, wq, wk, wv, qb, vb, rows, q_ref, k_ref, v_ref, p_ref, ctx_ref, masks)
            return carry

        lax.fori_loop(0, span // ROW_TILE, step, 0)

    outs = [((span, width), BF16)] + [((span, half), BF16)] * 3
    outs += [((span, half // HEAD_DIM * BLOCK), BF16), ((span, half), BF16)]
    return call(body, outs, (x, gain, shift, wq, wk, wv, qb, vb), vmem_mb=24,
                flops=2 * span * width * half * 3.5, bytes_accessed=8e6, name="own_attention")


def other_attention(a, parts, table, qb, vb):
    span, width = a.shape
    half = qb.shape[1]
    counts = [part.shape[0] for part in parts]
    n = len(parts)

    def body(a_ref, qb, vb, table, *refs):
        part_refs = refs[:n]
        wq, wk, wv, wo, q_ref, k_ref, v_ref, p_ref, ctx_ref, sems = refs[n:]
        masks = pair_masks()
        rows_q = width // PARTS
        rows_o = half // PARTS
        targets = [(i * rows_q, rows_q, ref, slice(None)) for i, ref in enumerate((wq, wk, wv))]
        targets += [(3 * rows_q + i * rows_o, rows_o, wo, pl.ds(i * half, half)) for i in range(2)]
        copies = place_parts(part_refs, counts, table, targets, sems)
        for copy in copies:
            copy.start()
        for copy in copies:
            copy.wait()

        def step(i, carry):
            rows = rows_at(i)
            attention_forward(a_ref[rows, :], wq, wk, wv, qb, vb, rows, q_ref, k_ref, v_ref, p_ref, ctx_ref, masks)
            return carry

        lax.fori_loop(0, span // ROW_TILE, step, 0)

    outs = [((width, half), BF16)] * 3 + [((half, width), BF16)] + [((span, half), BF16)] * 3
    outs += [((span, half // HEAD_DIM * BLOCK), BF16), ((span, half), BF16)]
    spaces = {("in", 3): pltpu.SMEM}
    spaces.update({("in", 4 + i): pl.ANY for i in range(n)})
    return call(body, outs, (a, qb, vb, table, *parts), [pltpu.SemaphoreType.DMA((PARTS * 5,))], 24,
                2 * span * width * half * 3.5, 9e6, "other_attention", spaces)


def attention_output(x, ctx_own, ctx_other, wo_own, wo_other, bias, gain, shift):
    span, width = x.shape

    def body(x_ref, co, ct, wo, wt, b, g, s, h_ref, c_ref):
        def step(i, carry):
            rows = rows_at(i)
            middle = x_ref[rows, :].astype(F32) + b[...] + times(co[rows, :], wo[...]) + times(ct[rows, :], wt[...])
            h_ref[rows, :] = middle
            hat, _ = norm_stats(middle)
            c_ref[rows, :] = (hat * g[...] + s[...]).astype(BF16)
            return carry

        lax.fori_loop(0, span // ROW_TILE, step, 0)

    outs = [((span, width), F32), ((span, width), BF16)]
    return call(body, outs, (x, ctx_own, ctx_other, wo_own, wo_other, bias, gain, shift), vmem_mb=16,
                flops=2 * span * width * width, bytes_accessed=9e6, name="attention_output")


HIDDEN_TILE = 512


def feed_forward_half(c_ref, acc_ref, up, ub, down, hid_ref, slope_ref):
    span = c_ref.shape[0]
    units = up.shape[1]

    def step(j, carry):
        cols = rows_at(j, HIDDEN_TILE)
        for i in range(span // ROW_TILE):
            rows = slice(i * ROW_TILE, (i + 1) * ROW_TILE)
            upper = times(c_ref[rows, :], up[:, cols]) + ub[:, cols]
            hidden, slope = gelu_parts(upper)
            hidden = hidden.astype(BF16)
            hid_ref[rows, cols] = hidden
            slope_ref[rows, cols] = slope.astype(BF16)
            acc_ref[rows, :] += times(hidden, down[cols, :])
        return carry

    lax.fori_loop(0, units // HIDDEN_TILE, step, 0)


def own_feed_forward(c, middle, bias, up, ub, down):
    span, width = c.shape
    units = up.shape[1]

    def body(c_ref, m_ref, b, up, ub, down, hid_ref, slope_ref, acc_ref):
        acc_ref[...] = m_ref[...] + b[...]
        feed_forward_half(c_ref, acc_ref, up, ub, down, hid_ref, slope_ref)

    outs = [((span, units), BF16)] * 2 + [((span, width), F32)]
    return call(body, outs, (c, middle, bias, up, ub, down), vmem_mb=28,
                flops=4 * span * width * units, bytes_accessed=16e6, name="own_feed_forward")


def other_feed_forward(c, acc, ub, up_parts, down_parts, table):
    span, width = c.shape
    units = ub.shape[1]
    counts = [part.shape[0] for part in up_parts]
    n = len(up_parts)

    def body(c_ref, a_ref, ub, table, *refs):
        up_refs, down_refs = refs[:n], refs[n : 2 * n]
        up, down, hid_ref, slope_ref, acc_ref, up_sems, down_sems = refs[2 * n :]
        ups = place_parts(up_refs, counts, table, [(0, width // PARTS, up, slice(None))], up_sems)
        downs = place_parts(down_refs, counts, table, [(0, units // PARTS, down, slice(None))], down_sems)
        for copy in ups + downs:
            copy.start()
        acc_ref[...] = a_ref[...]
        for copy in ups + downs:
            copy.wait()
        feed_forward_half(c_ref, acc_ref, up, ub, down, hid_ref, slope_ref)

    outs = [((width, units), BF16), ((units, width), BF16)] + [((span, units), BF16)] * 2 + [((span, width), F32)]
    spaces = {("in", 3): pltpu.SMEM}
    spaces.update({("in", 4 + i): pl.ANY for i in range(2 * n)})
    sems = [pltpu.SemaphoreType.DMA((PARTS,))] * 2
    return call(body, outs, (c, acc, ub, table, *up_parts, *down_parts), sems, 28,
                4 * span * width * units, 18e6, "other_feed_forward", spaces)


def downsample(h2, wc_own, wc_parts, table, bias, gain, shift, cot, cot_first):
    span, width = h2.shape
    half = width // 2
    mols = span // STRIDE
    counts = [part.shape[0] for part in wc_parts]
    n = len(wc_parts)

    def body(h_ref, wo, b, g, s, cot_ref, first_ref, table, *refs):
        part_refs = refs[:n]
        hs_ref, dc_ref, mol_ref, mol0_ref, dh_ref, dh16_ref, vec_ref, wt, strip, sems = refs[n:]
        copies = place_parts(part_refs, counts, table, [(0, STRIDE * width // PARTS, wt, slice(None))], sems)
        for copy in copies:
            copy.start()
        pre_own = jnp.zeros((mols, half), F32)
        for lane in range(width // 128):
            strip[lane] = h_ref[:, lane * 128 : (lane + 1) * 128]
        for tap in range(STRIDE):
            window = jnp.concatenate(
                [strip[lane, pl.ds(tap, mols, stride=STRIDE), :] for lane in range(width // 128)], 1
            ).astype(BF16)
            hs_ref[tap * mols : (tap + 1) * mols, :] = window
            pre_own += times(window, wo[tap * width : (tap + 1) * width, :])
        for copy in copies:
            copy.wait()
        pre_other = jnp.zeros((mols, half), F32)
        for tap in range(STRIDE):
            window = hs_ref[tap * mols : (tap + 1) * mols, :]
            pre_other += times(window, wt[tap * width : (tap + 1) * width, :])
        conv = jnp.concatenate([pre_own, pre_other], 1) + b[...]
        act, slope = gelu_parts(conv)
        hat, inv = norm_stats(act)
        mol_ref[...] = (hat * g[...] + s[...]).astype(BF16)
        cotangent = cot_ref[...].astype(F32)
        dpre = norm_back(cotangent * g[...], hat, inv)
        dconv = dpre * slope
        dconv16 = dconv.astype(BF16)
        dc_ref[...] = dconv16
        hat0, inv0 = norm_stats(h_ref[0:8, :])
        mol0_ref[...] = hat0 * g[...] + s[...]
        cot0 = first_ref[...]
        dpre0 = norm_back(cot0 * g[...], hat0, inv0)
        vec_ref[...] = jnp.zeros_like(vec_ref)
        vec_ref[0:1, :] = column_sum(cotangent * hat) + column_sum(cot0 * hat0)
        vec_ref[1:2, :] = column_sum(cotangent) + column_sum(cot0)
        vec_ref[2:3, :] = column_sum(dconv)
        for tap in range(STRIDE):
            taps = slice(tap * width, (tap + 1) * width)
            back = times_t(dconv16[:, :half], wo[taps, :]) + times_t(dconv16[:, half:], wt[taps, :])
            for lane in range(width // 128):
                strip[lane, pl.ds(tap, mols, stride=STRIDE), :] = back[:, lane * 128 : (lane + 1) * 128]
        for lane in range(width // 128):
            dh_ref[:, lane * 128 : (lane + 1) * 128] = strip[lane]
        dh_ref[0:8, :] += dpre0
        total = jnp.zeros((1, width), F32)
        for i in range(span // ROW_TILE):
            rows = slice(i * ROW_TILE, (i + 1) * ROW_TILE)
            grad = dh_ref[rows, :]
            dh16_ref[rows, :] = grad.astype(BF16)
            total += column_sum(grad)
        vec_ref[3:4, :] = total

    outs = [((span, width), BF16), ((mols, width), BF16), ((mols, width), BF16), ((8, width), F32),
            ((span, width), F32), ((span, width), BF16), ((8, width), F32)]
    spaces = {("in", 7): pltpu.SMEM}
    spaces.update({("in", 8 + i): pl.ANY for i in range(n)})
    scratch = [pltpu.VMEM((STRIDE * width, half), BF16), pltpu.VMEM((width // 128, span, 128), F32), pltpu.SemaphoreType.DMA((PARTS,))]
    return call(body, outs, (h2, wc_own, bias, gain, shift, cot, cot_first, table, *wc_parts), scratch, 28,
                8 * span * width * width / 2, 16e6, "downsample", spaces)


def scatter_blocks(scratch, table, keep_ref, send_ref, sems, rows):
    copies = []
    for where, ref in enumerate((keep_ref, send_ref)):
        for place in range(16):
            slot = where * 16 + place
            half = table[2 * slot]
            block = table[2 * slot + 1]
            copies.append(
                pltpu.make_async_copy(
                    scratch.at[half, pl.ds(pl.multiple_of(block * rows, 16), rows), :],
                    ref.at[place],
                    sems.at[slot],
                )
            )
    for copy in copies:
        copy.start()
    for copy in copies:
        copy.wait()


def conv_weight_grad(hs, dconv16, table):
    span, width = hs.shape
    half = width // 2
    mols = span // STRIDE
    rows = STRIDE * width // 16

    def body(hs_ref, dc_ref, table, keep_ref, send_ref, scratch, sems):
        def step(tap, carry):
            grad = t_times(hs_ref[pl.ds(pl.multiple_of(tap * mols, 16), mols), :], dc_ref[...]).astype(BF16)
            taps = pl.ds(pl.multiple_of(tap * width, 16), width)
            scratch[0, taps, :] = grad[:, :half]
            scratch[1, taps, :] = grad[:, half:]
            return carry

        lax.fori_loop(0, STRIDE, step, 0)
        scatter_blocks(scratch, table, keep_ref, send_ref, sems, rows)

    outs = [((16, rows, half), BF16)] * 2
    spaces = {("in", 2): pltpu.SMEM, ("out", 0): pl.ANY, ("out", 1): pl.ANY}
    scratch = [pltpu.VMEM((2, STRIDE * width, half), BF16), pltpu.SemaphoreType.DMA((32,))]
    return call(body, outs, (hs, dconv16, table), scratch, 16, 2 * span * width * width, 7e6, "conv_weight_grad", spaces)


def weight_grad(lefts, rights, table, name):
    span, width = lefts[0].shape
    units = sum(array.shape[1] for _, array in rights[0])
    rows = width // 16
    flat = [array for group in rights for _, array in group]
    nl, nr = len(lefts), len(flat)

    def body(*refs):
        left_refs, right_refs = refs[:nl], refs[nl : nl + nr]
        table = refs[nl + nr]
        keep_ref, send_ref, turned, scratch, sems = refs[nl + nr + 1 :]
        for i, ref in enumerate(left_refs):
            turned[i] = ref[...].T
        at = 0
        for group_index, group in enumerate(rights):
            column = 0
            for which, array in group:
                ref = right_refs[at]
                at += 1
                tile = min(HIDDEN_TILE, array.shape[1])

                def step(j, carry, ref=ref, which=which, group_index=group_index, column=column, tile=tile):
                    cols = rows_at(j, tile)
                    target = pl.ds(pl.multiple_of(column + j * tile, 128), tile)
                    for i in range(width // ROW_TILE):
                        part = slice(i * ROW_TILE, (i + 1) * ROW_TILE)
                        scratch[group_index, part, target] = times(turned[which, part, :], ref[:, cols]).astype(BF16)
                    return carry

                lax.fori_loop(0, array.shape[1] // tile, step, 0)
                column += array.shape[1]
        scatter_blocks(scratch, table, keep_ref, send_ref, sems, rows)

    outs = [((16, rows, units), BF16)] * 2
    spaces = {("in", nl + nr): pltpu.SMEM, ("out", 0): pl.ANY, ("out", 1): pl.ANY}
    scratch = [pltpu.VMEM((nl, width, span), BF16), pltpu.VMEM((2, width, units), BF16), pltpu.SemaphoreType.DMA((32,))]
    return call(body, outs, (*lefts, *flat, table), scratch, 20, 4 * span * width * units, 12e6, name, spaces)


def feed_forward_backward(dh2, dh2_16, middle, gain, slopes, ups, downs):
    span, width = dh2.shape
    units = ups[0].shape[1]

    def body(dh_ref, dh16_ref, m_ref, g, slope_o, slope_t, up_o, up_t, down_o, down_t,
             du_o, du_t, dm_ref, dm16_ref, vec_ref, ub_o, ub_t, acc_ref):
        acc_ref[...] = jnp.zeros_like(acc_ref)
        for slope_ref, up, down, du_ref, ub_ref in (
            (slope_o, up_o, down_o, du_o, ub_o),
            (slope_t, up_t, down_t, du_t, ub_t),
        ):
            def step(j, carry, slope_ref=slope_ref, up=up, down=down, du_ref=du_ref, ub_ref=ub_ref):
                cols = rows_at(j, HIDDEN_TILE)
                total = jnp.zeros((1, HIDDEN_TILE), F32)
                for i in range(span // ROW_TILE):
                    rows = slice(i * ROW_TILE, (i + 1) * ROW_TILE)
                    grad = times_t(dh16_ref[rows, :], down[cols, :]) * slope_ref[rows, cols].astype(F32)
                    total += column_sum(grad)
                    grad16 = grad.astype(BF16)
                    du_ref[rows, cols] = grad16
                    acc_ref[rows, :] += times_t(grad16, up[:, cols])
                ub_ref[:, cols] = total
                return carry

            lax.fori_loop(0, units // HIDDEN_TILE, step, 0)
        vec_ref[...] = jnp.zeros_like(vec_ref)

        def close(i, carry):
            rows = rows_at(i)
            back = acc_ref[rows, :]
            hat, inv = norm_stats(m_ref[rows, :])
            grad = dh_ref[rows, :] + norm_back(back * g[...], hat, inv)
            dm_ref[rows, :] = grad
            dm16_ref[rows, :] = grad.astype(BF16)
            vec_ref[0:1, :] += column_sum(back * hat)
            vec_ref[1:2, :] += column_sum(back)
            vec_ref[2:3, :] += column_sum(grad)
            return carry

        lax.fori_loop(0, span // ROW_TILE, close, 0)

    outs = [((span, units), BF16)] * 2 + [((span, width), F32), ((span, width), BF16), ((8, width), F32)]
    outs += [((1, units), F32)] * 2
    return call(body, outs, (dh2, dh2_16, middle, gain, *slopes, *ups, *downs), [pltpu.VMEM((span, width), F32)], 40,
                8 * span * width * units, 30e6, "feed_forward_backward")


def attention_backward(dm16, wo, probs, q, k, v, name):
    span, width = dm16.shape
    half = q.shape[1]

    def body(dm_ref, wo, p_ref, q_ref, k_ref, v_ref, dq_ref, dk_ref, dv_ref, vec_ref):
        masks = pair_masks()
        lane = lax.broadcasted_iota(jnp.int32, (1, 2 * HEAD_DIM), 1) < HEAD_DIM
        vec_ref[...] = jnp.zeros_like(vec_ref)

        def step(i, carry):
            rows = rows_at(i)
            dctx = times_t(dm_ref[rows, :], wo[...]).astype(BF16)
            for block in range(ROW_TILE // BLOCK):
                chars = slice(block * BLOCK, (block + 1) * BLOCK)
                here = pl.ds(rows.start + block * BLOCK, BLOCK)
                for pair in range(half // (2 * HEAD_DIM)):
                    lanes = slice(pair * 2 * HEAD_DIM, (pair + 1) * 2 * HEAD_DIM)
                    keys = slice(pair * 2 * BLOCK, (pair + 1) * 2 * BLOCK)
                    p = p_ref[here, keys]
                    grad = dctx[chars, lanes]
                    dv2 = t_times(p, grad)
                    dv = jnp.where(lane, dv2[:BLOCK], dv2[BLOCK:])
                    dp = times_t(grad, stacked(v_ref[here, lanes], masks))
                    p32 = p.astype(F32)
                    ds = []
                    for head in range(2):
                        part = slice(head * BLOCK, (head + 1) * BLOCK)
                        weighted = p32[:, part] * dp[:, part]
                        inner = jnp.sum(weighted, -1, keepdims=True)
                        ds.append((weighted - p32[:, part] * inner) * HEAD_DIM ** (-0.5))
                    ds = jnp.concatenate(ds, 1).astype(BF16)
                    dq = times(ds, stacked(k_ref[here, lanes], masks))
                    dk2 = t_times(ds, q_ref[here, lanes])
                    dk = jnp.where(lane, dk2[:BLOCK], dk2[BLOCK:])
                    dq_ref[here, lanes] = dq.astype(BF16)
                    dk_ref[here, lanes] = dk.astype(BF16)
                    dv_ref[here, lanes] = dv.astype(BF16)
                    vec_ref[0:1, lanes] += column_sum(dq)
                    vec_ref[1:2, lanes] += column_sum(dv)
            return carry

        lax.fori_loop(0, span // ROW_TILE, step, 0)

    outs = [((span, half), BF16)] * 3 + [((8, half), F32)]
    return call(body, outs, (dm16, wo, probs, q, k, v), vmem_mb=16,
                flops=2 * span * width * half * 2, bytes_accessed=8e6, name=name)


def input_backward(dm, x, gain, grads, weights):
    span, width = dm.shape
    n = len(grads)

    def body(dm_ref, x_ref, g, *refs):
        grad_refs, weight_refs = refs[:n], refs[n : 2 * n]
        out_ref, vec_ref = refs[2 * n :]
        vec_ref[...] = jnp.zeros_like(vec_ref)

        def step(i, carry):
            rows = rows_at(i)
            back = times_t(grad_refs[0][rows, :], weight_refs[0][...])
            for grad_ref, weight_ref in zip(grad_refs[1:], weight_refs[1:]):
                back += times_t(grad_ref[rows, :], weight_ref[...])
            hat, inv = norm_stats(x_ref[rows, :].astype(F32))
            out_ref[rows, :] = dm_ref[rows, :] + norm_back(back * g[...], hat, inv)
            vec_ref[0:1, :] += column_sum(back * hat)
            vec_ref[1:2, :] += column_sum(back)
            return carry

        lax.fori_loop(0, span // ROW_TILE, step, 0)

    outs = [((span, width), F32), ((8, width), F32)]
    return call(body, outs, (dm, x, gain, *grads, *weights), vmem_mb=24,
                flops=2 * span * width * 3 * width, bytes_accessed=12e6, name="input_backward")


def flat_permute(value, route, dp_size):
    pairs = []
    for d in range(dp_size):
        for t in range(2):
            d2, t2 = route(d, t)
            pairs.append((d * 2 + t, d2 * 2 + t2))
    return lax.ppermute(value, ("dp", "tensor"), pairs)


def over_x(d, t):
    return d, 1 - t


def over_core(d, t):
    return d ^ 1, t


def over_y(d, t):
    return d ^ 2, t


def over_z_near(d, t):
    return d ^ 4, t


def over_z_far(d, t):
    return d ^ 8, t


def by_core(first, second):
    return lambda d, t: (second if d & 1 else first)(d, t)


class Grid:
    def __init__(self):
        self.dp = lax.axis_size("dp")
        self.index = lax.axis_index("dp")
        self.side = lax.axis_index("tensor")
        self.fast = self.dp == 16
        core = self.index % 2
        y = (self.index // 2) % 2
        z = self.index // 4
        if not self.fast:
            self.parts_table = jnp.arange(PARTS, dtype=jnp.int32)
            order = [v for half in range(2) for block in range(16) for v in (half, block)]
            self.block_table = jnp.array(order, jnp.int32)
            return
        self.mine = core * 4 + y * 2 + z % 2
        near = jnp.where(core == 0, 2, 1)
        far = 3 - near
        me = self.mine
        self.parts_table = jnp.stack(
            [me, me ^ near, me ^ far, me ^ 3, me ^ 4, me ^ 4 ^ far, me ^ 4 ^ near, me ^ 7]
        ).astype(jnp.int32)
        table = []
        for where in range(2):
            target = core ^ where
            for place in range(16):
                b1, b2, b3, b4 = [(place >> s) & 1 for s in (3, 2, 1, 0)]
                half = jnp.where(target == 0, b1, b2)
                flip = jnp.where(target == 0, b2, b1)
                table += [half, (z ^ (b3 + 2 * b4)) * 4 + (y ^ flip) * 2 + target]
        self.block_table = jnp.stack(table).astype(jnp.int32)

    def send(self, value, route):
        return flat_permute(value, route, self.dp)

    def gather(self, own):
        if not self.fast:
            return [self.send(own, over_x)]
        mine = lax.dynamic_slice_in_dim(own, self.mine, 1, 0)
        first = self.send(mine, over_x)
        second = self.send(first, by_core(over_y, over_z_near))
        third = self.send(jnp.concatenate([first, second], 0), by_core(over_z_near, over_y))
        fourth = self.send(jnp.concatenate([first, second, third], 0), over_core)
        return [first, second, third, fourth]

    def reduce(self, keep, away):
        if not self.fast:
            total = keep.astype(F32) + self.send(away, over_x).astype(F32)
            total = total.reshape(-1, total.shape[-1])
            return lax.psum_scatter(total, "dp", scatter_dimension=0, tiled=True)
        got = self.send(away, over_core)
        routes = (by_core(over_x, over_y), by_core(over_y, over_x), over_z_near, over_z_far)
        for route in routes:
            size = keep.shape[0] // 2
            out = (keep[size:].astype(F32) + got[size:].astype(F32)).astype(BF16)
            keep = (keep[:size].astype(F32) + got[:size].astype(F32)).astype(BF16)
            got = self.send(out, route)
        return (keep.astype(F32) + got.astype(F32))[0]

    def reduce_vectors(self, shared, own, other):
        rows = shared.shape[0]
        got = self.send(jnp.concatenate([shared, other], 0), over_x)
        total = jnp.concatenate([shared, own], 0) + got
        if not self.fast:
            total = lax.psum(total, "dp")
        else:
            for route in (over_core, over_y, over_z_near, over_z_far):
                total = total + self.send(total, route)
        return total[:rows], total[rows:]


def per_device(
    characters, first_gain, first_shift, query_weight, query_bias, key_weight, value_weight, value_bias,
    out_weight, out_bias, second_gain, second_shift, up_weight, up_bias, down_weight, down_bias,
    conv_weight, conv_bias, third_gain, third_shift, cotangent,
):
    _, length, width = characters.shape
    span = length // 2
    half = width // 2
    units = up_weight.shape[1]
    mols = span // STRIDE
    grid = Grid()
    side = grid.side

    def row(vector):
        return vector.astype(F32).reshape(1, -1)

    packed = jnp.concatenate([query_bias, value_bias, conv_bias, third_gain, third_shift, up_bias]).reshape(-1, half)
    packed_other = grid.send(packed, over_x)
    other_query_bias, other_value_bias = row(packed_other[0]), row(packed_other[1])
    conv_bias_both, third_gain_both, third_shift_both = (
        jnp.concatenate([row(packed[i]), row(packed_other[i])], 1) for i in (2, 3, 4)
    )
    other_up_bias = row(packed_other[5:])

    piece = jnp.concatenate(
        [w.reshape(PARTS, width // PARTS, half) for w in (query_weight, key_weight, value_weight)]
        + [out_weight[:, i * half : (i + 1) * half].reshape(PARTS, half // PARTS, half) for i in range(2)],
        1,
    )
    attention_parts = grid.gather(piece)
    up_parts = grid.gather(up_weight.reshape(PARTS, width // PARTS, units))
    down_parts = grid.gather(down_weight.reshape(PARTS, units // PARTS, width))
    conv_parts = grid.gather(conv_weight.reshape(PARTS, STRIDE * width // PARTS, half))

    x = lax.dynamic_slice_in_dim(characters[0], side * span, span, 0)
    a, q_own, k_own, v_own, p_own, ctx_own = own_attention(
        x, row(first_gain), row(first_shift), query_weight, key_weight, value_weight, row(query_bias), row(value_bias)
    )
    wq_other, wk_other, wv_other, wo_other, q_other, k_other, v_other, p_other, ctx_other = other_attention(
        a, attention_parts, grid.parts_table, other_query_bias, other_value_bias
    )
    middle, c = attention_output(
        x, ctx_own, ctx_other, out_weight, wo_other, row(out_bias), row(second_gain), row(second_shift)
    )
    hid_own, slope_own, acc = own_feed_forward(c, middle, row(down_bias), up_weight, row(up_bias), down_weight)
    up_other, down_other, hid_other, slope_other, h2 = other_feed_forward(
        c, acc, other_up_bias, up_parts, down_parts, grid.parts_table
    )

    cot = cotangent[0]
    cot_rows = lax.dynamic_slice_in_dim(jnp.pad(cot, ((0, 1), (0, 0))), side * mols + 1, mols, 0)
    cot_rows = jnp.where(side == 0, cot_rows, jnp.concatenate([cot_rows[:, half:], cot_rows[:, :half]], 1))
    cot_first = jnp.pad(jnp.where(side == 0, cot[0:1].astype(F32), 0.0), ((0, 7), (0, 0)))
    hs, dconv16, mol, mol_first, dh2, dh2_16, conv_vec = downsample(
        h2, conv_weight, conv_parts, grid.parts_table, conv_bias_both, third_gain_both, third_shift_both,
        cot_rows, cot_first,
    )
    mine = jnp.concatenate([mol_first[0:1].astype(BF16), mol], 0)
    theirs = grid.send(mine[:, half:], over_x)
    mine = mine[:, :half]
    upper = jnp.where(side == 0, mine, theirs)
    lower = jnp.where(side == 0, theirs, mine)
    molecules = jnp.concatenate([upper, lower[1:mols]], 0)[None]
    sum_conv_weight = grid.reduce(*conv_weight_grad(hs, dconv16, grid.block_table))

    sum_down = grid.reduce(
        *weight_grad((dh2_16,), [[(0, hid_own)], [(0, hid_other)]], grid.block_table, "down_weight_grad")
    )
    du_own, du_other, dm, dm16, ffn_vec, up_vec_own, up_vec_other = feed_forward_backward(
        dh2, dh2_16, middle, row(second_gain), (slope_own, slope_other), (up_weight, up_other), (down_weight, down_other)
    )
    sum_up = grid.reduce(*weight_grad((c,), [[(0, du_own)], [(0, du_other)]], grid.block_table, "up_weight_grad"))
    dq_own, dk_own, dv_own, vec_own = attention_backward(
        dm16, out_weight, p_own, q_own, k_own, v_own, "own_attention_backward"
    )
    dq_other, dk_other, dv_other, vec_other = attention_backward(
        dm16, wo_other, p_other, q_other, k_other, v_other, "other_attention_backward"
    )
    sum_attention = grid.reduce(
        *weight_grad(
            (a, dm16),
            [
                [(0, dq_own), (0, dk_own), (0, dv_own), (1, ctx_own)],
                [(0, dq_other), (0, dk_other), (0, dv_other), (1, ctx_other)],
            ],
            grid.block_table,
            "attention_weight_grad",
        )
    )
    input_rows, in_vec = input_backward(
        dm, x, row(first_gain), (dq_own, dk_own, dv_own, dq_other, dk_other, dv_other),
        (query_weight, key_weight, value_weight, wq_other, wk_other, wv_other),
    )

    shared = jnp.concatenate([conv_vec[3:4], ffn_vec[0:3], in_vec[0:2]], 0).reshape(-1, half)
    own = jnp.concatenate([conv_vec[0:3, :half], vec_own[0:2], up_vec_own.reshape(-1, half)], 0)
    other = jnp.concatenate([conv_vec[0:3, half:], vec_other[0:2], up_vec_other.reshape(-1, half)], 0)
    shared, own = grid.reduce_vectors(shared, own, other)
    shared = shared.reshape(-1, width)
    block = width // grid.dp
    shared = lax.dynamic_slice_in_dim(shared, grid.index * block, block, 1)
    return (
        molecules,
        input_rows[None],
        shared[4],
        shared[5],
        sum_attention[:, :half],
        own[3],
        sum_attention[:, half : 2 * half],
        sum_attention[:, 2 * half : 3 * half],
        own[4],
        sum_attention[:, 3 * half :].T,
        shared[3],
        shared[1],
        shared[2],
        sum_up,
        own[5:].reshape(-1),
        sum_down.T,
        shared[0],
        sum_conv_weight,
        own[2],
        own[0],
        own[1],
    )


def solution(mesh):
    return jax.shard_map(
        per_device,
        mesh=mesh,
        in_specs=(
            P("dp", None, None),
            P(),
            P(),
            P(None, "tensor"),
            P("tensor"),
            P(None, "tensor"),
            P(None, "tensor"),
            P("tensor"),
            P("tensor", None),
            P(),
            P(),
            P(),
            P(None, "tensor"),
            P("tensor"),
            P("tensor", None),
            P(),
            P(None, "tensor"),
            P("tensor"),
            P("tensor"),
            P("tensor"),
            P("dp", None, None),
        ),
        out_specs=(
            P("dp", None, "tensor"),
            P("dp", "tensor", None),
            P("dp"),
            P("dp"),
            P("dp", "tensor"),
            P("tensor"),
            P("dp", "tensor"),
            P("dp", "tensor"),
            P("tensor"),
            P("tensor", "dp"),
            P("dp"),
            P("dp"),
            P("dp"),
            P("dp", "tensor"),
            P("tensor"),
            P("tensor", "dp"),
            P("dp"),
            P("dp", "tensor"),
            P("tensor"),
            P("tensor"),
            P("tensor"),
        ),
        check_vma=False,
    )
```

```python
import functools

import jax
import jax.numpy as jnp
from jax import lax
from jax.experimental import pallas as pl
from jax.experimental.pallas import tpu as pltpu
from jax.sharding import PartitionSpec as P

HEAD_DIM = 64
BLOCK = 128
STRIDE = 4
EPSILON = 1e-05
INV_ROOT_TWO = 0.7071067811865476
INV_ROOT_TWO_PI = 0.3989422804014327
F32 = jnp.float32
BF16 = jnp.bfloat16
PARTS = 4
ROW_TILE = 256


def times(left, right):
    return jnp.dot(left, right, preferred_element_type=F32)


def times_t(left, right):
    return lax.dot_general(left, right, (((1,), (1,)), ((), ())), preferred_element_type=F32)


def t_times(left, right):
    return lax.dot_general(left, right, (((0,), (0,)), ((), ())), preferred_element_type=F32)


def gelu_parts(u):
    phi = 0.5 + 0.5 * lax.erf(u * INV_ROOT_TWO)
    return u * phi, phi + u * (jnp.exp(-0.5 * (u * u)) * INV_ROOT_TWO_PI)


def norm_stats(values):
    mean = jnp.mean(values, -1, keepdims=True)
    centered = values - mean
    inv = lax.rsqrt(jnp.mean(centered * centered, -1, keepdims=True) + EPSILON)
    return centered * inv, inv


def norm_back(scaled, hat, inv):
    return inv * (
        scaled
        - jnp.mean(scaled, -1, keepdims=True)
        - hat * jnp.mean(scaled * hat, -1, keepdims=True)
    )


def vector_row(ref, index, width):
    return ref[:, index * width : (index + 1) * width]


def column_sum(values):
    return jnp.sum(values, 0, keepdims=True)


def call(body, outs, ins, scratch=(), vmem_mb=32, flops=0, bytes_accessed=0, name=None, spaces=None):
    spaces = spaces or {}
    in_specs = [pl.BlockSpec(memory_space=spaces.get(("in", i), pltpu.VMEM)) for i in range(len(ins))]
    out_specs = [pl.BlockSpec(memory_space=spaces.get(("out", i), pltpu.VMEM)) for i in range(len(outs))]
    return pl.pallas_call(
        body,
        out_shape=[jax.ShapeDtypeStruct(shape, dtype) for shape, dtype in outs],
        in_specs=in_specs,
        out_specs=out_specs,
        scratch_shapes=list(scratch),
        compiler_params=pltpu.CompilerParams(vmem_limit_bytes=vmem_mb << 20),
        cost_estimate=pl.CostEstimate(
            flops=int(flops), bytes_accessed=int(bytes_accessed), transcendentals=0
        ),
        name=name,
    )(*ins)


def rows_at(step, tile=ROW_TILE):
    return pl.ds(pl.multiple_of(step * tile, tile), tile)


def pair_masks():
    lane = lax.broadcasted_iota(jnp.int32, (1, 2 * HEAD_DIM), 1)
    low = (lane < HEAD_DIM).astype(F32).astype(BF16)
    high = (lane >= HEAD_DIM).astype(F32).astype(BF16)
    return low, high


def stacked(pair, masks):
    return jnp.concatenate([pair * masks[0], pair * masks[1]], 0)


TAIL = 16


def piece_groups(wq, wk, wv, wo, up, down, conv):
    width, half = wq.shape
    units = up.shape[1]
    groups = [[(ref, 0, width, 0) for ref in (wq, wk, wv)] + [(wo, 0, half, j * half) for j in range(2)]]
    for first in (0, units // 2):
        groups.append(
            [(up, 0, width, first + j * half) for j in range(units // 2 // half)]
            + [(down, first, units // 2, j * half) for j in range(2)]
        )
    groups.append([(conv, 0, conv.shape[0], 0)])
    return groups


class Place:
    def __init__(self):
        self.fast = lax.axis_size("dp") == 16
        index = lax.axis_index("dp")
        self.index, self.side = index, lax.axis_index("tensor")
        self.core, self.y, self.z = index & 1, (index >> 1) & 1, index >> 2
        self.low = jnp.where(self.core == 0, self.y, self.z & 1)
        self.piece = self.core * 2 + self.low

    def parts(self):
        if not self.fast:
            return list(range(PARTS))
        other_low = jnp.where(self.core == 0, self.z & 1, self.y)
        other = (1 - self.core) * 2 + other_low
        return [self.piece, self.piece ^ 1, other, other ^ 1]

    def position(self, block, half):
        if not self.fast:
            return block
        y_flip = ((block >> 1) & 1) ^ self.y
        z_flip = (block >> 2) ^ self.z
        high = half * 8 + y_flip * 4 if block % 2 == 0 else y_flip * 8 + half * 4
        return high + (z_flip & 1) * 2 + (z_flip >> 1)


def store_blocks(place, blocks, keep_ref, send_ref, columns):
    def store(swap):
        for block, half, values in blocks:
            away = (block % 2) ^ swap if place.fast else half
            (send_ref if away else keep_ref)[place.position(block, half), :, columns] = values

    if place.fast:
        for core in range(2):
            pl.when(place.core == core)(functools.partial(store, core))
    else:
        store(0)


def place_parts(part_refs, counts, targets, sems):
    table = Place().parts()
    copies = []
    slot = 0
    place = 0
    for ref, count in zip(part_refs, counts):
        for item in range(count):
            where = table[place]
            place += 1
            for start, rows, target, columns in targets:
                copies.append(
                    pltpu.make_async_copy(
                        ref.at[item, pl.ds(start, rows), :],
                        target.at[pl.ds(pl.multiple_of(where * rows, 16), rows), columns],
                        sems.at[slot],
                    )
                )
                slot += 1
    return copies


def pick_pieces(characters, matrices, wide_vectors, narrow_vectors):
    length, width = characters.shape
    span = length // 2
    half = matrices[0].shape[1]
    nm, vectors = len(matrices), (*wide_vectors, *narrow_vectors)
    nv, nw = len(vectors), len(wide_vectors)

    def body(*refs):
        chars, matrix_refs, vector_refs = refs[0], refs[1 : 1 + nm], refs[1 + nm : 1 + nm + nv]
        x_ref, pa, pb, pc, pd, tail, wide, narrow = refs[1 + nm + nv : 9 + nm + nv]
        flat, sems = refs[9 + nm + nv : -1], refs[-1]
        wq, wk, wv, wo, up, down, conv = matrix_refs
        place = Place()
        copies = []

        def copy(source, target):
            made = pltpu.make_async_copy(source, target, sems.at[len(copies)])
            made.start()
            copies.append(made)

        for source, target in zip(vector_refs, flat):
            copy(source, target)
        for out, groups in zip((pa, pb, pc, pd), piece_groups(wq, wk, wv, wo, up, down, conv)):
            start = 0
            for ref, first, count, column in groups:
                rows = count // PARTS
                source = ref.at[
                    pl.ds(pl.multiple_of(first + place.piece * rows, 16), rows), pl.ds(column, half)
                ]
                copy(source, out.at[0, pl.ds(start, rows), :])
                start += rows
        copy(chars.at[pl.ds(pl.multiple_of(place.side * span, 16), span), :], x_ref)
        for made in copies[:nv]:
            made.wait()
        for out, some in ((wide, flat[:nw]), (narrow, flat[nw:])):
            out[...] = jnp.concatenate([ref[...].astype(F32).reshape(1, -1) for ref in some], 1)
        count = narrow.shape[1] // half
        rows = [narrow[:, i * half : (i + 1) * half] for i in range(count)]
        rows = jnp.concatenate(rows + [jnp.zeros((TAIL - count, half), F32)], 0).astype(BF16)
        tail[0] = rows
        pa[0, pa.shape[1] - TAIL :, :] = rows
        for made in copies[nv:]:
            made.wait()

    sizes = [v.shape[0] for v in vectors]
    outs = [((span, width), BF16), ((1, width + TAIL, half), BF16)] + [((1, width, half), BF16)] * 3
    outs += [((1, TAIL, half), BF16), ((1, sum(sizes[:nw])), F32), ((1, sum(sizes[nw:])), F32)]
    spaces = {("in", i): pltpu.HBM for i in range(1 + nm + nv)}
    scratch = [pltpu.VMEM((size,), BF16) for size in sizes] + [pltpu.SemaphoreType.DMA((40,))]
    return call(body, outs, (characters, *matrices, *vectors), scratch, 56, 0, 4e6, "pick_pieces", spaces)


def attention_forward(attn_in, wq, wk, wv, qb, vb, rows, kept, masks):
    queries = (times(attn_in, wq[...]) + qb).astype(BF16)
    keys = times(attn_in, wk[...]).astype(BF16)
    values = (times(attn_in, wv[...]) + vb).astype(BF16)
    half = queries.shape[1]
    kept[rows, 0:half] = queries
    kept[rows, half : 2 * half] = keys
    kept[rows, 2 * half : 3 * half] = values
    pairs = half // (2 * HEAD_DIM)
    for block in range(attn_in.shape[0] // BLOCK):
        chars = slice(block * BLOCK, (block + 1) * BLOCK)
        here = pl.ds(rows.start + block * BLOCK, BLOCK)
        for pair in range(pairs):
            lanes = slice(pair * 2 * HEAD_DIM, (pair + 1) * 2 * HEAD_DIM)
            scores = times_t(queries[chars, lanes], stacked(keys[chars, lanes], masks))
            scores = scores * HEAD_DIM ** (-0.5)
            probs = []
            for head in range(2):
                part = scores[:, head * BLOCK : (head + 1) * BLOCK]
                expo = jnp.exp(part - jnp.max(part, -1, keepdims=True))
                probs.append(expo * (1.0 / jnp.sum(expo, -1, keepdims=True)))
            both = jnp.concatenate(probs, 1).astype(BF16)
            kept[here, 4 * half + pair * 2 * BLOCK : 4 * half + (pair + 1) * 2 * BLOCK] = both
            kept[here, 3 * half + pair * 2 * HEAD_DIM : 3 * half + (pair + 1) * 2 * HEAD_DIM] = times(both, stacked(values[chars, lanes], masks)).astype(BF16)


def own_attention(x, wide, narrow, wq, wk, wv):
    span, width = x.shape
    half = wq.shape[1]

    def body(x_ref, wide, narrow, wq, wk, wv, a_ref, kept):
        masks = pair_masks()
        g, s = vector_row(wide, 0, width), vector_row(wide, 1, width)
        qb, vb = vector_row(narrow, 0, half), vector_row(narrow, 1, half)

        def step(i, carry):
            rows = rows_at(i)
            hat, _ = norm_stats(x_ref[rows, :].astype(F32))
            attn_in = (hat * g + s).astype(BF16)
            a_ref[rows, :] = attn_in
            attention_forward(attn_in, wq, wk, wv, qb, vb, rows, kept, masks)
            return carry

        lax.fori_loop(0, span // ROW_TILE, step, 0)

    outs = [((span, width), BF16), ((span, 4 * half + half // HEAD_DIM * BLOCK), BF16)]
    return call(body, outs, (x, wide, narrow, wq, wk, wv), vmem_mb=5,
                flops=2 * span * width * half * 3.5, bytes_accessed=8e6, name="own_attention")


def other_attention(a, parts, tail, half):
    span, width = a.shape
    counts = [part.shape[0] for part in parts]
    n = len(parts)
    last = tail.shape[1]

    def body(a_ref, tail_ref, *refs):
        part_refs = refs[:n]
        wqkv, wo, kept, narrow, sems = refs[n:]
        masks = pair_masks()
        rows_q = width // PARTS
        rows_o = half // PARTS
        targets = [(i * rows_q, rows_q, wqkv, pl.ds(i * half, half)) for i in range(3)]
        targets += [(3 * rows_q + i * rows_o, rows_o, wo, pl.ds(i * half, half)) for i in range(2)]
        copies = place_parts(part_refs, counts, targets, sems)
        for copy in copies:
            copy.start()
        rows = tail_ref[0, last - TAIL :, :].astype(F32)
        narrow[...] = jnp.concatenate([rows[i : i + 1, :] for i in range(narrow.shape[1] // half)], 1)
        qb, vb = vector_row(narrow, 0, half), vector_row(narrow, 1, half)
        for copy in copies:
            copy.wait()
        weights = [wqkv.at[:, pl.ds(i * half, half)] for i in range(3)]

        def step(i, carry):
            rows = rows_at(i)
            attention_forward(a_ref[rows, :], *weights, qb, vb, rows, kept, masks)
            return carry

        lax.fori_loop(0, span // ROW_TILE, step, 0)

    outs = [((width, 3 * half), BF16), ((half, width), BF16), ((span, 4 * half + half // HEAD_DIM * BLOCK), BF16)]
    outs += [((1, 9 * half), F32)]
    return call(body, outs, (a, tail, *parts), [pltpu.SemaphoreType.DMA((PARTS * 5,))], 5,
                2 * span * width * half * 3.5, 9e6, "other_attention")


def attention_output(x, kept_own, kept_other, wo_own, wo_other, wide):
    span, width = x.shape
    half = width // 2

    def body(x_ref, ko, kt, wo, wt, wide, h_ref, c_ref):
        b, g, s = [vector_row(wide, i, width) for i in (2, 3, 4)]
        ctx = slice(3 * half, 4 * half)

        def step(i, carry):
            rows = rows_at(i)
            middle = x_ref[rows, :].astype(F32) + b + times(ko[rows, ctx], wo[...]) + times(kt[rows, ctx], wt[...])
            h_ref[rows, :] = middle
            hat, _ = norm_stats(middle)
            c_ref[rows, :] = (hat * g + s).astype(BF16)
            return carry

        lax.fori_loop(0, span // ROW_TILE, step, 0)

    outs = [((span, width), F32), ((span, width), BF16)]
    return call(body, outs, (x, kept_own, kept_other, wo_own, wo_other, wide), vmem_mb=4,
                flops=2 * span * width * width, bytes_accessed=9e6, name="attention_output")


HIDDEN_TILE = 384


def feed_forward_half(c_ref, acc_ref, up, narrow, start, down, hid_ref, slope_ref, ub):
    span = c_ref.shape[0]
    units = up.shape[1]
    ub[...] = narrow[:, start : start + units]

    def step(j, carry):
        cols = rows_at(j, HIDDEN_TILE)
        for i in range(span // ROW_TILE):
            rows = slice(i * ROW_TILE, (i + 1) * ROW_TILE)
            upper = times(c_ref[rows, :], up[:, cols]) + ub[:, cols]
            hidden, slope = gelu_parts(upper)
            hidden = hidden.astype(BF16)
            hid_ref[rows, cols] = hidden
            slope_ref[rows, cols] = slope.astype(BF16)
            acc_ref[rows, :] += times(hidden, down[cols, :])
        return carry

    lax.fori_loop(0, units // HIDDEN_TILE, step, 0)


def own_feed_forward(c, middle, wide, narrow, up, down):
    span, width = c.shape
    units = up.shape[1]

    def body(c_ref, m_ref, wide, narrow, up, down, hid_ref, slope_ref, acc_ref, ub):
        acc_ref[...] = m_ref[...] + vector_row(wide, 5, width)
        feed_forward_half(c_ref, acc_ref, up, narrow, narrow.shape[1] - units, down, hid_ref, slope_ref, ub)

    outs = [((span, units), BF16)] * 2 + [((span, width), F32)]
    return call(body, outs, (c, middle, wide, narrow, up, down), [pltpu.VMEM((1, units), F32)], vmem_mb=4,
                flops=4 * span * width * units, bytes_accessed=16e6, name="own_feed_forward")


def other_feed_forward(c, acc, narrow, units, start, parts, name):
    span, width = c.shape
    half = width // 2
    counts = [part.shape[0] for part in parts]
    n = len(parts)

    def body(c_ref, a_ref, narrow, *refs):
        up, down, hid_ref, slope_ref, acc_ref, sems, ub = refs[n:]
        rows_u, rows_d = width // PARTS, units // PARTS
        targets = [(j * rows_u, rows_u, up, pl.ds(j * half, half)) for j in range(units // half)]
        first = len(targets) * rows_u
        targets += [(first + j * rows_d, rows_d, down, pl.ds(j * half, half)) for j in range(width // half)]
        copies = place_parts(refs[:n], counts, targets, sems)
        for copy in copies:
            copy.start()
        acc_ref[...] = a_ref[...]
        for copy in copies:
            copy.wait()
        feed_forward_half(c_ref, acc_ref, up, narrow, start, down, hid_ref, slope_ref, ub)

    outs = [((width, units), BF16), ((units, width), BF16)] + [((span, units), BF16)] * 2 + [((span, width), F32)]
    scratch = [pltpu.SemaphoreType.DMA((PARTS * 4,)), pltpu.VMEM((1, units), F32)]
    return call(body, outs, (c, acc, narrow, *parts), scratch, 4, 4 * span * width * units, 9e6, name)


def downsample(h2, wc_own, wc_parts, narrow, narrow_other, cot):
    span, width = h2.shape
    half = width // 2
    mols = span // STRIDE
    counts = [part.shape[0] for part in wc_parts]
    n = len(wc_parts)

    def body(h_ref, wo, narrow, narrow_other, cot_ref, *refs):
        part_refs = refs[:n]
        hs_ref, dc_ref, mol_own, mol_other, dh_ref, dh16_ref, vec_ref, wt, strip, sems = refs[n:]
        left = lax.axis_index("tensor") == 0
        b, g, s = (
            jnp.concatenate([vector_row(ref, i, half) for ref in (narrow, narrow_other)], 1) for i in (2, 3, 4)
        )
        copies = place_parts(part_refs, counts, [(0, STRIDE * width // PARTS, wt, slice(None))], sems)
        for copy in copies:
            copy.start()
        pre_own = jnp.zeros((mols, half), F32)
        for lane in range(width // 128):
            strip[lane] = h_ref[:, lane * 128 : (lane + 1) * 128]
        for tap in range(STRIDE):
            window = jnp.concatenate(
                [strip[lane, pl.ds(tap, mols, stride=STRIDE), :] for lane in range(width // 128)], 1
            ).astype(BF16)
            hs_ref[tap * mols : (tap + 1) * mols, :] = window
            pre_own += times(window, wo[tap * width : (tap + 1) * width, :])
        for copy in copies:
            copy.wait()
        pre_other = jnp.zeros((mols, half), F32)
        for tap in range(STRIDE):
            window = hs_ref[tap * mols : (tap + 1) * mols, :]
            pre_other += times(window, wt[tap * width : (tap + 1) * width, :])
        conv = jnp.concatenate([pre_own, pre_other], 1) + b
        act, slope = gelu_parts(conv)
        hat, inv = norm_stats(act)
        whole = cot_ref[...].astype(F32)
        after = whole[mols + 1 :, :]
        after = jnp.concatenate([after, jnp.zeros((1, width), F32)], 0)
        after = jnp.concatenate([after[:, half:], after[:, :half]], 1)
        cotangent = jnp.where(left, whole[1 : mols + 1, :], after)
        dpre = norm_back(cotangent * g, hat, inv)
        dconv = dpre * slope
        dconv16 = dconv.astype(BF16)
        dc_ref[...] = dconv16
        hat0, inv0 = norm_stats(h_ref[0:8, :])
        only = (lax.broadcasted_iota(jnp.int32, (8, width), 0) == 0) & left
        cot0 = jnp.where(only, whole[0:8, :], 0.0)
        dpre0 = norm_back(cot0 * g, hat0, inv0)
        mol = jnp.concatenate([(hat0 * g + s)[0:1], hat * g + s, jnp.zeros((15, width), F32)], 0).astype(BF16)
        mol_own[...] = mol[:, :half]
        mol_other[...] = mol[:, half:]
        vec_ref[...] = jnp.zeros_like(vec_ref)
        vec_ref[0:1, :] = column_sum(cotangent * hat) + column_sum(cot0 * hat0)
        vec_ref[1:2, :] = column_sum(cotangent) + column_sum(cot0)
        vec_ref[2:3, :] = column_sum(dconv)
        for tap in range(STRIDE):
            taps = slice(tap * width, (tap + 1) * width)
            back = times_t(dconv16[:, :half], wo[taps, :]) + times_t(dconv16[:, half:], wt[taps, :])
            for lane in range(width // 128):
                strip[lane, pl.ds(tap, mols, stride=STRIDE), :] = back[:, lane * 128 : (lane + 1) * 128]
        for lane in range(width // 128):
            dh_ref[:, lane * 128 : (lane + 1) * 128] = strip[lane]
        dh_ref[0:8, :] += dpre0
        total = jnp.zeros((1, width), F32)
        for i in range(span // ROW_TILE):
            rows = slice(i * ROW_TILE, (i + 1) * ROW_TILE)
            grad = dh_ref[rows, :]
            dh16_ref[rows, :] = grad.astype(BF16)
            total += column_sum(grad)
        vec_ref[3:4, :] = total

    outs = [((span, width), BF16), ((mols, width), BF16), ((mols + 16, half), BF16), ((mols + 16, half), BF16),
            ((span, width), F32), ((span, width), BF16), ((8, width), F32)]
    spaces = None
    scratch = [pltpu.VMEM((STRIDE * width, half), BF16), pltpu.VMEM((width // 128, span, 128), F32), pltpu.SemaphoreType.DMA((PARTS,))]
    return call(body, outs, (h2, wc_own, narrow, narrow_other, cot, *wc_parts), scratch, 10,
                8 * span * width * width / 2, 16e6, "downsample", spaces)


def conv_weight_grad(hs, dconv16):
    span, width = hs.shape
    half = width // 2
    mols = span // STRIDE
    rows = STRIDE * width // 16

    def body(hs_ref, dc_ref, keep_ref, send_ref):
        place = Place()
        for tap in range(STRIDE):
            grad = t_times(hs_ref[tap * mols : (tap + 1) * mols, :], dc_ref[...]).astype(BF16)
            blocks = [
                (tap * 4 + i, group, grad[i * rows : (i + 1) * rows, group * half : (group + 1) * half])
                for i in range(4)
                for group in range(2)
            ]
            store_blocks(place, blocks, keep_ref, send_ref, slice(None))

    outs = [((16, rows, half), BF16)] * 2
    return call(body, outs, (hs, dconv16), (), 8, 2 * span * width * width, 7e6, "conv_weight_grad")


GRAD_TILE = 384


def weight_grad(lefts, rights, name):
    span, width = lefts[0].shape
    units = sum(item[3] for item in rights[0])
    rows = width // 16
    flat = [item[1] for group in rights for item in group]
    nl, nr = len(lefts), len(flat)

    def body(*refs):
        left_refs, right_refs = refs[:nl], refs[nl : nl + nr]
        keep_ref, send_ref, turned = refs[nl + nr :]
        place = Place()
        for i, ref in enumerate(left_refs):
            turned[i] = ref[...].T
        at = 0
        for group_index, group in enumerate(rights):
            column = 0
            for which, _, first, count in group:
                ref = right_refs[at]
                at += 1
                tile = min(HIDDEN_TILE, count)

                def step(j, carry, ref=ref, which=which, group_index=group_index, column=column, first=first):
                    cols = pl.ds(pl.multiple_of(first + j * tile, 128), tile)
                    target = pl.ds(pl.multiple_of(column + j * tile, 128), tile)
                    blocks = []
                    for i in range(width // GRAD_TILE):
                        grad = times(turned[which, i * GRAD_TILE : (i + 1) * GRAD_TILE, :], ref[:, cols]).astype(BF16)
                        per = GRAD_TILE // rows
                        blocks += [(i * per + k, group_index, grad[k * rows : (k + 1) * rows]) for k in range(per)]
                    store_blocks(place, blocks, keep_ref, send_ref, target)
                    return carry

                lax.fori_loop(0, count // tile, step, 0)
                column += count

    outs = [((16, rows, units), BF16)] * 2
    return call(body, outs, (*lefts, *flat), [pltpu.VMEM((nl, width, span), BF16)], 8,
                4 * span * width * units, 12e6, name)


def feed_forward_backward(dh2, dh2_16, middle, wide, slopes, ups, downs):
    span, width = dh2.shape
    n = len(ups)
    sizes = [up.shape[1] for up in ups]

    def body(dh_ref, dh16_ref, m_ref, wide, *refs):
        slope_refs, up_refs, down_refs = refs[:n], refs[n : 2 * n], refs[2 * n : 3 * n]
        du_refs, (dm_ref, dm16_ref, vec_ref), ub_refs = refs[3 * n : 4 * n], refs[4 * n : 4 * n + 3], refs[4 * n + 3 : 5 * n + 3]
        acc_ref = refs[-1]
        acc_ref[...] = jnp.zeros_like(acc_ref)
        g = vector_row(wide, 3, width)
        for slope_ref, up, down, du_ref, ub_ref in zip(slope_refs, up_refs, down_refs, du_refs, ub_refs):
            def step(j, carry, slope_ref=slope_ref, up=up, down=down, du_ref=du_ref, ub_ref=ub_ref):
                cols = rows_at(j, HIDDEN_TILE)
                total = jnp.zeros((1, HIDDEN_TILE), F32)
                for i in range(span // ROW_TILE):
                    rows = slice(i * ROW_TILE, (i + 1) * ROW_TILE)
                    grad = times_t(dh16_ref[rows, :], down[cols, :]) * slope_ref[rows, cols].astype(F32)
                    total += column_sum(grad)
                    grad16 = grad.astype(BF16)
                    du_ref[rows, cols] = grad16
                    acc_ref[rows, :] += times_t(grad16, up[:, cols])
                ub_ref[:, cols] = total
                return carry

            lax.fori_loop(0, up.shape[1] // HIDDEN_TILE, step, 0)
        vec_ref[...] = jnp.zeros_like(vec_ref)

        def close(i, carry):
            rows = rows_at(i)
            back = acc_ref[rows, :]
            hat, inv = norm_stats(m_ref[rows, :])
            grad = dh_ref[rows, :] + norm_back(back * g, hat, inv)
            dm_ref[rows, :] = grad
            dm16_ref[rows, :] = grad.astype(BF16)
            vec_ref[0:1, :] += column_sum(back * hat)
            vec_ref[1:2, :] += column_sum(back)
            vec_ref[2:3, :] += column_sum(grad)
            return carry

        lax.fori_loop(0, span // ROW_TILE, close, 0)

    outs = [((span, size), BF16) for size in sizes] + [((span, width), F32), ((span, width), BF16), ((8, width), F32)]
    outs += [((1, size), F32) for size in sizes]
    return call(body, outs, (dh2, dh2_16, middle, wide, *slopes, *ups, *downs), [pltpu.VMEM((span, width), F32)], 22,
                8 * span * width * sum(sizes) / 2, 30e6, "feed_forward_backward")


def attention_backward(dm16, wo, kept, name):
    span, width = dm16.shape
    half = width // 2

    def body(dm_ref, wo, kept, grads, vec_ref):
        masks = pair_masks()
        lane = lax.broadcasted_iota(jnp.int32, (1, 2 * HEAD_DIM), 1) < HEAD_DIM
        vec_ref[...] = jnp.zeros_like(vec_ref)

        def step(i, carry):
            rows = rows_at(i)
            dctx = times_t(dm_ref[rows, :], wo[...]).astype(BF16)
            for block in range(ROW_TILE // BLOCK):
                chars = slice(block * BLOCK, (block + 1) * BLOCK)
                here = pl.ds(rows.start + block * BLOCK, BLOCK)
                for pair in range(half // (2 * HEAD_DIM)):
                    first = pair * 2 * HEAD_DIM
                    q, k, v = [kept[here, i * half + first : i * half + first + 2 * HEAD_DIM] for i in range(3)]
                    p = kept[here, 4 * half + pair * 2 * BLOCK : 4 * half + (pair + 1) * 2 * BLOCK]
                    grad = dctx[chars, first : first + 2 * HEAD_DIM]
                    dv2 = t_times(p, grad)
                    dv = jnp.where(lane, dv2[:BLOCK], dv2[BLOCK:])
                    dp = times_t(grad, stacked(v, masks))
                    p32 = p.astype(F32)
                    ds = []
                    for head in range(2):
                        part = slice(head * BLOCK, (head + 1) * BLOCK)
                        weighted = p32[:, part] * dp[:, part]
                        inner = jnp.sum(weighted, -1, keepdims=True)
                        ds.append((weighted - p32[:, part] * inner) * HEAD_DIM ** (-0.5))
                    ds = jnp.concatenate(ds, 1).astype(BF16)
                    dq = times(ds, stacked(k, masks))
                    dk2 = t_times(ds, q)
                    dk = jnp.where(lane, dk2[:BLOCK], dk2[BLOCK:])
                    for i, value in enumerate((dq, dk, dv)):
                        grads[here, i * half + first : i * half + first + 2 * HEAD_DIM] = value.astype(BF16)
                    lanes = slice(first, first + 2 * HEAD_DIM)
                    vec_ref[0:1, lanes] += column_sum(dq)
                    vec_ref[1:2, lanes] += column_sum(dv)
            return carry

        lax.fori_loop(0, span // ROW_TILE, step, 0)

    outs = [((span, 3 * half), BF16), ((8, half), F32)]
    return call(body, outs, (dm16, wo, kept), vmem_mb=4,
                flops=2 * span * width * half * 2, bytes_accessed=8e6, name=name)


def input_backward(dm, x, wide, grads_own, grads_other, own_weights, other_weight):
    span, width = dm.shape
    half = width // 2

    def body(dm_ref, x_ref, wide, go, gt, wq, wk, wv, wt, out_ref, vec_ref):
        g = vector_row(wide, 0, width)
        vec_ref[...] = jnp.zeros_like(vec_ref)

        def step(i, carry):
            rows = rows_at(i)
            back = times_t(gt[rows, :], wt[...])
            for i, ref in enumerate((wq, wk, wv)):
                back += times_t(go[rows, i * half : (i + 1) * half], ref[...])
            hat, inv = norm_stats(x_ref[rows, :].astype(F32))
            out_ref[rows, :] = dm_ref[rows, :] + norm_back(back * g, hat, inv)
            vec_ref[0:1, :] += column_sum(back * hat)
            vec_ref[1:2, :] += column_sum(back)
            return carry

        lax.fori_loop(0, span // ROW_TILE, step, 0)

    outs = [((span, width), F32), ((8, width), F32)]
    return call(body, outs, (dm, x, wide, grads_own, grads_other, *own_weights, other_weight), vmem_mb=9,
                flops=2 * span * width * 3 * width, bytes_accessed=12e6, name="input_backward")


def flat_permute(value, route, dp_size):
    pairs = []
    for d in range(dp_size):
        for t in range(2):
            d2, t2 = route(d, t)
            pairs.append((d * 2 + t, d2 * 2 + t2))
    return lax.ppermute(value, ("dp", "tensor"), pairs)


def over_x(d, t):
    return d, 1 - t


def over_core(d, t):
    return d ^ 1, t


def over_y(d, t):
    return d ^ 2, t


def over_z_near(d, t):
    return d ^ 4, t


def over_z_far(d, t):
    return d ^ 8, t


def by_core(first, second):
    return lambda d, t: (second if d & 1 else first)(d, t)


class Order:
    def __init__(self):
        self.last = None

    def __call__(self, step, *args):
        if self.last is not None:
            args = lax.optimization_barrier((args, self.last))[0]
        self.last = step(*args)
        return self.last


def split_sum(keep, got):
    size = keep.shape[0] // 2
    total = [(keep[at : at + size].astype(F32) + got[at : at + size].astype(F32)).astype(BF16) for at in (0, size)]
    return tuple(total)


class Reduction:
    def __init__(self, grid, order, blocks):
        self.grid, self.order = grid, order
        self.keep = blocks[0]
        self.stage = 0
        if grid.fast:
            self.got = grid.send(blocks[1], over_core)
        else:
            self.got = grid.send(blocks[1], over_x)

    def step(self):
        if not self.grid.fast:
            return
        route = (by_core(over_x, over_y), by_core(over_y, over_x), over_z_near, over_z_far)[self.stage]
        self.keep, out = self.order(split_sum, self.keep, self.got)
        self.got = self.grid.send(out, route)
        self.stage += 1

    def finish(self):
        if not self.grid.fast:
            total = self.keep.astype(F32) + self.got.astype(F32)
            total = total.reshape(-1, total.shape[-1])
            return lax.psum_scatter(total, "dp", scatter_dimension=0, tiled=True)
        return self.order(lambda keep, got: (keep.astype(F32) + got.astype(F32))[0], self.keep, self.got)


class Grid:
    def __init__(self):
        self.dp = lax.axis_size("dp")
        self.index = lax.axis_index("dp")
        self.side = lax.axis_index("tensor")
        self.fast = self.dp == 16

    def send(self, value, route):
        return flat_permute(value, route, self.dp)

    def gather(self, piece, ready=lambda value: value):
        if not self.fast:
            return [self.send(piece, over_x)]
        first = self.send(piece, over_x)
        first = ready(first)
        second = self.send(first, by_core(over_y, over_z_near))
        return [first, second, self.send(first, over_core), self.send(second, over_core)]

    def reduce_vectors(self, shared, own, other):
        rows = shared.shape[0]
        got = self.send(jnp.concatenate([shared, other], 0), over_x)
        total = jnp.concatenate([shared, own], 0) + got
        if not self.fast:
            total = lax.psum(total, "dp")
        else:
            for route in (over_core, over_y, over_z_near, over_z_far):
                total = total + self.send(total, route)
        return total[:rows], total[rows:]


def per_device(
    characters, first_gain, first_shift, query_weight, query_bias, key_weight, value_weight, value_bias,
    out_weight, out_bias, second_gain, second_shift, up_weight, up_bias, down_weight, down_bias,
    conv_weight, conv_bias, third_gain, third_shift, cotangent,
):
    _, length, width = characters.shape
    span = length // 2
    half = width // 2
    units = up_weight.shape[1]
    mols = span // STRIDE
    grid = Grid()
    side = grid.side

    order = Order()
    matrices = (query_weight, key_weight, value_weight, out_weight, up_weight, down_weight, conv_weight)
    x, *pieces, tail, wide, narrow = pick_pieces(
        characters[0],
        matrices,
        (first_gain, first_shift, out_bias, second_gain, second_shift, down_bias),
        (query_bias, value_bias, conv_bias, third_gain, third_shift, up_bias),
    )
    if not grid.fast:
        pieces = [
            jnp.concatenate(
                [
                    ref[first : first + count, column : column + half].reshape(PARTS, count // PARTS, half)
                    for ref, first, count, column in group
                ],
                1,
            )
            for group in piece_groups(*matrices)
        ]

    a, kept_own = own_attention(x, wide, narrow, query_weight, key_weight, value_weight)
    attention_parts = grid.gather(pieces[0], lambda value: lax.optimization_barrier((value, a))[0])
    first_parts, second_parts, conv_parts = [grid.gather(piece) for piece in pieces[1:]]
    tail = attention_parts[0] if grid.fast else grid.send(tail, over_x)
    wqkv_other, wo_other, kept_other, narrow_other = other_attention(a, attention_parts, tail, half)
    middle, c = attention_output(x, kept_own, kept_other, out_weight, wo_other, wide)
    hid_own, slope_own, acc = own_feed_forward(c, middle, wide, narrow, up_weight, down_weight)
    ups, downs, hids, slopes = [up_weight], [down_weight], [hid_own], [slope_own]
    for i, parts in enumerate((first_parts, second_parts)):
        start = narrow.shape[1] - units + i * units // 2
        up, down, hid, slope, acc = other_feed_forward(
            c, acc, narrow_other, units // 2, start, parts, f"other_feed_forward_{i}"
        )
        for some, value in zip((ups, downs, hids, slopes), (up, down, hid, slope)):
            some.append(value)

    hs, dconv16, mol_own, mol_other, dh2, dh2_16, conv_vec = order(
        lambda *args: downsample(*args[:2], args[4:], *args[2:4], cotangent[0]),
        acc, conv_weight, narrow, narrow_other, *conv_parts,
    )
    theirs = grid.send(mol_other, over_x)

    def whole(which, array):
        return (which, array, 0, array.shape[1])

    conv_sum = Reduction(grid, order, order(conv_weight_grad, hs, dconv16))
    down_sum = Reduction(
        grid,
        order,
        order(
            lambda left, own, *others: weight_grad(
                (left,), [[whole(0, own)], [whole(0, v) for v in others]], "down_weight_grad"
            ),
            dh2_16, *hids,
        ),
    )
    conv_sum.step()
    du_own, du_first, du_second, dm, dm16, ffn_vec, *up_vecs = order(
        lambda *args: feed_forward_backward(*args[:4], args[4:7], args[7:10], args[10:]),
        dh2, dh2_16, middle, wide, *slopes, *ups, *downs,
    )
    down_sum.step()
    conv_sum.step()
    up_sum = Reduction(
        grid,
        order,
        order(
            lambda c, dm16, own, first, second, kept_own, kept_other: weight_grad(
                (c, dm16),
                [
                    [whole(0, own), (1, kept_own, 3 * half, half)],
                    [whole(0, first), whole(0, second), (1, kept_other, 3 * half, half)],
                ],
                "up_weight_grad",
            ),
            c, dm16, du_own, du_first, du_second, kept_own, kept_other,
        ),
    )
    dqkv_own, vec_own = order(
        functools.partial(attention_backward, name="own_attention_backward"), dm16, out_weight, kept_own
    )
    up_sum.step()
    conv_sum.step()
    dqkv_other, vec_other = order(
        functools.partial(attention_backward, name="other_attention_backward"), dm16, wo_other, kept_other
    )
    down_sum.step()
    conv_sum.step()
    attention_sum = Reduction(
        grid,
        order,
        order(
            lambda a, own, other: weight_grad((a,), [[whole(0, own)], [whole(0, other)]], "attention_weight_grad"),
            a, dqkv_own, dqkv_other,
        ),
    )
    down_sum.step()
    up_sum.step()
    input_rows, in_vec = order(
        lambda *args: input_backward(*args[:5], args[5:8], args[8]),
        dm, x, wide, dqkv_own, dqkv_other, query_weight, key_weight, value_weight, wqkv_other,
    )
    attention_sum.step()
    sum_conv_weight = conv_sum.finish()
    down_sum.step()
    up_sum.step()
    sum_down = down_sum.finish()
    attention_sum.step()
    up_sum.step()
    attention_sum.step()
    sum_up = up_sum.finish()
    attention_sum.step()
    sum_attention = attention_sum.finish()

    mine, theirs = mol_own[: mols + 1], theirs[: mols + 1]
    upper = jnp.where(side == 0, mine, theirs)
    lower = jnp.where(side == 0, theirs, mine)
    molecules = jnp.concatenate([upper, lower[1:mols]], 0)[None]

    shared = jnp.concatenate([conv_vec[3:4], ffn_vec[0:3], in_vec[0:2]], 0).reshape(-1, half)
    own = jnp.concatenate([conv_vec[0:3, :half], vec_own[0:2], up_vecs[0].reshape(-1, half)], 0)
    other = jnp.concatenate([conv_vec[0:3, half:], vec_other[0:2]] + [v.reshape(-1, half) for v in up_vecs[1:]], 0)
    shared, own = grid.reduce_vectors(shared, own, other)
    shared = shared.reshape(-1, width)
    block = width // grid.dp
    shared = lax.dynamic_slice_in_dim(shared, grid.index * block, block, 1)
    return (
        molecules,
        input_rows[None],
        shared[4],
        shared[5],
        sum_attention[:, :half],
        own[3],
        sum_attention[:, half : 2 * half],
        sum_attention[:, 2 * half : 3 * half],
        own[4],
        sum_up[:, units:].T,
        shared[3],
        shared[1],
        shared[2],
        sum_up[:, :units],
        own[5:].reshape(-1),
        sum_down.T,
        shared[0],
        sum_conv_weight,
        own[2],
        own[0],
        own[1],
    )


def solution(mesh):
    return jax.shard_map(
        per_device,
        mesh=mesh,
        in_specs=(
            P("dp", None, None),
            P(),
            P(),
            P(None, "tensor"),
            P("tensor"),
            P(None, "tensor"),
            P(None, "tensor"),
            P("tensor"),
            P("tensor", None),
            P(),
            P(),
            P(),
            P(None, "tensor"),
            P("tensor"),
            P("tensor", None),
            P(),
            P(None, "tensor"),
            P("tensor"),
            P("tensor"),
            P("tensor"),
            P("dp", None, None),
        ),
        out_specs=(
            P("dp", None, "tensor"),
            P("dp", "tensor", None),
            P("dp"),
            P("dp"),
            P("dp", "tensor"),
            P("tensor"),
            P("dp", "tensor"),
            P("dp", "tensor"),
            P("tensor"),
            P("tensor", "dp"),
            P("dp"),
            P("dp"),
            P("dp"),
            P("dp", "tensor"),
            P("tensor"),
            P("tensor", "dp"),
            P("dp"),
            P("dp", "tensor"),
            P("tensor"),
            P("tensor"),
            P("tensor"),
        ),
        check_vma=False,
    )
```

```python
import functools

import jax
import jax.numpy as jnp
from jax import lax
from jax.experimental import pallas as pl
from jax.experimental.pallas import tpu as pltpu
from jax.sharding import PartitionSpec as P

HEAD_DIM = 64
BLOCK = 128
STRIDE = 4
EPSILON = 1e-05
INV_ROOT_TWO = 0.7071067811865476
INV_ROOT_TWO_PI = 0.3989422804014327
F32 = jnp.float32
BF16 = jnp.bfloat16
PARTS = 4
ROW_TILE = 256
LONG = 8


def times(left, right):
    return jnp.dot(left, right, preferred_element_type=F32)


def times_t(left, right):
    return lax.dot_general(left, right, (((1,), (1,)), ((), ())), preferred_element_type=F32)


def t_times(left, right):
    return lax.dot_general(left, right, (((0,), (0,)), ((), ())), preferred_element_type=F32)


def gelu_parts(u):
    phi = 0.5 + 0.5 * lax.erf(u * INV_ROOT_TWO)
    return u * phi, phi + u * (jnp.exp(-0.5 * (u * u)) * INV_ROOT_TWO_PI)


def norm_stats(values):
    mean = jnp.mean(values, -1, keepdims=True)
    centered = values - mean
    inv = lax.rsqrt(jnp.mean(centered * centered, -1, keepdims=True) + EPSILON)
    return centered * inv, inv


def norm_back(scaled, hat, inv):
    return inv * (
        scaled
        - jnp.mean(scaled, -1, keepdims=True)
        - hat * jnp.mean(scaled * hat, -1, keepdims=True)
    )


def vector_row(ref, index, width):
    return ref[:, index * width : (index + 1) * width]


def column_sum(values):
    return jnp.sum(values, 0, keepdims=True)


def call(body, outs, ins, scratch=(), vmem_mb=32, flops=0, bytes_accessed=0, name=None, spaces=None, weight=1):
    spaces = spaces or {}
    in_specs = [pl.BlockSpec(memory_space=spaces.get(("in", i), pltpu.VMEM)) for i in range(len(ins))]
    out_specs = [pl.BlockSpec(memory_space=spaces.get(("out", i), pltpu.VMEM)) for i in range(len(outs))]
    return pl.pallas_call(
        body,
        out_shape=[jax.ShapeDtypeStruct(shape, dtype) for shape, dtype in outs],
        in_specs=in_specs,
        out_specs=out_specs,
        scratch_shapes=list(scratch),
        compiler_params=pltpu.CompilerParams(vmem_limit_bytes=vmem_mb << 20),
        cost_estimate=pl.CostEstimate(
            flops=int(flops * weight), bytes_accessed=int(bytes_accessed * weight), transcendentals=0
        ),
        name=name,
    )(*ins)


def rows_at(step, tile=ROW_TILE):
    return pl.ds(pl.multiple_of(step * tile, tile), tile)


def pair_masks():
    lane = lax.broadcasted_iota(jnp.int32, (1, 2 * HEAD_DIM), 1)
    low = (lane < HEAD_DIM).astype(F32).astype(BF16)
    high = (lane >= HEAD_DIM).astype(F32).astype(BF16)
    return low, high


def stacked(pair, masks):
    return jnp.concatenate([pair * masks[0], pair * masks[1]], 0)


TAIL = 16


def piece_groups(wq, wk, wv, wo, up, down, conv):
    width, half = wq.shape
    units = up.shape[1]
    groups = [[(ref, 0, width, 0) for ref in (wq, wk, wv)] + [(wo, 0, half, j * half) for j in range(2)]]
    for first in (0, units // 2):
        groups.append(
            [(up, 0, width, first + j * half) for j in range(units // 2 // half)]
            + [(down, first, units // 2, j * half) for j in range(2)]
        )
    groups.append([(conv, 0, conv.shape[0], 0)])
    return groups


class Place:
    def __init__(self):
        self.fast = lax.axis_size("dp") == 16
        index = lax.axis_index("dp")
        self.index, self.side = index, lax.axis_index("tensor")
        self.core, self.y, self.z = index & 1, (index >> 1) & 1, index >> 2
        self.low = jnp.where(self.core == 0, self.y, self.z & 1)
        self.piece = self.core * 2 + self.low

    def parts(self):
        if not self.fast:
            return list(range(PARTS))
        other_low = jnp.where(self.core == 0, self.z & 1, self.y)
        other = (1 - self.core) * 2 + other_low
        return [self.piece, self.piece ^ 1, other, other ^ 1]

    def position(self, block, half):
        if not self.fast:
            return block
        y_flip = ((block >> 1) & 1) ^ self.y
        z_flip = (block >> 2) ^ self.z
        high = half * 8 + y_flip * 4 if block % 2 == 0 else y_flip * 8 + half * 4
        return high + (z_flip & 1) * 2 + (z_flip >> 1)


def store_blocks(place, blocks, keep_ref, send_ref, columns):
    def store(swap):
        for block, half, values in blocks:
            away = (block % 2) ^ swap if place.fast else half
            (send_ref if away else keep_ref)[place.position(block, half), :, columns] = values

    if place.fast:
        for core in range(2):
            pl.when(place.core == core)(functools.partial(store, core))
    else:
        store(0)


def place_parts(part_refs, counts, targets, sems):
    table = Place().parts()
    copies = []
    slot = 0
    place = 0
    for ref, count in zip(part_refs, counts):
        for item in range(count):
            where = table[place]
            place += 1
            for start, rows, target, columns in targets:
                copies.append(
                    pltpu.make_async_copy(
                        ref.at[item, pl.ds(start, rows), :],
                        target.at[pl.ds(pl.multiple_of(where * rows, 16), rows), columns],
                        sems.at[slot],
                    )
                )
                slot += 1
    return copies


def pick_pieces(characters, matrices, wide_vectors, narrow_vectors):
    length, width = characters.shape
    span = length // 2
    half = matrices[0].shape[1]
    nm, vectors = len(matrices), (*wide_vectors, *narrow_vectors)
    nv, nw = len(vectors), len(wide_vectors)

    def body(*refs):
        chars, matrix_refs, vector_refs = refs[0], refs[1 : 1 + nm], refs[1 + nm : 1 + nm + nv]
        x_ref, pa, pb, pc, pd, tail, wide, narrow = refs[1 + nm + nv : 9 + nm + nv]
        flat, sems = refs[9 + nm + nv : -1], refs[-1]
        wq, wk, wv, wo, up, down, conv = matrix_refs
        place = Place()
        copies = []

        def copy(source, target):
            made = pltpu.make_async_copy(source, target, sems.at[len(copies)])
            made.start()
            copies.append(made)

        for source, target in zip(vector_refs, flat):
            copy(source, target)
        for out, groups in zip((pa, pb, pc, pd), piece_groups(wq, wk, wv, wo, up, down, conv)):
            start = 0
            for ref, first, count, column in groups:
                rows = count // PARTS
                source = ref.at[
                    pl.ds(pl.multiple_of(first + place.piece * rows, 16), rows), pl.ds(column, half)
                ]
                copy(source, out.at[0, pl.ds(start, rows), :])
                start += rows
        copy(chars.at[pl.ds(pl.multiple_of(place.side * span, 16), span), :], x_ref)
        for made in copies[:nv]:
            made.wait()
        for out, some in ((wide, flat[:nw]), (narrow, flat[nw:])):
            out[...] = jnp.concatenate([ref[...].astype(F32).reshape(1, -1) for ref in some], 1)
        count = narrow.shape[1] // half
        rows = [narrow[:, i * half : (i + 1) * half] for i in range(count)]
        rows = jnp.concatenate(rows + [jnp.zeros((TAIL - count, half), F32)], 0).astype(BF16)
        tail[0] = rows
        pa[0, pa.shape[1] - TAIL :, :] = rows
        for made in copies[nv:]:
            made.wait()

    sizes = [v.shape[0] for v in vectors]
    outs = [((span, width), BF16), ((1, width + TAIL, half), BF16)] + [((1, width, half), BF16)] * 3
    outs += [((1, TAIL, half), BF16), ((1, sum(sizes[:nw])), F32), ((1, sum(sizes[nw:])), F32)]
    spaces = {("in", i): pltpu.HBM for i in range(1 + nm + nv)}
    scratch = [pltpu.VMEM((size,), BF16) for size in sizes] + [pltpu.SemaphoreType.DMA((40,))]
    return call(body, outs, (characters, *matrices, *vectors), scratch, 56, 0, 4e6, "pick_pieces", spaces)


def attention_forward(attn_in, wq, wk, wv, qb, vb, rows, kept, masks):
    queries = (times(attn_in, wq[...]) + qb).astype(BF16)
    keys = times(attn_in, wk[...]).astype(BF16)
    values = (times(attn_in, wv[...]) + vb).astype(BF16)
    half = queries.shape[1]
    kept[rows, 0:half] = queries
    kept[rows, half : 2 * half] = keys
    kept[rows, 2 * half : 3 * half] = values
    pairs = half // (2 * HEAD_DIM)
    for block in range(attn_in.shape[0] // BLOCK):
        chars = slice(block * BLOCK, (block + 1) * BLOCK)
        here = pl.ds(rows.start + block * BLOCK, BLOCK)
        for pair in range(pairs):
            lanes = slice(pair * 2 * HEAD_DIM, (pair + 1) * 2 * HEAD_DIM)
            scores = times_t(queries[chars, lanes], stacked(keys[chars, lanes], masks))
            scores = scores * HEAD_DIM ** (-0.5)
            probs = []
            for head in range(2):
                part = scores[:, head * BLOCK : (head + 1) * BLOCK]
                expo = jnp.exp(part - jnp.max(part, -1, keepdims=True))
                probs.append(expo * (1.0 / jnp.sum(expo, -1, keepdims=True)))
            both = jnp.concatenate(probs, 1).astype(BF16)
            kept[here, 4 * half + pair * 2 * BLOCK : 4 * half + (pair + 1) * 2 * BLOCK] = both
            kept[here, 3 * half + pair * 2 * HEAD_DIM : 3 * half + (pair + 1) * 2 * HEAD_DIM] = times(both, stacked(values[chars, lanes], masks)).astype(BF16)


def own_attention(x, wide, narrow, wq, wk, wv):
    span, width = x.shape
    half = wq.shape[1]

    def body(x_ref, wide, narrow, wq, wk, wv, a_ref, kept):
        masks = pair_masks()
        g, s = vector_row(wide, 0, width), vector_row(wide, 1, width)
        qb, vb = vector_row(narrow, 0, half), vector_row(narrow, 1, half)

        def step(i, carry):
            rows = rows_at(i)
            hat, _ = norm_stats(x_ref[rows, :].astype(F32))
            attn_in = (hat * g + s).astype(BF16)
            a_ref[rows, :] = attn_in
            attention_forward(attn_in, wq, wk, wv, qb, vb, rows, kept, masks)
            return carry

        lax.fori_loop(0, span // ROW_TILE, step, 0)

    outs = [((span, width), BF16), ((span, 4 * half + half // HEAD_DIM * BLOCK), BF16)]
    return call(body, outs, (x, wide, narrow, wq, wk, wv), vmem_mb=5,
                flops=2 * span * width * half * 3.5, bytes_accessed=8e6, name="own_attention")


def other_attention(a, parts, tail, half):
    span, width = a.shape
    counts = [part.shape[0] for part in parts]
    n = len(parts)
    last = tail.shape[1]

    def body(a_ref, tail_ref, *refs):
        part_refs = refs[:n]
        wqkv, wo, kept, narrow, sems = refs[n:]
        masks = pair_masks()
        rows_q = width // PARTS
        rows_o = half // PARTS
        targets = [(i * rows_q, rows_q, wqkv, pl.ds(i * half, half)) for i in range(3)]
        targets += [(3 * rows_q + i * rows_o, rows_o, wo, pl.ds(i * half, half)) for i in range(2)]
        copies = place_parts(part_refs, counts, targets, sems)
        for copy in copies:
            copy.start()
        rows = tail_ref[0, last - TAIL :, :].astype(F32)
        narrow[...] = jnp.concatenate([rows[i : i + 1, :] for i in range(narrow.shape[1] // half)], 1)
        qb, vb = vector_row(narrow, 0, half), vector_row(narrow, 1, half)
        for copy in copies:
            copy.wait()
        weights = [wqkv.at[:, pl.ds(i * half, half)] for i in range(3)]

        def step(i, carry):
            rows = rows_at(i)
            attention_forward(a_ref[rows, :], *weights, qb, vb, rows, kept, masks)
            return carry

        lax.fori_loop(0, span // ROW_TILE, step, 0)

    outs = [((width, 3 * half), BF16), ((half, width), BF16), ((span, 4 * half + half // HEAD_DIM * BLOCK), BF16)]
    outs += [((1, 9 * half), F32)]
    return call(body, outs, (a, tail, *parts), [pltpu.SemaphoreType.DMA((PARTS * 5,))], 5,
                2 * span * width * half * 3.5, 9e6, "other_attention")


def attention_output(x, kept_own, kept_other, wo_own, wo_other, wide):
    span, width = x.shape
    half = width // 2

    def body(x_ref, ko, kt, wo, wt, wide, h_ref, c_ref):
        b, g, s = [vector_row(wide, i, width) for i in (2, 3, 4)]
        ctx = slice(3 * half, 4 * half)

        def step(i, carry):
            rows = rows_at(i)
            middle = x_ref[rows, :].astype(F32) + b + times(ko[rows, ctx], wo[...]) + times(kt[rows, ctx], wt[...])
            h_ref[rows, :] = middle
            hat, _ = norm_stats(middle)
            c_ref[rows, :] = (hat * g + s).astype(BF16)
            return carry

        lax.fori_loop(0, span // ROW_TILE, step, 0)

    outs = [((span, width), F32), ((span, width), BF16)]
    return call(body, outs, (x, kept_own, kept_other, wo_own, wo_other, wide), vmem_mb=4,
                flops=2 * span * width * width, bytes_accessed=9e6, name="attention_output")


HIDDEN_TILE = 384


def feed_forward_half(c_ref, acc_ref, up, narrow, start, down, hid_ref, slope_ref, ub):
    span = c_ref.shape[0]
    units = up.shape[1]
    ub[...] = narrow[:, start : start + units]

    def step(j, carry):
        cols = rows_at(j, HIDDEN_TILE)
        for i in range(span // ROW_TILE):
            rows = slice(i * ROW_TILE, (i + 1) * ROW_TILE)
            upper = times(c_ref[rows, :], up[:, cols]) + ub[:, cols]
            hidden, slope = gelu_parts(upper)
            hidden = hidden.astype(BF16)
            hid_ref[rows, cols] = hidden
            slope_ref[rows, cols] = slope.astype(BF16)
            acc_ref[rows, :] += times(hidden, down[cols, :])
        return carry

    lax.fori_loop(0, units // HIDDEN_TILE, step, 0)


def own_feed_forward(c, middle, wide, narrow, up, down):
    span, width = c.shape
    units = up.shape[1]

    def body(c_ref, m_ref, wide, narrow, up, down, hid_ref, slope_ref, acc_ref, ub):
        acc_ref[...] = m_ref[...] + vector_row(wide, 5, width)
        feed_forward_half(c_ref, acc_ref, up, narrow, narrow.shape[1] - units, down, hid_ref, slope_ref, ub)

    outs = [((span, units), BF16)] * 2 + [((span, width), F32)]
    return call(body, outs, (c, middle, wide, narrow, up, down), [pltpu.VMEM((1, units), F32)], vmem_mb=4,
                flops=4 * span * width * units, bytes_accessed=16e6, name="own_feed_forward")


def other_feed_forward(c, acc, narrow, units, start, parts, name):
    span, width = c.shape
    half = width // 2
    counts = [part.shape[0] for part in parts]
    n = len(parts)

    def body(c_ref, a_ref, narrow, *refs):
        up, down, hid_ref, slope_ref, acc_ref, sems, ub = refs[n:]
        rows_u, rows_d = width // PARTS, units // PARTS
        targets = [(j * rows_u, rows_u, up, pl.ds(j * half, half)) for j in range(units // half)]
        first = len(targets) * rows_u
        targets += [(first + j * rows_d, rows_d, down, pl.ds(j * half, half)) for j in range(width // half)]
        copies = place_parts(refs[:n], counts, targets, sems)
        for copy in copies:
            copy.start()
        acc_ref[...] = a_ref[...]
        for copy in copies:
            copy.wait()
        feed_forward_half(c_ref, acc_ref, up, narrow, start, down, hid_ref, slope_ref, ub)

    outs = [((width, units), BF16), ((units, width), BF16)] + [((span, units), BF16)] * 2 + [((span, width), F32)]
    scratch = [pltpu.SemaphoreType.DMA((PARTS * 4,)), pltpu.VMEM((1, units), F32)]
    return call(body, outs, (c, acc, narrow, *parts), scratch, 4, 4 * span * width * units, 9e6, name)


def downsample(h2, wc_own, wc_parts, narrow, narrow_other, cot):
    span, width = h2.shape
    half = width // 2
    mols = span // STRIDE
    counts = [part.shape[0] for part in wc_parts]
    n = len(wc_parts)

    def body(h_ref, wo, narrow, narrow_other, cot_ref, *refs):
        part_refs = refs[:n]
        hs_ref, dc_ref, mol_own, mol_other, dh_ref, dh16_ref, vec_ref, wt, strip, sems = refs[n:]
        left = lax.axis_index("tensor") == 0
        b, g, s = (
            jnp.concatenate([vector_row(ref, i, half) for ref in (narrow, narrow_other)], 1) for i in (2, 3, 4)
        )
        copies = place_parts(part_refs, counts, [(0, STRIDE * width // PARTS, wt, slice(None))], sems)
        for copy in copies:
            copy.start()
        pre_own = jnp.zeros((mols, half), F32)
        for lane in range(width // 128):
            strip[lane] = h_ref[:, lane * 128 : (lane + 1) * 128]
        for tap in range(STRIDE):
            window = jnp.concatenate(
                [strip[lane, pl.ds(tap, mols, stride=STRIDE), :] for lane in range(width // 128)], 1
            ).astype(BF16)
            hs_ref[tap * mols : (tap + 1) * mols, :] = window
            pre_own += times(window, wo[tap * width : (tap + 1) * width, :])
        for copy in copies:
            copy.wait()
        pre_other = jnp.zeros((mols, half), F32)
        for tap in range(STRIDE):
            window = hs_ref[tap * mols : (tap + 1) * mols, :]
            pre_other += times(window, wt[tap * width : (tap + 1) * width, :])
        conv = jnp.concatenate([pre_own, pre_other], 1) + b
        act, slope = gelu_parts(conv)
        hat, inv = norm_stats(act)
        whole = cot_ref[...].astype(F32)
        after = whole[mols + 1 :, :]
        after = jnp.concatenate([after, jnp.zeros((1, width), F32)], 0)
        after = jnp.concatenate([after[:, half:], after[:, :half]], 1)
        cotangent = jnp.where(left, whole[1 : mols + 1, :], after)
        dpre = norm_back(cotangent * g, hat, inv)
        dconv = dpre * slope
        dconv16 = dconv.astype(BF16)
        dc_ref[...] = dconv16
        hat0, inv0 = norm_stats(h_ref[0:8, :])
        only = (lax.broadcasted_iota(jnp.int32, (8, width), 0) == 0) & left
        cot0 = jnp.where(only, whole[0:8, :], 0.0)
        dpre0 = norm_back(cot0 * g, hat0, inv0)
        mol = jnp.concatenate([(hat0 * g + s)[0:1], hat * g + s, jnp.zeros((15, width), F32)], 0).astype(BF16)
        mol_own[...] = mol[:, :half]
        mol_other[...] = mol[:, half:]
        vec_ref[...] = jnp.zeros_like(vec_ref)
        vec_ref[0:1, :] = column_sum(cotangent * hat) + column_sum(cot0 * hat0)
        vec_ref[1:2, :] = column_sum(cotangent) + column_sum(cot0)
        vec_ref[2:3, :] = column_sum(dconv)
        for tap in range(STRIDE):
            taps = slice(tap * width, (tap + 1) * width)
            back = times_t(dconv16[:, :half], wo[taps, :]) + times_t(dconv16[:, half:], wt[taps, :])
            for lane in range(width // 128):
                strip[lane, pl.ds(tap, mols, stride=STRIDE), :] = back[:, lane * 128 : (lane + 1) * 128]
        for lane in range(width // 128):
            dh_ref[:, lane * 128 : (lane + 1) * 128] = strip[lane]
        dh_ref[0:8, :] += dpre0
        total = jnp.zeros((1, width), F32)
        for i in range(span // ROW_TILE):
            rows = slice(i * ROW_TILE, (i + 1) * ROW_TILE)
            grad = dh_ref[rows, :]
            dh16_ref[rows, :] = grad.astype(BF16)
            total += column_sum(grad)
        vec_ref[3:4, :] = total

    outs = [((span, width), BF16), ((mols, width), BF16), ((mols + 16, half), BF16), ((mols + 16, half), BF16),
            ((span, width), F32), ((span, width), BF16), ((8, width), F32)]
    spaces = None
    scratch = [pltpu.VMEM((STRIDE * width, half), BF16), pltpu.VMEM((width // 128, span, 128), F32), pltpu.SemaphoreType.DMA((PARTS,))]
    return call(body, outs, (h2, wc_own, narrow, narrow_other, cot, *wc_parts), scratch, 10,
                8 * span * width * width / 2, 16e6, "downsample", spaces)


def conv_weight_grad(hs, dconv16):
    span, width = hs.shape
    half = width // 2
    mols = span // STRIDE
    rows = STRIDE * width // 16

    def body(hs_ref, dc_ref, keep_ref, send_ref):
        place = Place()
        for tap in range(STRIDE):
            grad = t_times(hs_ref[tap * mols : (tap + 1) * mols, :], dc_ref[...]).astype(BF16)
            blocks = [
                (tap * 4 + i, group, grad[i * rows : (i + 1) * rows, group * half : (group + 1) * half])
                for i in range(4)
                for group in range(2)
            ]
            store_blocks(place, blocks, keep_ref, send_ref, slice(None))

    outs = [((16, rows, half), BF16)] * 2
    return call(body, outs, (hs, dconv16), (), 8, 2 * span * width * width, 7e6, "conv_weight_grad", weight=LONG)


GRAD_TILE = 384


def weight_grad(lefts, rights, name):
    span, width = lefts[0].shape
    units = sum(item[3] for item in rights[0])
    rows = width // 16
    flat = [item[1] for group in rights for item in group]
    nl, nr = len(lefts), len(flat)

    def body(*refs):
        left_refs, right_refs = refs[:nl], refs[nl : nl + nr]
        keep_ref, send_ref, turned = refs[nl + nr :]
        place = Place()
        for i, ref in enumerate(left_refs):
            turned[i] = ref[...].T
        at = 0
        for group_index, group in enumerate(rights):
            column = 0
            for which, _, first, count in group:
                ref = right_refs[at]
                at += 1
                tile = min(HIDDEN_TILE, count)

                def step(j, carry, ref=ref, which=which, group_index=group_index, column=column, first=first):
                    cols = pl.ds(pl.multiple_of(first + j * tile, 128), tile)
                    target = pl.ds(pl.multiple_of(column + j * tile, 128), tile)
                    blocks = []
                    for i in range(width // GRAD_TILE):
                        grad = times(turned[which, i * GRAD_TILE : (i + 1) * GRAD_TILE, :], ref[:, cols]).astype(BF16)
                        per = GRAD_TILE // rows
                        blocks += [(i * per + k, group_index, grad[k * rows : (k + 1) * rows]) for k in range(per)]
                    store_blocks(place, blocks, keep_ref, send_ref, target)
                    return carry

                lax.fori_loop(0, count // tile, step, 0)
                column += count

    outs = [((16, rows, units), BF16)] * 2
    return call(body, outs, (*lefts, *flat), [pltpu.VMEM((nl, width, span), BF16)], 8,
                4 * span * width * units, 12e6, name, weight=LONG)


def feed_forward_backward(dh2_16, slopes, ups, downs, name, acc=None, close=None):
    span, width = dh2_16.shape
    n = len(ups)
    sizes = [up.shape[1] for up in ups]
    more = (() if acc is None else (acc,)) + (() if close is None else close)

    def body(dh16_ref, *refs):
        slope_refs, up_refs, down_refs, refs = refs[:n], refs[n : 2 * n], refs[2 * n : 3 * n], refs[3 * n :]
        more_refs, du_refs, refs = refs[: len(more)], refs[len(more) : len(more) + n], refs[len(more) + n :]
        ub_refs, refs = refs[:n], refs[n:]
        acc_ref = refs[-1]
        if acc is None:
            acc_ref[...] = jnp.zeros_like(acc_ref)
        else:
            acc_ref[...] = more_refs[0][...]
        for slope_ref, up, down, du_ref, ub_ref in zip(slope_refs, up_refs, down_refs, du_refs, ub_refs):
            def step(j, carry, slope_ref=slope_ref, up=up, down=down, du_ref=du_ref, ub_ref=ub_ref):
                cols = rows_at(j, HIDDEN_TILE)
                total = jnp.zeros((1, HIDDEN_TILE), F32)
                for i in range(span // ROW_TILE):
                    rows = slice(i * ROW_TILE, (i + 1) * ROW_TILE)
                    grad = times_t(dh16_ref[rows, :], down[cols, :]) * slope_ref[rows, cols].astype(F32)
                    total += column_sum(grad)
                    grad16 = grad.astype(BF16)
                    du_ref[rows, cols] = grad16
                    acc_ref[rows, :] += times_t(grad16, up[:, cols])
                ub_ref[:, cols] = total
                return carry

            lax.fori_loop(0, up.shape[1] // HIDDEN_TILE, step, 0)
        if close is None:
            return
        dh_ref, m_ref, wide = more_refs[-3:]
        dm_ref, dm16_ref, vec_ref = refs[:3]
        g = vector_row(wide, 3, width)
        vec_ref[...] = jnp.zeros_like(vec_ref)

        def finish(i, carry):
            rows = rows_at(i)
            back = acc_ref[rows, :]
            hat, inv = norm_stats(m_ref[rows, :])
            grad = dh_ref[rows, :] + norm_back(back * g, hat, inv)
            dm_ref[rows, :] = grad
            dm16_ref[rows, :] = grad.astype(BF16)
            vec_ref[0:1, :] += column_sum(back * hat)
            vec_ref[1:2, :] += column_sum(back)
            vec_ref[2:3, :] += column_sum(grad)
            return carry

        lax.fori_loop(0, span // ROW_TILE, finish, 0)

    outs = [((span, size), BF16) for size in sizes] + [((1, size), F32) for size in sizes]
    if close is None:
        outs += [((span, width), F32)]
        scratch = []
    else:
        outs += [((span, width), F32), ((span, width), BF16), ((8, width), F32)]
        scratch = [pltpu.VMEM((span, width), F32)]
    return call(body, outs, (dh2_16, *slopes, *ups, *downs, *more), scratch, 12,
                8 * span * width * sum(sizes) / 2, 16e6, name, weight=LONG)


def attention_backward(dm16, wo, kept, name):
    span, width = dm16.shape
    half = width // 2

    def body(dm_ref, wo, kept, grads, vec_ref):
        masks = pair_masks()
        lane = lax.broadcasted_iota(jnp.int32, (1, 2 * HEAD_DIM), 1) < HEAD_DIM
        vec_ref[...] = jnp.zeros_like(vec_ref)

        def step(i, carry):
            rows = rows_at(i)
            dctx = times_t(dm_ref[rows, :], wo[...]).astype(BF16)
            for block in range(ROW_TILE // BLOCK):
                chars = slice(block * BLOCK, (block + 1) * BLOCK)
                here = pl.ds(rows.start + block * BLOCK, BLOCK)
                for pair in range(half // (2 * HEAD_DIM)):
                    first = pair * 2 * HEAD_DIM
                    q, k, v = [kept[here, i * half + first : i * half + first + 2 * HEAD_DIM] for i in range(3)]
                    p = kept[here, 4 * half + pair * 2 * BLOCK : 4 * half + (pair + 1) * 2 * BLOCK]
                    grad = dctx[chars, first : first + 2 * HEAD_DIM]
                    dv2 = t_times(p, grad)
                    dv = jnp.where(lane, dv2[:BLOCK], dv2[BLOCK:])
                    dp = times_t(grad, stacked(v, masks))
                    p32 = p.astype(F32)
                    ds = []
                    for head in range(2):
                        part = slice(head * BLOCK, (head + 1) * BLOCK)
                        weighted = p32[:, part] * dp[:, part]
                        inner = jnp.sum(weighted, -1, keepdims=True)
                        ds.append((weighted - p32[:, part] * inner) * HEAD_DIM ** (-0.5))
                    ds = jnp.concatenate(ds, 1).astype(BF16)
                    dq = times(ds, stacked(k, masks))
                    dk2 = t_times(ds, q)
                    dk = jnp.where(lane, dk2[:BLOCK], dk2[BLOCK:])
                    for i, value in enumerate((dq, dk, dv)):
                        grads[here, i * half + first : i * half + first + 2 * HEAD_DIM] = value.astype(BF16)
                    lanes = slice(first, first + 2 * HEAD_DIM)
                    vec_ref[0:1, lanes] += column_sum(dq)
                    vec_ref[1:2, lanes] += column_sum(dv)
            return carry

        lax.fori_loop(0, span // ROW_TILE, step, 0)

    outs = [((span, 3 * half), BF16), ((8, half), F32)]
    return call(body, outs, (dm16, wo, kept), vmem_mb=4,
                flops=2 * span * width * half * 2, bytes_accessed=8e6, name=name, weight=LONG)


def input_backward(dm, x, wide, grads_own, grads_other, own_weights, other_weight):
    span, width = dm.shape
    half = width // 2

    def body(dm_ref, x_ref, wide, go, gt, wq, wk, wv, wt, out_ref, vec_ref):
        g = vector_row(wide, 0, width)
        vec_ref[...] = jnp.zeros_like(vec_ref)

        def step(i, carry):
            rows = rows_at(i)
            back = times_t(gt[rows, :], wt[...])
            for i, ref in enumerate((wq, wk, wv)):
                back += times_t(go[rows, i * half : (i + 1) * half], ref[...])
            hat, inv = norm_stats(x_ref[rows, :].astype(F32))
            out_ref[rows, :] = dm_ref[rows, :] + norm_back(back * g, hat, inv)
            vec_ref[0:1, :] += column_sum(back * hat)
            vec_ref[1:2, :] += column_sum(back)
            return carry

        lax.fori_loop(0, span // ROW_TILE, step, 0)

    outs = [((span, width), F32), ((8, width), F32)]
    return call(body, outs, (dm, x, wide, grads_own, grads_other, *own_weights, other_weight), vmem_mb=9,
                flops=2 * span * width * 3 * width, bytes_accessed=12e6, name="input_backward", weight=LONG)


def pack_vectors(conv_vec, ffn_vec, in_vec, own_vec, other_vec, own_up, *other_ups):
    half = own_vec.shape[1]
    ups = own_up.shape[1] // half
    rows = -(-(12 + 5 + ups) // 8) * 8

    def body(conv, ffn, inp, own, other, up, *refs):
        other_up, (mine, theirs) = refs[:-2], refs[-2:]
        shared = [
            ref[i : i + 1, j * half : (j + 1) * half]
            for ref, i in ((conv, 3), (ffn, 0), (ffn, 1), (ffn, 2), (inp, 0), (inp, 1))
            for j in range(2)
        ]
        for out, vec, side, some in ((mine, own, 0, (up,)), (theirs, other, 1, other_up)):
            group = [conv[i : i + 1, side * half : (side + 1) * half] for i in range(3)]
            group += [vec[i : i + 1, :] for i in range(2)]
            group += [ref[:, j * half : (j + 1) * half] for ref in some for j in range(ref.shape[1] // half)]
            pad = [jnp.zeros((rows - 12 - len(group), half), F32)] if rows > 12 + len(group) else []
            out[...] = jnp.concatenate(shared + group + pad, 0)

    ins = (conv_vec, ffn_vec, in_vec, own_vec, other_vec, own_up, *other_ups)
    return call(body, [((rows, half), F32)] * 2, ins, (), 4, 0, 2e5, "pack_vectors")


def flat_permute(value, route, dp_size):
    pairs = []
    for d in range(dp_size):
        for t in range(2):
            d2, t2 = route(d, t)
            pairs.append((d * 2 + t, d2 * 2 + t2))
    return lax.ppermute(value, ("dp", "tensor"), pairs)


def over_x(d, t):
    return d, 1 - t


def over_core(d, t):
    return d ^ 1, t


def over_y(d, t):
    return d ^ 2, t


def over_z(flip):
    return lambda d, t: (d ^ (flip << 2), t)


def by_core(first, second):
    return lambda d, t: (second if d & 1 else first)(d, t)


def after(value, *others):
    others = [other for other in others if other is not None]
    return lax.optimization_barrier((value, *others))[0] if others else value


class Order:
    def __init__(self):
        self.last = None

    def __call__(self, step, *args):
        if self.last is not None:
            args = lax.optimization_barrier((args, self.last))[0]
        self.last = step(*args)
        return self.last


def split_sum(keep, got):
    size = keep.shape[0] // 2
    total = [(keep[at : at + size].astype(F32) + got[at : at + size].astype(F32)).astype(BF16) for at in (0, size)]
    return tuple(total)


class Reduction:
    def __init__(self, grid, order, blocks):
        self.grid, self.order = grid, order
        self.keep = blocks[0]
        self.stage = 0
        if grid.fast:
            self.got = grid.send(blocks[1], over_core)
        else:
            self.got = grid.send(blocks[1], over_x)

    def step(self):
        if not self.grid.fast:
            return
        route = (by_core(over_x, over_y), by_core(over_y, over_x), over_z(1), over_z(2))[self.stage]
        self.keep, out = self.order(split_sum, self.keep, self.got)
        self.got = self.grid.send(out, route)
        self.stage += 1

    def finish(self):
        if not self.grid.fast:
            total = self.keep.astype(F32) + self.got.astype(F32)
            total = total.reshape(-1, total.shape[-1])
            return lax.psum_scatter(total, "dp", scatter_dimension=0, tiled=True)
        return self.order(lambda keep, got: (keep.astype(F32) + got.astype(F32))[0], self.keep, self.got)


class Grid:
    def __init__(self):
        self.dp = lax.axis_size("dp")
        self.index = lax.axis_index("dp")
        self.side = lax.axis_index("tensor")
        self.fast = self.dp == 16

    def send(self, value, route):
        return flat_permute(value, route, self.dp)

    def gather(self, piece, before=None, again=None):
        first = self.send(piece, over_x)
        if not self.fast:
            return [first]
        first = after(first, before)
        second = self.send(first, by_core(over_y, over_z(1)))
        third = self.send(first, over_core)
        return [first, second, third, self.send(after(second, again), over_core)]


class VectorSum:
    def __init__(self, grid, order, packed):
        self.grid, self.order = grid, order
        self.routes = [over_core, over_y, over_z(1), over_z(2)] if grid.fast else []
        self.total, out = packed
        self.got = grid.send(out, over_x)

    def step(self):
        self.total = self.order(lambda total, got: total + got, self.total, self.got)
        if self.routes:
            self.got = self.grid.send(self.total, self.routes.pop(0))

    def finish(self):
        self.step()
        if not self.grid.fast:
            self.total = lax.psum(self.total, "dp")
        return self.total


def per_device(
    characters, first_gain, first_shift, query_weight, query_bias, key_weight, value_weight, value_bias,
    out_weight, out_bias, second_gain, second_shift, up_weight, up_bias, down_weight, down_bias,
    conv_weight, conv_bias, third_gain, third_shift, cotangent,
):
    _, length, width = characters.shape
    span = length // 2
    half = width // 2
    units = up_weight.shape[1]
    mols = span // STRIDE
    grid = Grid()
    side = grid.side

    order = Order()
    matrices = (query_weight, key_weight, value_weight, out_weight, up_weight, down_weight, conv_weight)
    x, *pieces, tail, wide, narrow = pick_pieces(
        characters[0],
        matrices,
        (first_gain, first_shift, out_bias, second_gain, second_shift, down_bias),
        (query_bias, value_bias, conv_bias, third_gain, third_shift, up_bias),
    )
    if not grid.fast:
        pieces = [
            jnp.concatenate(
                [
                    ref[first : first + count, column : column + half].reshape(PARTS, count // PARTS, half)
                    for ref, first, count, column in group
                ],
                1,
            )
            for group in piece_groups(*matrices)
        ]

    a, kept_own = own_attention(x, wide, narrow, query_weight, key_weight, value_weight)
    attention_parts = grid.gather(pieces[0], a)
    tail = attention_parts[0] if grid.fast else grid.send(tail, over_x)
    wqkv_other, wo_other, kept_other, narrow_other = other_attention(a, attention_parts, tail, half)
    middle, c = attention_output(x, kept_own, kept_other, out_weight, wo_other, wide)
    hid_own, slope_own, acc = own_feed_forward(c, middle, wide, narrow, up_weight, down_weight)
    ups, downs, hids, slopes = [up_weight], [down_weight], [hid_own], [slope_own]
    gates = [a, acc]
    for i in range(2):
        parts = grid.gather(pieces[1 + i], *gates)
        start = narrow.shape[1] - units + i * units // 2
        up, down, hid, slope, acc = other_feed_forward(
            c, acc, narrow_other, units // 2, start, parts, f"other_feed_forward_{i}"
        )
        gates = [gates[1], acc]
        for some, value in zip((ups, downs, hids, slopes), (up, down, hid, slope)):
            some.append(value)
    conv_parts = grid.gather(pieces[3], gates[0])

    hs, dconv16, mol_own, mol_other, dh2, dh2_16, conv_vec = order(
        lambda *args: downsample(*args[:2], args[4:], *args[2:4], cotangent[0]),
        acc, conv_weight, narrow, narrow_other, *conv_parts,
    )
    theirs = grid.send(mol_other, over_x)

    def whole(which, array):
        return (which, array, 0, array.shape[1])

    conv_sum = Reduction(grid, order, order(conv_weight_grad, hs, dconv16))
    down_sum = Reduction(
        grid,
        order,
        order(
            lambda left, own, *others: weight_grad(
                (left,), [[whole(0, own)], [whole(0, v) for v in others]], "down_weight_grad"
            ),
            dh2_16, *hids,
        ),
    )
    conv_sum.step()
    du_own, up_vec_own, acc = order(
        lambda dh16, slope, up, down: feed_forward_backward(dh16, [slope], [up], [down], "own_feed_forward_backward"),
        dh2_16, slopes[0], ups[0], downs[0],
    )
    down_sum.step()
    theirs = order(lambda value: value, theirs)
    du_first, du_second, *up_vecs, dm, dm16, ffn_vec = order(
        lambda dh16, acc, *args: feed_forward_backward(
            dh16, args[3:5], args[5:7], args[7:9], "other_feed_forward_backward", acc, args[:3]
        ),
        dh2_16, acc, dh2, middle, wide, *slopes[1:], *ups[1:], *downs[1:],
    )
    conv_sum.step()
    down_sum.step()
    up_sum = Reduction(
        grid,
        order,
        order(
            lambda c, dm16, own, first, second, kept_own, kept_other: weight_grad(
                (c, dm16),
                [
                    [whole(0, own), (1, kept_own, 3 * half, half)],
                    [whole(0, first), whole(0, second), (1, kept_other, 3 * half, half)],
                ],
                "up_weight_grad",
            ),
            c, dm16, du_own, du_first, du_second, kept_own, kept_other,
        ),
    )
    dqkv_own, vec_own = order(
        functools.partial(attention_backward, name="own_attention_backward"), dm16, out_weight, kept_own
    )
    up_sum.step()
    conv_sum.step()
    down_sum.step()
    dqkv_other, vec_other = order(
        functools.partial(attention_backward, name="other_attention_backward"), dm16, wo_other, kept_other
    )
    conv_sum.step()
    down_sum.step()
    attention_sum = Reduction(
        grid,
        order,
        order(
            lambda a, own, other: weight_grad((a,), [[whole(0, own)], [whole(0, other)]], "attention_weight_grad"),
            a, dqkv_own, dqkv_other,
        ),
    )
    up_sum.step()
    sum_conv_weight = conv_sum.finish()
    input_rows, in_vec = order(
        lambda *args: input_backward(*args[:5], args[5:8], args[8]),
        dm, x, wide, dqkv_own, dqkv_other, query_weight, key_weight, value_weight, wqkv_other,
    )
    attention_sum.step()
    vectors = VectorSum(
        grid, order, order(pack_vectors, conv_vec, ffn_vec, in_vec, vec_own, vec_other, up_vec_own, *up_vecs)
    )
    sum_down = down_sum.finish()
    up_sum.step()
    vectors.step()
    attention_sum.step()
    vectors.step()
    up_sum.step()
    attention_sum.step()
    vectors.step()
    attention_sum.step()
    vectors.step()
    sum_up = up_sum.finish()
    vectors.finish()
    shared, own = vectors.total[:12], vectors.total[12:]
    sum_attention = attention_sum.finish()

    mine, theirs = mol_own[: mols + 1], theirs[: mols + 1]
    upper = jnp.where(side == 0, mine, theirs)
    lower = jnp.where(side == 0, theirs, mine)
    molecules = jnp.concatenate([upper, lower[1:mols]], 0)[None]

    shared = shared.reshape(-1, width)
    block = width // grid.dp
    shared = lax.dynamic_slice_in_dim(shared, grid.index * block, block, 1)
    return (
        molecules,
        input_rows[None],
        shared[4],
        shared[5],
        sum_attention[:, :half],
        own[3],
        sum_attention[:, half : 2 * half],
        sum_attention[:, 2 * half : 3 * half],
        own[4],
        sum_up[:, units:].T,
        shared[3],
        shared[1],
        shared[2],
        sum_up[:, :units],
        own[5 : 5 + units // half].reshape(-1),
        sum_down.T,
        shared[0],
        sum_conv_weight,
        own[2],
        own[0],
        own[1],
    )


def solution(mesh):
    return jax.shard_map(
        per_device,
        mesh=mesh,
        in_specs=(
            P("dp", None, None),
            P(),
            P(),
            P(None, "tensor"),
            P("tensor"),
            P(None, "tensor"),
            P(None, "tensor"),
            P("tensor"),
            P("tensor", None),
            P(),
            P(),
            P(),
            P(None, "tensor"),
            P("tensor"),
            P("tensor", None),
            P(),
            P(None, "tensor"),
            P("tensor"),
            P("tensor"),
            P("tensor"),
            P("dp", None, None),
        ),
        out_specs=(
            P("dp", None, "tensor"),
            P("dp", "tensor", None),
            P("dp"),
            P("dp"),
            P("dp", "tensor"),
            P("tensor"),
            P("dp", "tensor"),
            P("dp", "tensor"),
            P("tensor"),
            P("tensor", "dp"),
            P("dp"),
            P("dp"),
            P("dp"),
            P("dp", "tensor"),
            P("tensor"),
            P("tensor", "dp"),
            P("dp"),
            P("dp", "tensor"),
            P("tensor"),
            P("tensor"),
            P("tensor"),
        ),
        check_vma=False,
    )
```

```python
import functools

import jax
import jax.numpy as jnp
from jax import lax
from jax.experimental import pallas as pl
from jax.experimental.pallas import tpu as pltpu
from jax.sharding import PartitionSpec as P

HEAD_DIM = 64
BLOCK = 128
STRIDE = 4
EPSILON = 1e-05
INV_ROOT_TWO = 0.7071067811865476
INV_ROOT_TWO_PI = 0.3989422804014327
F32 = jnp.float32
BF16 = jnp.bfloat16
PARTS = 4
ROW_TILE = 256
LONG = 8
SHORT = 0.1


def times(left, right):
    return jnp.dot(left, right, preferred_element_type=F32)


def times_t(left, right):
    return lax.dot_general(left, right, (((1,), (1,)), ((), ())), preferred_element_type=F32)


def t_times(left, right):
    return lax.dot_general(left, right, (((0,), (0,)), ((), ())), preferred_element_type=F32)


def gelu_parts(u):
    phi = 0.5 + 0.5 * lax.erf(u * INV_ROOT_TWO)
    return u * phi, phi + u * (jnp.exp(-0.5 * (u * u)) * INV_ROOT_TWO_PI)


def norm_stats(values):
    mean = jnp.mean(values, -1, keepdims=True)
    centered = values - mean
    inv = lax.rsqrt(jnp.mean(centered * centered, -1, keepdims=True) + EPSILON)
    return centered * inv, inv


def norm_back(scaled, hat, inv):
    return inv * (
        scaled
        - jnp.mean(scaled, -1, keepdims=True)
        - hat * jnp.mean(scaled * hat, -1, keepdims=True)
    )


def vector_row(ref, index, width):
    return ref[:, index * width : (index + 1) * width]


def column_sum(values):
    return jnp.sum(values, 0, keepdims=True)


def call(body, outs, ins, scratch=(), vmem_mb=32, flops=0, bytes_accessed=0, name=None, spaces=None, weight=1):
    spaces = spaces or {}
    in_specs = [pl.BlockSpec(memory_space=spaces.get(("in", i), pltpu.VMEM)) for i in range(len(ins))]
    out_specs = [pl.BlockSpec(memory_space=spaces.get(("out", i), pltpu.VMEM)) for i in range(len(outs))]
    return pl.pallas_call(
        body,
        out_shape=[jax.ShapeDtypeStruct(shape, dtype) for shape, dtype in outs],
        in_specs=in_specs,
        out_specs=out_specs,
        scratch_shapes=list(scratch),
        compiler_params=pltpu.CompilerParams(vmem_limit_bytes=vmem_mb << 20),
        cost_estimate=pl.CostEstimate(
            flops=int(flops * weight), bytes_accessed=int(bytes_accessed * weight), transcendentals=0
        ),
        name=name,
    )(*ins)


def rows_at(step, tile=ROW_TILE):
    return pl.ds(pl.multiple_of(step * tile, tile), tile)


def pair_masks():
    lane = lax.broadcasted_iota(jnp.int32, (1, 2 * HEAD_DIM), 1)
    low = (lane < HEAD_DIM).astype(F32).astype(BF16)
    high = (lane >= HEAD_DIM).astype(F32).astype(BF16)
    return low, high


def stacked(pair, masks):
    return jnp.concatenate([pair * masks[0], pair * masks[1]], 0)


TAIL = 16


def piece_groups(wq, wk, wv, wo, up, down, conv):
    width, half = wq.shape
    units = up.shape[1]
    groups = [[(ref, 0, width, 0) for ref in (wq, wk, wv)] + [(wo, 0, half, j * half) for j in range(2)]]
    for first in (0, units // 2):
        groups.append(
            [(up, 0, width, first + j * half) for j in range(units // 2 // half)]
            + [(down, first, units // 2, j * half) for j in range(2)]
        )
    groups.append([(conv, 0, conv.shape[0], 0)])
    return groups


class Place:
    def __init__(self):
        self.fast = lax.axis_size("dp") == 16
        index = lax.axis_index("dp")
        self.index, self.side = index, lax.axis_index("tensor")
        self.core, self.y, self.z = index & 1, (index >> 1) & 1, index >> 2
        self.low = jnp.where(self.core == 0, self.y, self.z & 1)
        self.piece = self.core * 2 + self.low

    def parts(self):
        if not self.fast:
            return list(range(PARTS))
        other_low = jnp.where(self.core == 0, self.z & 1, self.y)
        other = (1 - self.core) * 2 + other_low
        return [self.piece, self.piece ^ 1, other, other ^ 1]

    def position(self, block, core, half):
        if not self.fast:
            return block
        y_flip = ((block >> 1) & 1) ^ self.y
        z_flip = (block >> 2) ^ self.z
        high = half * 8 + y_flip * 4 if core % 2 == 0 else y_flip * 8 + half * 4
        return high + (z_flip & 1) * 2 + (z_flip >> 1)


def store_blocks(place, blocks, keep_ref, send_ref, columns):
    def store(swap):
        for block, core, half, values in blocks:
            away = (core % 2) ^ swap if place.fast else half
            (send_ref if away else keep_ref)[place.position(block, core, half), :, columns] = values

    if place.fast:
        for core in range(2):
            pl.when(place.core == core)(functools.partial(store, core))
    else:
        store(0)


def place_parts(part_refs, counts, targets, sems):
    table = Place().parts()
    copies = []
    slot = 0
    place = 0
    for ref, count in zip(part_refs, counts):
        for item in range(count):
            where = table[place]
            place += 1
            for start, rows, target, columns in targets:
                copies.append(
                    pltpu.make_async_copy(
                        ref.at[item, pl.ds(start, rows), :],
                        target.at[pl.ds(pl.multiple_of(where * rows, 16), rows), columns],
                        sems.at[slot],
                    )
                )
                slot += 1
    return copies


def pick_pieces(characters, matrices, wide_vectors, narrow_vectors):
    length, width = characters.shape
    span = length // 2
    half = matrices[0].shape[1]
    nm, vectors = len(matrices), (*wide_vectors, *narrow_vectors)
    nv, nw = len(vectors), len(wide_vectors)

    def body(*refs):
        chars, matrix_refs, vector_refs = refs[0], refs[1 : 1 + nm], refs[1 + nm : 1 + nm + nv]
        x_ref, pa, pair, pd, tail, wide, narrow = refs[1 + nm + nv : 8 + nm + nv]
        flat, sems = refs[8 + nm + nv : -1], refs[-1]
        targets = (pa.at[0], pair.at[0], pair.at[1], pd.at[0])
        wq, wk, wv, wo, up, down, conv = matrix_refs
        place = Place()
        copies = []

        def copy(source, target):
            made = pltpu.make_async_copy(source, target, sems.at[len(copies)])
            made.start()
            copies.append(made)

        for source, target in zip(vector_refs, flat):
            copy(source, target)
        for out, groups in zip(targets, piece_groups(wq, wk, wv, wo, up, down, conv)):
            start = 0
            for ref, first, count, column in groups:
                rows = count // PARTS
                source = ref.at[
                    pl.ds(pl.multiple_of(first + place.piece * rows, 16), rows), pl.ds(column, half)
                ]
                copy(source, out.at[pl.ds(start, rows), :])
                start += rows
        copy(chars.at[pl.ds(pl.multiple_of(place.side * span, 16), span), :], x_ref)
        for made in copies[:nv]:
            made.wait()
        for out, some in ((wide, flat[:nw]), (narrow, flat[nw:])):
            out[...] = jnp.concatenate([ref[...].astype(F32).reshape(1, -1) for ref in some], 1)
        count = narrow.shape[1] // half
        rows = [narrow[:, i * half : (i + 1) * half] for i in range(count)]
        rows = jnp.concatenate(rows + [jnp.zeros((TAIL - count, half), F32)], 0).astype(BF16)
        tail[0] = rows
        pa[0, pa.shape[1] - TAIL :, :] = rows
        for made in copies[nv:]:
            made.wait()

    sizes = [v.shape[0] for v in vectors]
    outs = [((span, width), BF16), ((1, width + TAIL, half), BF16)]
    outs += [((2, width, half), BF16), ((1, width, half), BF16)]
    outs += [((1, TAIL, half), BF16), ((1, sum(sizes[:nw])), F32), ((1, sum(sizes[nw:])), F32)]
    spaces = {("in", i): pltpu.HBM for i in range(1 + nm + nv)}
    scratch = [pltpu.VMEM((size,), BF16) for size in sizes] + [pltpu.SemaphoreType.DMA((40,))]
    return call(body, outs, (characters, *matrices, *vectors), scratch, 56, 0, 4e6, "pick_pieces", spaces)


def attention_forward(attn_in, wq, wk, wv, qb, vb, rows, kept, masks):
    queries = (times(attn_in, wq[...]) + qb).astype(BF16)
    keys = times(attn_in, wk[...]).astype(BF16)
    values = (times(attn_in, wv[...]) + vb).astype(BF16)
    half = queries.shape[1]
    kept[rows, 0:half] = queries
    kept[rows, half : 2 * half] = keys
    kept[rows, 2 * half : 3 * half] = values
    pairs = half // (2 * HEAD_DIM)
    for block in range(attn_in.shape[0] // BLOCK):
        chars = slice(block * BLOCK, (block + 1) * BLOCK)
        here = pl.ds(rows.start + block * BLOCK, BLOCK)
        for pair in range(pairs):
            lanes = slice(pair * 2 * HEAD_DIM, (pair + 1) * 2 * HEAD_DIM)
            scores = times_t(queries[chars, lanes], stacked(keys[chars, lanes], masks))
            scores = scores * HEAD_DIM ** (-0.5)
            probs = []
            for head in range(2):
                part = scores[:, head * BLOCK : (head + 1) * BLOCK]
                expo = jnp.exp(part - jnp.max(part, -1, keepdims=True))
                probs.append(expo * (1.0 / jnp.sum(expo, -1, keepdims=True)))
            both = jnp.concatenate(probs, 1).astype(BF16)
            kept[here, 4 * half + pair * 2 * BLOCK : 4 * half + (pair + 1) * 2 * BLOCK] = both
            kept[here, 3 * half + pair * 2 * HEAD_DIM : 3 * half + (pair + 1) * 2 * HEAD_DIM] = times(both, stacked(values[chars, lanes], masks)).astype(BF16)


def own_attention(x, wide, narrow, wq, wk, wv):
    span, width = x.shape
    half = wq.shape[1]

    def body(x_ref, wide, narrow, wq, wk, wv, a_ref, kept):
        masks = pair_masks()
        g, s = vector_row(wide, 0, width), vector_row(wide, 1, width)
        qb, vb = vector_row(narrow, 0, half), vector_row(narrow, 1, half)

        def step(i, carry):
            rows = rows_at(i)
            hat, _ = norm_stats(x_ref[rows, :].astype(F32))
            attn_in = (hat * g + s).astype(BF16)
            a_ref[rows, :] = attn_in
            attention_forward(attn_in, wq, wk, wv, qb, vb, rows, kept, masks)
            return carry

        lax.fori_loop(0, span // ROW_TILE, step, 0)

    outs = [((span, width), BF16), ((span, 4 * half + half // HEAD_DIM * BLOCK), BF16)]
    return call(body, outs, (x, wide, narrow, wq, wk, wv), vmem_mb=5,
                flops=2 * span * width * half * 3.5, bytes_accessed=8e6, name="own_attention")


def other_attention(a, parts, tail, half):
    span, width = a.shape
    counts = [part.shape[0] for part in parts]
    n = len(parts)
    last = tail.shape[1]

    def body(a_ref, tail_ref, *refs):
        part_refs = refs[:n]
        wqkv, wo, kept, narrow, sems = refs[n:]
        masks = pair_masks()
        rows_q = width // PARTS
        rows_o = half // PARTS
        targets = [(i * rows_q, rows_q, wqkv, pl.ds(i * half, half)) for i in range(3)]
        targets += [(3 * rows_q + i * rows_o, rows_o, wo, pl.ds(i * half, half)) for i in range(2)]
        copies = place_parts(part_refs, counts, targets, sems)
        for copy in copies:
            copy.start()
        rows = tail_ref[0, last - TAIL :, :].astype(F32)
        narrow[...] = jnp.concatenate([rows[i : i + 1, :] for i in range(narrow.shape[1] // half)], 1)
        qb, vb = vector_row(narrow, 0, half), vector_row(narrow, 1, half)
        for copy in copies:
            copy.wait()
        weights = [wqkv.at[:, pl.ds(i * half, half)] for i in range(3)]

        def step(i, carry):
            rows = rows_at(i)
            attention_forward(a_ref[rows, :], *weights, qb, vb, rows, kept, masks)
            return carry

        lax.fori_loop(0, span // ROW_TILE, step, 0)

    outs = [((width, 3 * half), BF16), ((half, width), BF16), ((span, 4 * half + half // HEAD_DIM * BLOCK), BF16)]
    outs += [((1, 9 * half), F32)]
    return call(body, outs, (a, tail, *parts), [pltpu.SemaphoreType.DMA((PARTS * 5,))], 5,
                2 * span * width * half * 3.5, 9e6, "other_attention")


def attention_output(x, kept_own, kept_other, wo_own, wo_other, wide):
    span, width = x.shape
    half = width // 2

    def body(x_ref, ko, kt, wo, wt, wide, h_ref, c_ref):
        b, g, s = [vector_row(wide, i, width) for i in (2, 3, 4)]
        ctx = slice(3 * half, 4 * half)

        def step(i, carry):
            rows = rows_at(i)
            middle = x_ref[rows, :].astype(F32) + b + times(ko[rows, ctx], wo[...]) + times(kt[rows, ctx], wt[...])
            h_ref[rows, :] = middle
            hat, _ = norm_stats(middle)
            c_ref[rows, :] = (hat * g + s).astype(BF16)
            return carry

        lax.fori_loop(0, span // ROW_TILE, step, 0)

    outs = [((span, width), F32), ((span, width), BF16)]
    return call(body, outs, (x, kept_own, kept_other, wo_own, wo_other, wide), vmem_mb=4,
                flops=2 * span * width * width, bytes_accessed=9e6, name="attention_output")


HIDDEN_TILE = 384


def feed_forward_half(c_ref, acc_ref, up, narrow, start, down, hid_ref, slope_ref, ub):
    span = c_ref.shape[0]
    units = up.shape[1]
    ub[...] = narrow[:, start : start + units]

    def step(j, carry):
        cols = rows_at(j, HIDDEN_TILE)
        for i in range(span // ROW_TILE):
            rows = slice(i * ROW_TILE, (i + 1) * ROW_TILE)
            upper = times(c_ref[rows, :], up[:, cols]) + ub[:, cols]
            hidden, slope = gelu_parts(upper)
            hidden = hidden.astype(BF16)
            hid_ref[rows, cols] = hidden
            slope_ref[rows, cols] = slope.astype(BF16)
            acc_ref[rows, :] += times(hidden, down[cols, :])
        return carry

    lax.fori_loop(0, units // HIDDEN_TILE, step, 0)


def own_feed_forward(c, middle, wide, narrow, up, down):
    span, width = c.shape
    units = up.shape[1]

    def body(c_ref, m_ref, wide, narrow, up, down, hid_ref, slope_ref, acc_ref, ub):
        acc_ref[...] = m_ref[...] + vector_row(wide, 5, width)
        feed_forward_half(c_ref, acc_ref, up, narrow, narrow.shape[1] - units, down, hid_ref, slope_ref, ub)

    outs = [((span, units), BF16)] * 2 + [((span, width), F32)]
    return call(body, outs, (c, middle, wide, narrow, up, down), [pltpu.VMEM((1, units), F32)], vmem_mb=4,
                flops=4 * span * width * units, bytes_accessed=16e6, name="own_feed_forward")


def other_feed_forward(c, acc, narrow, units, start, parts, name):
    span, width = c.shape
    half = width // 2
    counts = [part.shape[0] for part in parts]
    n = len(parts)

    def body(c_ref, a_ref, narrow, *refs):
        up, down, hid_ref, slope_ref, acc_ref, sems, ub = refs[n:]
        rows_u, rows_d = width // PARTS, units // PARTS
        targets = [(j * rows_u, rows_u, up, pl.ds(j * half, half)) for j in range(units // half)]
        first = len(targets) * rows_u
        targets += [(first + j * rows_d, rows_d, down, pl.ds(j * half, half)) for j in range(width // half)]
        copies = place_parts(refs[:n], counts, targets, sems)
        for copy in copies:
            copy.start()
        acc_ref[...] = a_ref[...]
        for copy in copies:
            copy.wait()
        feed_forward_half(c_ref, acc_ref, up, narrow, start, down, hid_ref, slope_ref, ub)

    outs = [((width, units), BF16), ((units, width), BF16)] + [((span, units), BF16)] * 2 + [((span, width), F32)]
    scratch = [pltpu.SemaphoreType.DMA((PARTS * 4,)), pltpu.VMEM((1, units), F32)]
    return call(body, outs, (c, acc, narrow, *parts), scratch, 4, 4 * span * width * units, 9e6, name)


def downsample(h2, wc_own, wc_parts, narrow, narrow_other, cot):
    span, width = h2.shape
    half = width // 2
    mols = span // STRIDE
    counts = [part.shape[0] for part in wc_parts]
    n = len(wc_parts)

    def body(h_ref, wo, narrow, narrow_other, cot_ref, *refs):
        part_refs = refs[:n]
        hs_ref, dc_ref, mol_own, mol_other, dh_ref, dh16_ref, vec_ref, wt, strip, sems = refs[n:]
        left = lax.axis_index("tensor") == 0
        b, g, s = (
            jnp.concatenate([vector_row(ref, i, half) for ref in (narrow, narrow_other)], 1) for i in (2, 3, 4)
        )
        copies = place_parts(part_refs, counts, [(0, STRIDE * width // PARTS, wt, slice(None))], sems)
        for copy in copies:
            copy.start()
        pre_own = jnp.zeros((mols, half), F32)
        for lane in range(width // 128):
            strip[lane] = h_ref[:, lane * 128 : (lane + 1) * 128]
        for tap in range(STRIDE):
            window = jnp.concatenate(
                [strip[lane, pl.ds(tap, mols, stride=STRIDE), :] for lane in range(width // 128)], 1
            ).astype(BF16)
            hs_ref[tap * mols : (tap + 1) * mols, :] = window
            pre_own += times(window, wo[tap * width : (tap + 1) * width, :])
        for copy in copies:
            copy.wait()
        pre_other = jnp.zeros((mols, half), F32)
        for tap in range(STRIDE):
            window = hs_ref[tap * mols : (tap + 1) * mols, :]
            pre_other += times(window, wt[tap * width : (tap + 1) * width, :])
        conv = jnp.concatenate([pre_own, pre_other], 1) + b
        act, slope = gelu_parts(conv)
        hat, inv = norm_stats(act)
        whole = cot_ref[...].astype(F32)
        after = whole[mols + 1 :, :]
        after = jnp.concatenate([after, jnp.zeros((1, width), F32)], 0)
        after = jnp.concatenate([after[:, half:], after[:, :half]], 1)
        cotangent = jnp.where(left, whole[1 : mols + 1, :], after)
        dpre = norm_back(cotangent * g, hat, inv)
        dconv = dpre * slope
        dconv16 = dconv.astype(BF16)
        dc_ref[...] = dconv16
        hat0, inv0 = norm_stats(h_ref[0:8, :])
        only = (lax.broadcasted_iota(jnp.int32, (8, width), 0) == 0) & left
        cot0 = jnp.where(only, whole[0:8, :], 0.0)
        dpre0 = norm_back(cot0 * g, hat0, inv0)
        mol = jnp.concatenate([(hat0 * g + s)[0:1], hat * g + s, jnp.zeros((15, width), F32)], 0).astype(BF16)
        mol_own[...] = mol[:, :half]
        mol_other[...] = mol[:, half:]
        vec_ref[...] = jnp.zeros_like(vec_ref)
        vec_ref[0:1, :] = column_sum(cotangent * hat) + column_sum(cot0 * hat0)
        vec_ref[1:2, :] = column_sum(cotangent) + column_sum(cot0)
        vec_ref[2:3, :] = column_sum(dconv)
        for tap in range(STRIDE):
            taps = slice(tap * width, (tap + 1) * width)
            back = times_t(dconv16[:, :half], wo[taps, :]) + times_t(dconv16[:, half:], wt[taps, :])
            for lane in range(width // 128):
                strip[lane, pl.ds(tap, mols, stride=STRIDE), :] = back[:, lane * 128 : (lane + 1) * 128]
        for lane in range(width // 128):
            dh_ref[:, lane * 128 : (lane + 1) * 128] = strip[lane]
        dh_ref[0:8, :] += dpre0
        total = jnp.zeros((1, width), F32)
        for i in range(span // ROW_TILE):
            rows = slice(i * ROW_TILE, (i + 1) * ROW_TILE)
            grad = dh_ref[rows, :]
            dh16_ref[rows, :] = grad.astype(BF16)
            total += column_sum(grad)
        vec_ref[3:4, :] = total

    outs = [((span, width), BF16), ((mols, width), BF16), ((mols + 16, half), BF16), ((mols + 16, half), BF16),
            ((span, width), F32), ((span, width), BF16), ((8, width), F32)]
    spaces = None
    scratch = [pltpu.VMEM((STRIDE * width, half), BF16), pltpu.VMEM((width // 128, span, 128), F32), pltpu.SemaphoreType.DMA((PARTS,))]
    return call(body, outs, (h2, wc_own, narrow, narrow_other, cot, *wc_parts), scratch, 10,
                8 * span * width * width / 2, 16e6, "downsample", spaces)


def conv_weight_grad(hs, dconv16):
    span, width = hs.shape
    half = width // 2
    mols = span // STRIDE
    rows = STRIDE * width // 16

    def body(hs_ref, dc_ref, keep_ref, send_ref):
        place = Place()
        dc = dc_ref[...]

        def step(tap, carry):
            grad = t_times(hs_ref[pl.ds(pl.multiple_of(tap * mols, 16), mols), :], dc).astype(BF16)
            blocks = [
                (tap * 4 + i, i, group, grad[i * rows : (i + 1) * rows, group * half : (group + 1) * half])
                for i in range(4)
                for group in range(2)
            ]
            store_blocks(place, blocks, keep_ref, send_ref, slice(None))
            return carry

        lax.fori_loop(0, STRIDE, step, 0)

    outs = [((16, rows, half), BF16)] * 2
    return call(body, outs, (hs, dconv16), (), 8, 2 * span * width * width, 7e6, "conv_weight_grad", weight=LONG)


GRAD_TILE = 384


def weight_grad(lefts, rights, name):
    span, width = lefts[0].shape
    units = sum(item[3] for item in rights[0])
    rows = width // 16
    flat = [item[1] for group in rights for item in group]
    nl, nr = len(lefts), len(flat)

    def body(*refs):
        left_refs, right_refs = refs[:nl], refs[nl : nl + nr]
        keep_ref, send_ref, turned = refs[nl + nr :]
        place = Place()
        for i, ref in enumerate(left_refs):
            turned[i] = ref[...].T
        at = 0
        for group_index, group in enumerate(rights):
            column = 0
            for which, _, first, count in group:
                ref = right_refs[at]
                at += 1
                tile = min(HIDDEN_TILE, count)

                def step(j, carry, ref=ref, which=which, group_index=group_index, column=column, first=first):
                    cols = pl.ds(pl.multiple_of(first + j * tile, 128), tile)
                    target = pl.ds(pl.multiple_of(column + j * tile, 128), tile)
                    blocks = []
                    for i in range(width // GRAD_TILE):
                        grad = times(turned[which, i * GRAD_TILE : (i + 1) * GRAD_TILE, :], ref[:, cols]).astype(BF16)
                        per = GRAD_TILE // rows
                        blocks += [(i * per + k, i * per + k, group_index, grad[k * rows : (k + 1) * rows]) for k in range(per)]
                    store_blocks(place, blocks, keep_ref, send_ref, target)
                    return carry

                lax.fori_loop(0, count // tile, step, 0)
                column += count

    outs = [((16, rows, units), BF16)] * 2
    return call(body, outs, (*lefts, *flat), [pltpu.VMEM((nl, width, span), BF16)], 8,
                4 * span * width * units, 12e6, name, weight=LONG)


def feed_forward_backward(dh2_16, slopes, ups, downs, name, acc=None, close=None):
    span, width = dh2_16.shape
    n = len(ups)
    sizes = [up.shape[1] for up in ups]
    more = (() if acc is None else (acc,)) + (() if close is None else close)

    def body(dh16_ref, *refs):
        slope_refs, up_refs, down_refs, refs = refs[:n], refs[n : 2 * n], refs[2 * n : 3 * n], refs[3 * n :]
        more_refs, du_refs, refs = refs[: len(more)], refs[len(more) : len(more) + n], refs[len(more) + n :]
        ub_refs, refs = refs[:n], refs[n:]
        acc_ref = refs[-1]
        if acc is None:
            acc_ref[...] = jnp.zeros_like(acc_ref)
        else:
            acc_ref[...] = more_refs[0][...]
        for slope_ref, up, down, du_ref, ub_ref in zip(slope_refs, up_refs, down_refs, du_refs, ub_refs):
            def step(j, carry, slope_ref=slope_ref, up=up, down=down, du_ref=du_ref, ub_ref=ub_ref):
                cols = rows_at(j, HIDDEN_TILE)
                total = jnp.zeros((1, HIDDEN_TILE), F32)
                for i in range(span // ROW_TILE):
                    rows = slice(i * ROW_TILE, (i + 1) * ROW_TILE)
                    grad = times_t(dh16_ref[rows, :], down[cols, :]) * slope_ref[rows, cols].astype(F32)
                    total += column_sum(grad)
                    grad16 = grad.astype(BF16)
                    du_ref[rows, cols] = grad16
                    acc_ref[rows, :] += times_t(grad16, up[:, cols])
                ub_ref[:, cols] = total
                return carry

            lax.fori_loop(0, up.shape[1] // HIDDEN_TILE, step, 0)
        if close is None:
            return
        dh_ref, m_ref, wide = more_refs[-3:]
        dm_ref, dm16_ref, vec_ref = refs[:3]
        g = vector_row(wide, 3, width)
        vec_ref[...] = jnp.zeros_like(vec_ref)

        def finish(i, carry):
            rows = rows_at(i)
            back = acc_ref[rows, :]
            hat, inv = norm_stats(m_ref[rows, :])
            grad = dh_ref[rows, :] + norm_back(back * g, hat, inv)
            dm_ref[rows, :] = grad
            dm16_ref[rows, :] = grad.astype(BF16)
            vec_ref[0:1, :] += column_sum(back * hat)
            vec_ref[1:2, :] += column_sum(back)
            vec_ref[2:3, :] += column_sum(grad)
            return carry

        lax.fori_loop(0, span // ROW_TILE, finish, 0)

    outs = [((span, size), BF16) for size in sizes] + [((1, size), F32) for size in sizes]
    if close is None:
        outs += [((span, width), F32)]
        scratch = []
    else:
        outs += [((span, width), F32), ((span, width), BF16), ((8, width), F32)]
        scratch = [pltpu.VMEM((span, width), F32)]
    return call(body, outs, (dh2_16, *slopes, *ups, *downs, *more), scratch, 12,
                8 * span * width * sum(sizes) / 2, 16e6, name, weight=LONG)


def attention_backward(dm16, wo, kept, name):
    span, width = dm16.shape
    half = width // 2

    def body(dm_ref, wo, kept, grads, vec_ref):
        masks = pair_masks()
        lane = lax.broadcasted_iota(jnp.int32, (1, 2 * HEAD_DIM), 1) < HEAD_DIM
        vec_ref[...] = jnp.zeros_like(vec_ref)

        def step(i, carry):
            rows = rows_at(i)
            dctx = times_t(dm_ref[rows, :], wo[...]).astype(BF16)
            for block in range(ROW_TILE // BLOCK):
                chars = slice(block * BLOCK, (block + 1) * BLOCK)
                here = pl.ds(rows.start + block * BLOCK, BLOCK)
                for pair in range(half // (2 * HEAD_DIM)):
                    first = pair * 2 * HEAD_DIM
                    q, k, v = [kept[here, i * half + first : i * half + first + 2 * HEAD_DIM] for i in range(3)]
                    p = kept[here, 4 * half + pair * 2 * BLOCK : 4 * half + (pair + 1) * 2 * BLOCK]
                    grad = dctx[chars, first : first + 2 * HEAD_DIM]
                    dv2 = t_times(p, grad)
                    dv = jnp.where(lane, dv2[:BLOCK], dv2[BLOCK:])
                    dp = times_t(grad, stacked(v, masks))
                    p32 = p.astype(F32)
                    ds = []
                    for head in range(2):
                        part = slice(head * BLOCK, (head + 1) * BLOCK)
                        weighted = p32[:, part] * dp[:, part]
                        inner = jnp.sum(weighted, -1, keepdims=True)
                        ds.append((weighted - p32[:, part] * inner) * HEAD_DIM ** (-0.5))
                    ds = jnp.concatenate(ds, 1).astype(BF16)
                    dq = times(ds, stacked(k, masks))
                    dk2 = t_times(ds, q)
                    dk = jnp.where(lane, dk2[:BLOCK], dk2[BLOCK:])
                    for i, value in enumerate((dq, dk, dv)):
                        grads[here, i * half + first : i * half + first + 2 * HEAD_DIM] = value.astype(BF16)
                    lanes = slice(first, first + 2 * HEAD_DIM)
                    vec_ref[0:1, lanes] += column_sum(dq)
                    vec_ref[1:2, lanes] += column_sum(dv)
            return carry

        lax.fori_loop(0, span // ROW_TILE, step, 0)

    outs = [((span, 3 * half), BF16), ((8, half), F32)]
    return call(body, outs, (dm16, wo, kept), vmem_mb=4,
                flops=2 * span * width * half * 2, bytes_accessed=8e6, name=name, weight=LONG)


def input_backward(dm, x, wide, grads_own, grads_other, own_weights, other_weight):
    span, width = dm.shape
    half = width // 2

    def body(dm_ref, x_ref, wide, go, gt, wq, wk, wv, wt, out_ref, vec_ref):
        g = vector_row(wide, 0, width)
        vec_ref[...] = jnp.zeros_like(vec_ref)

        def step(i, carry):
            rows = rows_at(i)
            back = times_t(gt[rows, :], wt[...])
            for i, ref in enumerate((wq, wk, wv)):
                back += times_t(go[rows, i * half : (i + 1) * half], ref[...])
            hat, inv = norm_stats(x_ref[rows, :].astype(F32))
            out_ref[rows, :] = dm_ref[rows, :] + norm_back(back * g, hat, inv)
            vec_ref[0:1, :] += column_sum(back * hat)
            vec_ref[1:2, :] += column_sum(back)
            return carry

        lax.fori_loop(0, span // ROW_TILE, step, 0)

    outs = [((span, width), F32), ((8, width), F32)]
    return call(body, outs, (dm, x, wide, grads_own, grads_other, *own_weights, other_weight), vmem_mb=9,
                flops=2 * span * width * 3 * width, bytes_accessed=12e6, name="input_backward", weight=LONG)


def pack_vectors(conv_vec, ffn_vec, in_vec, own_vec, other_vec, own_up, *other_ups):
    half = own_vec.shape[1]
    ups = own_up.shape[1] // half
    rows = -(-(12 + 5 + ups) // 8) * 8

    def body(conv, ffn, inp, own, other, up, *refs):
        other_up, (mine, theirs) = refs[:-2], refs[-2:]
        shared = [
            ref[i : i + 1, j * half : (j + 1) * half]
            for ref, i in ((conv, 3), (ffn, 0), (ffn, 1), (ffn, 2), (inp, 0), (inp, 1))
            for j in range(2)
        ]
        for out, vec, side, some in ((mine, own, 0, (up,)), (theirs, other, 1, other_up)):
            group = [conv[i : i + 1, side * half : (side + 1) * half] for i in range(3)]
            group += [vec[i : i + 1, :] for i in range(2)]
            group += [ref[:, j * half : (j + 1) * half] for ref in some for j in range(ref.shape[1] // half)]
            pad = [jnp.zeros((rows - 12 - len(group), half), F32)] if rows > 12 + len(group) else []
            out[...] = jnp.concatenate(shared + group + pad, 0)

    ins = (conv_vec, ffn_vec, in_vec, own_vec, other_vec, own_up, *other_ups)
    return call(body, [((rows, half), F32)] * 2, ins, (), 4, 0, 2e5, "pack_vectors")


def flat_permute(value, route, dp_size):
    pairs = []
    for d in range(dp_size):
        for t in range(2):
            d2, t2 = route(d, t)
            pairs.append((d * 2 + t, d2 * 2 + t2))
    return lax.ppermute(value, ("dp", "tensor"), pairs)


def over_x(d, t):
    return d, 1 - t


def over_core(d, t):
    return d ^ 1, t


def over_y(d, t):
    return d ^ 2, t


def over_z(flip):
    return lambda d, t: (d ^ (flip << 2), t)


def by_core(first, second):
    return lambda d, t: (second if d & 1 else first)(d, t)


def after(value, *others):
    others = [other for other in others if other is not None]
    return lax.optimization_barrier((value, *others))[0] if others else value


class Order:
    def __init__(self):
        self.last = None

    def __call__(self, step, *args):
        if self.last is not None:
            args = lax.optimization_barrier((args, self.last))[0]
        self.last = step(*args)
        return self.last


def split_sum(keep, got):
    size = keep.shape[0] // 2
    total = [(keep[at : at + size].astype(F32) + got[at : at + size].astype(F32)).astype(BF16) for at in (0, size)]
    return tuple(total)


class Reduction:
    def __init__(self, grid, order, blocks):
        self.grid, self.order = grid, order
        self.keep = blocks[0]
        self.stage = 0
        if grid.fast:
            self.got = grid.send(blocks[1], over_core)
        else:
            self.got = grid.send(blocks[1], over_x)

    def step(self):
        if not self.grid.fast:
            return
        route = (by_core(over_x, over_y), by_core(over_y, over_x), over_z(1), over_z(2))[self.stage]
        self.keep, out = self.order(split_sum, self.keep, self.got)
        self.got = self.grid.send(out, route)
        self.stage += 1

    def finish(self):
        if not self.grid.fast:
            total = self.keep.astype(F32) + self.got.astype(F32)
            total = total.reshape(-1, total.shape[-1])
            return lax.psum_scatter(total, "dp", scatter_dimension=0, tiled=True)
        return self.order(lambda keep, got: (keep.astype(F32) + got.astype(F32))[0], self.keep, self.got)


class Grid:
    def __init__(self):
        self.dp = lax.axis_size("dp")
        self.index = lax.axis_index("dp")
        self.side = lax.axis_index("tensor")
        self.fast = self.dp == 16

    def send(self, value, route):
        return flat_permute(value, route, self.dp)

    def hops(self, first, *again):
        if not self.fast:
            return [first]
        second = self.send(first, by_core(over_y, over_z(1)))
        return [first, second, self.send(first, over_core), self.send(after(second, *again), over_core)]


class VectorSum:
    def __init__(self, grid, order, packed):
        self.grid, self.order = grid, order
        self.routes = [over_core, over_y, over_z(1), over_z(2)] if grid.fast else []
        self.total, out = packed
        self.got = grid.send(out, over_x)

    def step(self):
        self.total = self.order(lambda total, got: total + got, self.total, self.got)
        if self.routes:
            self.got = self.grid.send(self.total, self.routes.pop(0))

    def finish(self):
        self.step()
        if not self.grid.fast:
            self.total = lax.psum(self.total, "dp")
        return self.total


def per_device(
    characters, first_gain, first_shift, query_weight, query_bias, key_weight, value_weight, value_bias,
    out_weight, out_bias, second_gain, second_shift, up_weight, up_bias, down_weight, down_bias,
    conv_weight, conv_bias, third_gain, third_shift, cotangent,
):
    _, length, width = characters.shape
    span = length // 2
    half = width // 2
    units = up_weight.shape[1]
    mols = span // STRIDE
    grid = Grid()
    side = grid.side

    order = Order()
    matrices = (query_weight, key_weight, value_weight, out_weight, up_weight, down_weight, conv_weight)
    x, *pieces, tail, wide, narrow = pick_pieces(
        characters[0],
        matrices,
        (first_gain, first_shift, out_bias, second_gain, second_shift, down_bias),
        (query_bias, value_bias, conv_bias, third_gain, third_shift, up_bias),
    )
    if not grid.fast:
        pieces = [
            jnp.concatenate(
                [
                    ref[first : first + count, column : column + half].reshape(PARTS, count // PARTS, half)
                    for ref, first, count, column in group
                ],
                1,
            )
            for group in piece_groups(*matrices)
        ]

    a, kept_own = own_attention(x, wide, narrow, query_weight, key_weight, value_weight)
    firsts = [grid.send(piece, over_x) for piece in pieces]
    firsts[0] = after(firsts[0], a)
    attention_parts = grid.hops(firsts[0])
    tail = attention_parts[0] if grid.fast else grid.send(tail, over_x)
    wqkv_other, wo_other, kept_other, narrow_other = other_attention(a, attention_parts, tail, half)
    middle, c = attention_output(x, kept_own, kept_other, out_weight, wo_other, wide)
    hid_own, slope_own, acc = own_feed_forward(c, middle, wide, narrow, up_weight, down_weight)
    if grid.fast:
        pair, acc = lax.optimization_barrier((firsts[1], acc))
        firsts[1:2] = [pair[:1], pair[1:]]
    ups, downs, hids, slopes = [up_weight], [down_weight], [hid_own], [slope_own]
    firsts[3] = after(firsts[3], acc)
    parts, more = [grid.hops(first, firsts[3]) for first in firsts[1:3]]
    for i in range(2):
        start = narrow.shape[1] - units + i * units // 2
        up, down, hid, slope, acc = other_feed_forward(
            c, acc, narrow_other, units // 2, start, parts, f"other_feed_forward_{i}"
        )
        if i == 0:
            parts, conv_parts = more, grid.hops(firsts[3], acc)
        for some, value in zip((ups, downs, hids, slopes), (up, down, hid, slope)):
            some.append(value)

    hs, dconv16, mol_own, mol_other, dh2, dh2_16, conv_vec = order(
        lambda *args: downsample(*args[:2], args[4:], *args[2:4], cotangent[0]),
        acc, conv_weight, narrow, narrow_other, *conv_parts,
    )
    theirs = grid.send(mol_other, over_x)

    def whole(which, array):
        return (which, array, 0, array.shape[1])

    conv_sum = Reduction(grid, order, order(conv_weight_grad, hs, dconv16))
    down_sum = Reduction(
        grid,
        order,
        order(
            lambda left, own, *others: weight_grad(
                (left,), [[whole(0, own)], [whole(0, v) for v in others]], "down_weight_grad"
            ),
            dh2_16, *hids,
        ),
    )
    conv_sum.step()
    du_own, up_vec_own, acc = order(
        lambda dh16, slope, up, down: feed_forward_backward(dh16, [slope], [up], [down], "own_feed_forward_backward"),
        dh2_16, slopes[0], ups[0], downs[0],
    )
    down_sum.step()
    theirs = order(lambda value: value, theirs)
    du_first, du_second, *up_vecs, dm, dm16, ffn_vec = order(
        lambda dh16, acc, *args: feed_forward_backward(
            dh16, args[3:5], args[5:7], args[7:9], "other_feed_forward_backward", acc, args[:3]
        ),
        dh2_16, acc, dh2, middle, wide, *slopes[1:], *ups[1:], *downs[1:],
    )
    conv_sum.step()
    down_sum.step()
    up_sum = Reduction(
        grid,
        order,
        order(
            lambda c, dm16, own, first, second, kept_own, kept_other: weight_grad(
                (c, dm16),
                [
                    [whole(0, own), (1, kept_own, 3 * half, half)],
                    [whole(0, first), whole(0, second), (1, kept_other, 3 * half, half)],
                ],
                "up_weight_grad",
            ),
            c, dm16, du_own, du_first, du_second, kept_own, kept_other,
        ),
    )
    dqkv_own, vec_own = order(
        functools.partial(attention_backward, name="own_attention_backward"), dm16, out_weight, kept_own
    )
    up_sum.step()
    conv_sum.step()
    down_sum.step()
    dqkv_other, vec_other = order(
        functools.partial(attention_backward, name="other_attention_backward"), dm16, wo_other, kept_other
    )
    conv_sum.step()
    attention_sum = Reduction(
        grid,
        order,
        order(
            lambda a, own, other: weight_grad((a,), [[whole(0, own)], [whole(0, other)]], "attention_weight_grad"),
            a, dqkv_own, dqkv_other,
        ),
    )
    up_sum.step()
    down_sum.step()
    sum_conv_weight = conv_sum.finish()
    input_rows, in_vec = order(
        lambda *args: input_backward(*args[:5], args[5:8], args[8]),
        dm, x, wide, dqkv_own, dqkv_other, query_weight, key_weight, value_weight, wqkv_other,
    )
    attention_sum.step()
    vectors = VectorSum(
        grid, order, order(pack_vectors, conv_vec, ffn_vec, in_vec, vec_own, vec_other, up_vec_own, *up_vecs)
    )
    up_sum.step()
    vectors.step()
    sum_down = down_sum.finish()
    attention_sum.step()
    vectors.step()
    up_sum.step()
    attention_sum.step()
    vectors.step()
    attention_sum.step()
    vectors.step()
    sum_up = up_sum.finish()
    vectors.finish()
    shared, own = vectors.total[:12], vectors.total[12:]
    sum_attention = attention_sum.finish()

    mine, theirs = mol_own[: mols + 1], theirs[: mols + 1]
    upper = jnp.where(side == 0, mine, theirs)
    lower = jnp.where(side == 0, theirs, mine)
    molecules = jnp.concatenate([upper, lower[1:mols]], 0)[None]

    shared = shared.reshape(-1, width)
    block = width // grid.dp
    shared = lax.dynamic_slice_in_dim(shared, grid.index * block, block, 1)
    return (
        molecules,
        input_rows[None],
        shared[4],
        shared[5],
        sum_attention[:, :half],
        own[3],
        sum_attention[:, half : 2 * half],
        sum_attention[:, 2 * half : 3 * half],
        own[4],
        sum_up[:, units:].T,
        shared[3],
        shared[1],
        shared[2],
        sum_up[:, :units],
        own[5 : 5 + units // half].reshape(-1),
        sum_down.T,
        shared[0],
        sum_conv_weight,
        own[2],
        own[0],
        own[1],
    )


def solution(mesh):
    return jax.shard_map(
        per_device,
        mesh=mesh,
        in_specs=(
            P("dp", None, None),
            P(),
            P(),
            P(None, "tensor"),
            P("tensor"),
            P(None, "tensor"),
            P(None, "tensor"),
            P("tensor"),
            P("tensor", None),
            P(),
            P(),
            P(),
            P(None, "tensor"),
            P("tensor"),
            P("tensor", None),
            P(),
            P(None, "tensor"),
            P("tensor"),
            P("tensor"),
            P("tensor"),
            P("dp", None, None),
        ),
        out_specs=(
            P("dp", None, "tensor"),
            P("dp", "tensor", None),
            P("dp"),
            P("dp"),
            P("dp", "tensor"),
            P("tensor"),
            P("dp", "tensor"),
            P("dp", "tensor"),
            P("tensor"),
            P("tensor", "dp"),
            P("dp"),
            P("dp"),
            P("dp"),
            P("dp", "tensor"),
            P("tensor"),
            P("tensor", "dp"),
            P("dp"),
            P("dp", "tensor"),
            P("tensor"),
            P("tensor"),
            P("tensor"),
        ),
        check_vma=False,
    )
```

```python
import functools

import jax
import jax.numpy as jnp
from jax import lax
from jax.experimental import pallas as pl
from jax.experimental.pallas import tpu as pltpu
from jax.sharding import PartitionSpec as P

HEAD_DIM = 64
BLOCK = 128
STRIDE = 4
EPSILON = 1e-05
INV_ROOT_TWO = 0.7071067811865476
INV_ROOT_TWO_PI = 0.3989422804014327
F32 = jnp.float32
BF16 = jnp.bfloat16
PARTS = 4
ROW_TILE = 256
LONG = 8
SHORT = 0.1


def times(left, right):
    return jnp.dot(left, right, preferred_element_type=F32)


def times_t(left, right):
    return lax.dot_general(left, right, (((1,), (1,)), ((), ())), preferred_element_type=F32)


def t_times(left, right):
    return lax.dot_general(left, right, (((0,), (0,)), ((), ())), preferred_element_type=F32)


def gelu_parts(u):
    phi = 0.5 + 0.5 * lax.erf(u * INV_ROOT_TWO)
    return u * phi, phi + u * (jnp.exp(-0.5 * (u * u)) * INV_ROOT_TWO_PI)


def norm_stats(values):
    mean = jnp.mean(values, -1, keepdims=True)
    centered = values - mean
    inv = lax.rsqrt(jnp.mean(centered * centered, -1, keepdims=True) + EPSILON)
    return centered * inv, inv


def norm_back(scaled, hat, inv):
    return inv * (
        scaled
        - jnp.mean(scaled, -1, keepdims=True)
        - hat * jnp.mean(scaled * hat, -1, keepdims=True)
    )


def vector_row(ref, index, width):
    return ref[:, index * width : (index + 1) * width]


def column_sum(values):
    return jnp.sum(values, 0, keepdims=True)


def call(body, outs, ins, scratch=(), vmem_mb=32, flops=0, bytes_accessed=0, name=None, spaces=None, weight=1):
    spaces = spaces or {}
    in_specs = [pl.BlockSpec(memory_space=spaces.get(("in", i), pltpu.VMEM)) for i in range(len(ins))]
    out_specs = [pl.BlockSpec(memory_space=spaces.get(("out", i), pltpu.VMEM)) for i in range(len(outs))]
    return pl.pallas_call(
        body,
        out_shape=[jax.ShapeDtypeStruct(shape, dtype) for shape, dtype in outs],
        in_specs=in_specs,
        out_specs=out_specs,
        scratch_shapes=list(scratch),
        compiler_params=pltpu.CompilerParams(vmem_limit_bytes=vmem_mb << 20),
        cost_estimate=pl.CostEstimate(
            flops=int(flops * weight), bytes_accessed=int(bytes_accessed * weight), transcendentals=0
        ),
        name=name,
    )(*ins)


def rows_at(step, tile=ROW_TILE):
    return pl.ds(pl.multiple_of(step * tile, tile), tile)


def pair_masks():
    lane = lax.broadcasted_iota(jnp.int32, (1, 2 * HEAD_DIM), 1)
    low = (lane < HEAD_DIM).astype(F32).astype(BF16)
    high = (lane >= HEAD_DIM).astype(F32).astype(BF16)
    return low, high


def stacked(pair, masks):
    return jnp.concatenate([pair * masks[0], pair * masks[1]], 0)


TAIL = 16


def piece_groups(wq, wk, wv, wo, up, down, conv):
    width, half = wq.shape
    units = up.shape[1]
    groups = [[(ref, 0, width, 0) for ref in (wq, wk, wv)] + [(wo, 0, half, j * half) for j in range(2)]]
    for first in (0, units // 2):
        groups.append(
            [(up, 0, width, first + j * half) for j in range(units // 2 // half)]
            + [(down, first, units // 2, j * half) for j in range(2)]
        )
    groups.append([(conv, 0, conv.shape[0], 0)])
    return groups


class Place:
    def __init__(self):
        self.fast = lax.axis_size("dp") == 16
        index = lax.axis_index("dp")
        self.index, self.side = index, lax.axis_index("tensor")
        self.core, self.y, self.z = index & 1, (index >> 1) & 1, index >> 2
        self.low = jnp.where(self.core == 0, self.y, self.z & 1)
        self.piece = self.core * 2 + self.low

    def parts(self):
        if not self.fast:
            return list(range(PARTS))
        other_low = jnp.where(self.core == 0, self.z & 1, self.y)
        other = (1 - self.core) * 2 + other_low
        return [self.piece, self.piece ^ 1, other, other ^ 1]

    def position(self, block, core, half):
        if not self.fast:
            return block
        y_flip = ((block >> 1) & 1) ^ self.y
        z_flip = (block >> 2) ^ self.z
        high = half * 8 + y_flip * 4 if core % 2 == 0 else y_flip * 8 + half * 4
        return high + (z_flip & 1) * 2 + (z_flip >> 1)


def store_blocks(place, blocks, keep_ref, send_ref, columns):
    def store(swap):
        for block, core, half, values in blocks:
            away = (core % 2) ^ swap if place.fast else half
            (send_ref if away else keep_ref)[place.position(block, core, half), :, columns] = values

    if place.fast:
        for core in range(2):
            pl.when(place.core == core)(functools.partial(store, core))
    else:
        store(0)


def place_parts(part_refs, counts, targets, sems):
    table = Place().parts()
    copies = []
    slot = 0
    place = 0
    for ref, count in zip(part_refs, counts):
        for item in range(count):
            where = table[place]
            place += 1
            for start, rows, target, columns in targets:
                copies.append(
                    pltpu.make_async_copy(
                        ref.at[item, pl.ds(start, rows), :],
                        target.at[pl.ds(pl.multiple_of(where * rows, 16), rows), columns],
                        sems.at[slot],
                    )
                )
                slot += 1
    return copies


def pick_pieces(characters, matrices, wide_vectors, narrow_vectors):
    length, width = characters.shape
    span = length // 2
    half = matrices[0].shape[1]
    nm, vectors = len(matrices), (*wide_vectors, *narrow_vectors)
    nv, nw = len(vectors), len(wide_vectors)

    def body(*refs):
        chars, matrix_refs, vector_refs = refs[0], refs[1 : 1 + nm], refs[1 + nm : 1 + nm + nv]
        x_ref, pa, pair, pd, tail, wide, narrow = refs[1 + nm + nv : 8 + nm + nv]
        flat, sems = refs[8 + nm + nv : -1], refs[-1]
        targets = (pa.at[0], pair.at[0], pair.at[1], pd.at[0])
        wq, wk, wv, wo, up, down, conv = matrix_refs
        place = Place()
        copies = []

        def copy(source, target):
            made = pltpu.make_async_copy(source, target, sems.at[len(copies)])
            made.start()
            copies.append(made)

        for source, target in zip(vector_refs, flat):
            copy(source, target)
        for out, groups in zip(targets, piece_groups(wq, wk, wv, wo, up, down, conv)):
            start = 0
            for ref, first, count, column in groups:
                rows = count // PARTS
                source = ref.at[
                    pl.ds(pl.multiple_of(first + place.piece * rows, 16), rows), pl.ds(column, half)
                ]
                copy(source, out.at[pl.ds(start, rows), :])
                start += rows
        copy(chars.at[pl.ds(pl.multiple_of(place.side * span, 16), span), :], x_ref)
        for made in copies[:nv]:
            made.wait()
        for out, some in ((wide, flat[:nw]), (narrow, flat[nw:])):
            out[...] = jnp.concatenate([ref[...].astype(F32).reshape(1, -1) for ref in some], 1)
        count = narrow.shape[1] // half
        rows = [narrow[:, i * half : (i + 1) * half] for i in range(count)]
        rows = jnp.concatenate(rows + [jnp.zeros((TAIL - count, half), F32)], 0).astype(BF16)
        tail[0] = rows
        pa[0, pa.shape[1] - TAIL :, :] = rows
        for made in copies[nv:]:
            made.wait()

    sizes = [v.shape[0] for v in vectors]
    outs = [((span, width), BF16), ((1, width + TAIL, half), BF16)]
    outs += [((2, width, half), BF16), ((1, width, half), BF16)]
    outs += [((1, TAIL, half), BF16), ((1, sum(sizes[:nw])), F32), ((1, sum(sizes[nw:])), F32)]
    spaces = {("in", i): pltpu.HBM for i in range(1 + nm + nv)}
    scratch = [pltpu.VMEM((size,), BF16) for size in sizes] + [pltpu.SemaphoreType.DMA((40,))]
    return call(body, outs, (characters, *matrices, *vectors), scratch, 56, 0, 4e6, "pick_pieces", spaces)


def attention_forward(attn_in, wq, wk, wv, qb, vb, rows, kept, masks):
    queries = (times(attn_in, wq[...]) + qb).astype(BF16)
    keys = times(attn_in, wk[...]).astype(BF16)
    values = (times(attn_in, wv[...]) + vb).astype(BF16)
    half = queries.shape[1]
    kept[rows, 0:half] = queries
    kept[rows, half : 2 * half] = keys
    kept[rows, 2 * half : 3 * half] = values
    pairs = half // (2 * HEAD_DIM)
    for block in range(attn_in.shape[0] // BLOCK):
        chars = slice(block * BLOCK, (block + 1) * BLOCK)
        here = pl.ds(rows.start + block * BLOCK, BLOCK)
        for pair in range(pairs):
            lanes = slice(pair * 2 * HEAD_DIM, (pair + 1) * 2 * HEAD_DIM)
            scores = times_t(queries[chars, lanes], stacked(keys[chars, lanes], masks))
            scores = scores * HEAD_DIM ** (-0.5)
            probs = []
            for head in range(2):
                part = scores[:, head * BLOCK : (head + 1) * BLOCK]
                expo = jnp.exp(part - jnp.max(part, -1, keepdims=True))
                probs.append(expo * (1.0 / jnp.sum(expo, -1, keepdims=True)))
            both = jnp.concatenate(probs, 1).astype(BF16)
            kept[here, 4 * half + pair * 2 * BLOCK : 4 * half + (pair + 1) * 2 * BLOCK] = both
            kept[here, 3 * half + pair * 2 * HEAD_DIM : 3 * half + (pair + 1) * 2 * HEAD_DIM] = times(both, stacked(values[chars, lanes], masks)).astype(BF16)


def own_attention(x, wide, narrow, wq, wk, wv):
    span, width = x.shape
    half = wq.shape[1]

    def body(x_ref, wide, narrow, wq, wk, wv, a_ref, kept):
        masks = pair_masks()
        g, s = vector_row(wide, 0, width), vector_row(wide, 1, width)
        qb, vb = vector_row(narrow, 0, half), vector_row(narrow, 1, half)

        def step(i, carry):
            rows = rows_at(i)
            hat, _ = norm_stats(x_ref[rows, :].astype(F32))
            attn_in = (hat * g + s).astype(BF16)
            a_ref[rows, :] = attn_in
            attention_forward(attn_in, wq, wk, wv, qb, vb, rows, kept, masks)
            return carry

        lax.fori_loop(0, span // ROW_TILE, step, 0)

    outs = [((span, width), BF16), ((span, 4 * half + half // HEAD_DIM * BLOCK), BF16)]
    return call(body, outs, (x, wide, narrow, wq, wk, wv), vmem_mb=5,
                flops=2 * span * width * half * 3.5, bytes_accessed=8e6, name="own_attention")


def other_attention(a, parts, tail, half):
    span, width = a.shape
    counts = [part.shape[0] for part in parts]
    n = len(parts)
    last = tail.shape[1]

    def body(a_ref, tail_ref, *refs):
        part_refs = refs[:n]
        wqkv, wo, kept, narrow, sems = refs[n:]
        masks = pair_masks()
        rows_q = width // PARTS
        rows_o = half // PARTS
        targets = [(i * rows_q, rows_q, wqkv, pl.ds(i * half, half)) for i in range(3)]
        targets += [(3 * rows_q + i * rows_o, rows_o, wo, pl.ds(i * half, half)) for i in range(2)]
        copies = place_parts(part_refs, counts, targets, sems)
        for copy in copies:
            copy.start()
        rows = tail_ref[0, last - TAIL :, :].astype(F32)
        narrow[...] = jnp.concatenate([rows[i : i + 1, :] for i in range(narrow.shape[1] // half)], 1)
        qb, vb = vector_row(narrow, 0, half), vector_row(narrow, 1, half)
        for copy in copies:
            copy.wait()
        weights = [wqkv.at[:, pl.ds(i * half, half)] for i in range(3)]

        def step(i, carry):
            rows = rows_at(i)
            attention_forward(a_ref[rows, :], *weights, qb, vb, rows, kept, masks)
            return carry

        lax.fori_loop(0, span // ROW_TILE, step, 0)

    outs = [((width, 3 * half), BF16), ((half, width), BF16), ((span, 4 * half + half // HEAD_DIM * BLOCK), BF16)]
    outs += [((1, 9 * half), F32)]
    return call(body, outs, (a, tail, *parts), [pltpu.SemaphoreType.DMA((PARTS * 5,))], 5,
                2 * span * width * half * 3.5, 9e6, "other_attention")


def attention_output(x, kept_own, kept_other, wo_own, wo_other, wide):
    span, width = x.shape
    half = width // 2

    def body(x_ref, ko, kt, wo, wt, wide, h_ref, c_ref):
        b, g, s = [vector_row(wide, i, width) for i in (2, 3, 4)]
        ctx = slice(3 * half, 4 * half)

        def step(i, carry):
            rows = rows_at(i)
            middle = x_ref[rows, :].astype(F32) + b + times(ko[rows, ctx], wo[...]) + times(kt[rows, ctx], wt[...])
            h_ref[rows, :] = middle
            hat, _ = norm_stats(middle)
            c_ref[rows, :] = (hat * g + s).astype(BF16)
            return carry

        lax.fori_loop(0, span // ROW_TILE, step, 0)

    outs = [((span, width), F32), ((span, width), BF16)]
    return call(body, outs, (x, kept_own, kept_other, wo_own, wo_other, wide), vmem_mb=4,
                flops=2 * span * width * width, bytes_accessed=9e6, name="attention_output")


HIDDEN_TILE = 384


def feed_forward_half(c_ref, acc_ref, up, narrow, start, down, hid_ref, slope_ref, ub):
    span = c_ref.shape[0]
    units = up.shape[1]
    ub[...] = narrow[:, start : start + units]

    def step(j, carry):
        cols = rows_at(j, HIDDEN_TILE)
        for i in range(span // ROW_TILE):
            rows = slice(i * ROW_TILE, (i + 1) * ROW_TILE)
            upper = times(c_ref[rows, :], up[:, cols]) + ub[:, cols]
            hidden, slope = gelu_parts(upper)
            hidden = hidden.astype(BF16)
            hid_ref[rows, cols] = hidden
            slope_ref[rows, cols] = slope.astype(BF16)
            acc_ref[rows, :] += times(hidden, down[cols, :])
        return carry

    lax.fori_loop(0, units // HIDDEN_TILE, step, 0)


def own_feed_forward(c, middle, wide, narrow, up, down):
    span, width = c.shape
    units = up.shape[1]

    def body(c_ref, m_ref, wide, narrow, up, down, hid_ref, slope_ref, acc_ref, ub):
        acc_ref[...] = m_ref[...] + vector_row(wide, 5, width)
        feed_forward_half(c_ref, acc_ref, up, narrow, narrow.shape[1] - units, down, hid_ref, slope_ref, ub)

    outs = [((span, units), BF16)] * 2 + [((span, width), F32)]
    return call(body, outs, (c, middle, wide, narrow, up, down), [pltpu.VMEM((1, units), F32)], vmem_mb=4,
                flops=4 * span * width * units, bytes_accessed=16e6, name="own_feed_forward")


def other_feed_forward(c, acc, narrow, units, start, parts, name):
    span, width = c.shape
    half = width // 2
    counts = [part.shape[0] for part in parts]
    n = len(parts)

    def body(c_ref, a_ref, narrow, *refs):
        up, down, hid_ref, slope_ref, acc_ref, sems, ub = refs[n:]
        rows_u, rows_d = width // PARTS, units // PARTS
        targets = [(j * rows_u, rows_u, up, pl.ds(j * half, half)) for j in range(units // half)]
        first = len(targets) * rows_u
        targets += [(first + j * rows_d, rows_d, down, pl.ds(j * half, half)) for j in range(width // half)]
        copies = place_parts(refs[:n], counts, targets, sems)
        for copy in copies:
            copy.start()
        acc_ref[...] = a_ref[...]
        for copy in copies:
            copy.wait()
        feed_forward_half(c_ref, acc_ref, up, narrow, start, down, hid_ref, slope_ref, ub)

    outs = [((width, units), BF16), ((units, width), BF16)] + [((span, units), BF16)] * 2 + [((span, width), F32)]
    scratch = [pltpu.SemaphoreType.DMA((PARTS * 4,)), pltpu.VMEM((1, units), F32)]
    return call(body, outs, (c, acc, narrow, *parts), scratch, 4, 4 * span * width * units, 9e6, name)


def downsample(h2, wc_own, wc_parts, narrow, narrow_other, cot):
    span, width = h2.shape
    half = width // 2
    mols = span // STRIDE
    counts = [part.shape[0] for part in wc_parts]
    n = len(wc_parts)

    def body(h_ref, wo, narrow, narrow_other, cot_ref, *refs):
        part_refs = refs[:n]
        hs_ref, dc_ref, mol_own, mol_other, dh_ref, dh16_ref, vec_ref, wt, strip, pre, sems = refs[n:]
        left = lax.axis_index("tensor") == 0
        b, g, s = (
            jnp.concatenate([vector_row(ref, i, half) for ref in (narrow, narrow_other)], 1) for i in (2, 3, 4)
        )
        copies = place_parts(part_refs, counts, [(0, STRIDE * width // PARTS, wt, slice(None))], sems)
        for copy in copies:
            copy.start()
        pre[...] = jnp.zeros_like(pre)
        for lane in range(width // 128):
            strip[lane] = h_ref[:, lane * 128 : (lane + 1) * 128]

        def own_tap(tap, carry):
            window = jnp.concatenate(
                [strip[lane, pl.ds(tap, mols, stride=STRIDE), :] for lane in range(width // 128)], 1
            ).astype(BF16)
            hs_ref[rows_at(tap, mols), :] = window
            pre[:, :half] += times(window, wo[rows_at(tap, width), :])
            return carry

        lax.fori_loop(0, STRIDE, own_tap, 0)
        for copy in copies:
            copy.wait()

        def other_tap(tap, carry):
            pre[:, half:] += times(hs_ref[rows_at(tap, mols), :], wt[rows_at(tap, width), :])
            return carry

        lax.fori_loop(0, STRIDE, other_tap, 0)
        conv = pre[...] + b
        act, slope = gelu_parts(conv)
        hat, inv = norm_stats(act)
        whole = cot_ref[...].astype(F32)
        after = whole[mols + 1 :, :]
        after = jnp.concatenate([after, jnp.zeros((1, width), F32)], 0)
        after = jnp.concatenate([after[:, half:], after[:, :half]], 1)
        cotangent = jnp.where(left, whole[1 : mols + 1, :], after)
        dpre = norm_back(cotangent * g, hat, inv)
        dconv = dpre * slope
        dconv16 = dconv.astype(BF16)
        dc_ref[...] = dconv16
        hat0, inv0 = norm_stats(h_ref[0:8, :])
        only = (lax.broadcasted_iota(jnp.int32, (8, width), 0) == 0) & left
        cot0 = jnp.where(only, whole[0:8, :], 0.0)
        dpre0 = norm_back(cot0 * g, hat0, inv0)
        mol = jnp.concatenate([(hat0 * g + s)[0:1], hat * g + s, jnp.zeros((15, width), F32)], 0).astype(BF16)
        mol_own[...] = mol[:, :half]
        mol_other[...] = mol[:, half:]
        vec_ref[...] = jnp.zeros_like(vec_ref)
        vec_ref[0:1, :] = column_sum(cotangent * hat) + column_sum(cot0 * hat0)
        vec_ref[1:2, :] = column_sum(cotangent) + column_sum(cot0)
        vec_ref[2:3, :] = column_sum(dconv)
        def back_tap(tap, carry):
            taps = rows_at(tap, width)
            back = times_t(dconv16[:, :half], wo[taps, :]) + times_t(dconv16[:, half:], wt[taps, :])
            for lane in range(width // 128):
                strip[lane, pl.ds(tap, mols, stride=STRIDE), :] = back[:, lane * 128 : (lane + 1) * 128]
            return carry

        lax.fori_loop(0, STRIDE, back_tap, 0)
        for lane in range(width // 128):
            dh_ref[:, lane * 128 : (lane + 1) * 128] = strip[lane]
        dh_ref[0:8, :] += dpre0
        total = jnp.zeros((1, width), F32)
        for i in range(span // ROW_TILE):
            rows = slice(i * ROW_TILE, (i + 1) * ROW_TILE)
            grad = dh_ref[rows, :]
            dh16_ref[rows, :] = grad.astype(BF16)
            total += column_sum(grad)
        vec_ref[3:4, :] = total

    outs = [((span, width), BF16), ((mols, width), BF16), ((mols + 16, half), BF16), ((mols + 16, half), BF16),
            ((span, width), F32), ((span, width), BF16), ((8, width), F32)]
    spaces = None
    scratch = [pltpu.VMEM((STRIDE * width, half), BF16), pltpu.VMEM((width // 128, span, 128), F32)]
    scratch += [pltpu.VMEM((mols, width), F32), pltpu.SemaphoreType.DMA((PARTS,))]
    return call(body, outs, (h2, wc_own, narrow, narrow_other, cot, *wc_parts), scratch, 10,
                8 * span * width * width / 2, 16e6, "downsample", spaces)


def conv_weight_grad(hs, dconv16):
    span, width = hs.shape
    half = width // 2
    mols = span // STRIDE
    rows = STRIDE * width // 16

    def body(hs_ref, dc_ref, keep_ref, send_ref):
        place = Place()
        dc = dc_ref[...]

        def step(tap, carry):
            grad = t_times(hs_ref[pl.ds(pl.multiple_of(tap * mols, 16), mols), :], dc).astype(BF16)
            blocks = [
                (tap * 4 + i, i, group, grad[i * rows : (i + 1) * rows, group * half : (group + 1) * half])
                for i in range(4)
                for group in range(2)
            ]
            store_blocks(place, blocks, keep_ref, send_ref, slice(None))
            return carry

        lax.fori_loop(0, STRIDE, step, 0)

    outs = [((16, rows, half), BF16)] * 2
    return call(body, outs, (hs, dconv16), (), 8, 2 * span * width * width, 7e6, "conv_weight_grad", weight=LONG)


GRAD_TILE = 384


def weight_grad(lefts, rights, name):
    span, width = lefts[0].shape
    units = sum(item[3] for item in rights[0])
    rows = width // 16
    flat = [item[1] for group in rights for item in group]
    nl, nr = len(lefts), len(flat)

    def body(*refs):
        left_refs, right_refs = refs[:nl], refs[nl : nl + nr]
        keep_ref, send_ref, turned = refs[nl + nr :]
        place = Place()
        for i, ref in enumerate(left_refs):
            def turn(t, carry, i=i, ref=ref):
                turned[i, :, rows_at(t)] = ref[rows_at(t), :].T
                return carry

            lax.fori_loop(0, span // ROW_TILE, turn, 0)
        at = 0
        for group_index, group in enumerate(rights):
            column = 0
            for which, _, first, count in group:
                ref = right_refs[at]
                at += 1
                tile = min(HIDDEN_TILE, count)

                splits = width // GRAD_TILE

                def step(n, carry, ref=ref, which=which, group_index=group_index, column=column, first=first):
                    j, i = lax.div(n, splits), lax.rem(n, splits)
                    cols = pl.ds(pl.multiple_of(first + j * tile, 128), tile)
                    target = pl.ds(pl.multiple_of(column + j * tile, 128), tile)
                    left = turned[which, pl.ds(pl.multiple_of(i * GRAD_TILE, 128), GRAD_TILE), :]
                    grad = times(left, ref[:, cols]).astype(BF16)
                    per = GRAD_TILE // rows
                    blocks = [(i * per + k, k, group_index, grad[k * rows : (k + 1) * rows]) for k in range(per)]
                    store_blocks(place, blocks, keep_ref, send_ref, target)
                    return carry

                lax.fori_loop(0, count // tile * splits, step, 0)
                column += count

    outs = [((16, rows, units), BF16)] * 2
    return call(body, outs, (*lefts, *flat), [pltpu.VMEM((nl, width, span), BF16)], 8,
                4 * span * width * units, 12e6, name, weight=LONG)


def feed_forward_backward(dh2_16, slopes, ups, downs, name, acc=None, close=None):
    span, width = dh2_16.shape
    n = len(ups)
    sizes = [up.shape[1] for up in ups]
    more = (() if acc is None else (acc,)) + (() if close is None else close)

    def body(dh16_ref, *refs):
        slope_refs, up_refs, down_refs, refs = refs[:n], refs[n : 2 * n], refs[2 * n : 3 * n], refs[3 * n :]
        more_refs, du_refs, refs = refs[: len(more)], refs[len(more) : len(more) + n], refs[len(more) + n :]
        ub_refs, refs = refs[:n], refs[n:]
        acc_ref = refs[-1]
        if acc is None:
            acc_ref[...] = jnp.zeros_like(acc_ref)
        else:
            acc_ref[...] = more_refs[0][...]
        for slope_ref, up, down, du_ref, ub_ref in zip(slope_refs, up_refs, down_refs, du_refs, ub_refs):
            def step(j, carry, slope_ref=slope_ref, up=up, down=down, du_ref=du_ref, ub_ref=ub_ref):
                cols = rows_at(j, HIDDEN_TILE)
                total = jnp.zeros((1, HIDDEN_TILE), F32)
                for i in range(span // ROW_TILE):
                    rows = slice(i * ROW_TILE, (i + 1) * ROW_TILE)
                    grad = times_t(dh16_ref[rows, :], down[cols, :]) * slope_ref[rows, cols].astype(F32)
                    total += column_sum(grad)
                    grad16 = grad.astype(BF16)
                    du_ref[rows, cols] = grad16
                    acc_ref[rows, :] += times_t(grad16, up[:, cols])
                ub_ref[:, cols] = total
                return carry

            lax.fori_loop(0, up.shape[1] // HIDDEN_TILE, step, 0)
        if close is None:
            return
        dh_ref, m_ref, wide = more_refs[-3:]
        dm_ref, dm16_ref, vec_ref = refs[:3]
        g = vector_row(wide, 3, width)
        vec_ref[...] = jnp.zeros_like(vec_ref)

        def finish(i, carry):
            rows = rows_at(i)
            back = acc_ref[rows, :]
            hat, inv = norm_stats(m_ref[rows, :])
            grad = dh_ref[rows, :] + norm_back(back * g, hat, inv)
            dm_ref[rows, :] = grad
            dm16_ref[rows, :] = grad.astype(BF16)
            vec_ref[0:1, :] += column_sum(back * hat)
            vec_ref[1:2, :] += column_sum(back)
            vec_ref[2:3, :] += column_sum(grad)
            return carry

        lax.fori_loop(0, span // ROW_TILE, finish, 0)

    outs = [((span, size), BF16) for size in sizes] + [((1, size), F32) for size in sizes]
    if close is None:
        outs += [((span, width), F32)]
        scratch = []
    else:
        outs += [((span, width), F32), ((span, width), BF16), ((8, width), F32)]
        scratch = [pltpu.VMEM((span, width), F32)]
    return call(body, outs, (dh2_16, *slopes, *ups, *downs, *more), scratch, 12,
                8 * span * width * sum(sizes) / 2, 16e6, name, weight=LONG)


def attention_backward(dm16, wo, kept, name):
    span, width = dm16.shape
    half = width // 2

    def body(dm_ref, wo, kept, grads, vec_ref):
        masks = pair_masks()
        lane = lax.broadcasted_iota(jnp.int32, (1, 2 * HEAD_DIM), 1) < HEAD_DIM
        vec_ref[...] = jnp.zeros_like(vec_ref)

        def step(i, carry):
            rows = rows_at(i)
            dctx = times_t(dm_ref[rows, :], wo[...]).astype(BF16)
            for block in range(ROW_TILE // BLOCK):
                chars = slice(block * BLOCK, (block + 1) * BLOCK)
                here = pl.ds(rows.start + block * BLOCK, BLOCK)
                for pair in range(half // (2 * HEAD_DIM)):
                    first = pair * 2 * HEAD_DIM
                    q, k, v = [kept[here, i * half + first : i * half + first + 2 * HEAD_DIM] for i in range(3)]
                    p = kept[here, 4 * half + pair * 2 * BLOCK : 4 * half + (pair + 1) * 2 * BLOCK]
                    grad = dctx[chars, first : first + 2 * HEAD_DIM]
                    dv2 = t_times(p, grad)
                    dv = jnp.where(lane, dv2[:BLOCK], dv2[BLOCK:])
                    dp = times_t(grad, stacked(v, masks))
                    p32 = p.astype(F32)
                    ds = []
                    for head in range(2):
                        part = slice(head * BLOCK, (head + 1) * BLOCK)
                        weighted = p32[:, part] * dp[:, part]
                        inner = jnp.sum(weighted, -1, keepdims=True)
                        ds.append((weighted - p32[:, part] * inner) * HEAD_DIM ** (-0.5))
                    ds = jnp.concatenate(ds, 1).astype(BF16)
                    dq = times(ds, stacked(k, masks))
                    dk2 = t_times(ds, q)
                    dk = jnp.where(lane, dk2[:BLOCK], dk2[BLOCK:])
                    for i, value in enumerate((dq, dk, dv)):
                        grads[here, i * half + first : i * half + first + 2 * HEAD_DIM] = value.astype(BF16)
                    lanes = slice(first, first + 2 * HEAD_DIM)
                    vec_ref[0:1, lanes] += column_sum(dq)
                    vec_ref[1:2, lanes] += column_sum(dv)
            return carry

        lax.fori_loop(0, span // ROW_TILE, step, 0)

    outs = [((span, 3 * half), BF16), ((8, half), F32)]
    return call(body, outs, (dm16, wo, kept), vmem_mb=4,
                flops=2 * span * width * half * 2, bytes_accessed=8e6, name=name, weight=LONG)


def input_backward(dm, x, wide, grads_own, grads_other, own_weights, other_weight):
    span, width = dm.shape
    half = width // 2

    def body(dm_ref, x_ref, wide, go, gt, wq, wk, wv, wt, out_ref, vec_ref):
        g = vector_row(wide, 0, width)
        vec_ref[...] = jnp.zeros_like(vec_ref)

        def step(i, carry):
            rows = rows_at(i)
            back = times_t(gt[rows, :], wt[...])
            for i, ref in enumerate((wq, wk, wv)):
                back += times_t(go[rows, i * half : (i + 1) * half], ref[...])
            hat, inv = norm_stats(x_ref[rows, :].astype(F32))
            out_ref[rows, :] = dm_ref[rows, :] + norm_back(back * g, hat, inv)
            vec_ref[0:1, :] += column_sum(back * hat)
            vec_ref[1:2, :] += column_sum(back)
            return carry

        lax.fori_loop(0, span // ROW_TILE, step, 0)

    outs = [((span, width), F32), ((8, width), F32)]
    return call(body, outs, (dm, x, wide, grads_own, grads_other, *own_weights, other_weight), vmem_mb=9,
                flops=2 * span * width * 3 * width, bytes_accessed=12e6, name="input_backward", weight=LONG)


def pack_vectors(conv_vec, ffn_vec, in_vec, own_vec, other_vec, own_up, *other_ups):
    half = own_vec.shape[1]
    ups = own_up.shape[1] // half
    rows = -(-(12 + 5 + ups) // 8) * 8

    def body(conv, ffn, inp, own, other, up, *refs):
        other_up, (mine, theirs) = refs[:-2], refs[-2:]
        shared = [
            ref[i : i + 1, j * half : (j + 1) * half]
            for ref, i in ((conv, 3), (ffn, 0), (ffn, 1), (ffn, 2), (inp, 0), (inp, 1))
            for j in range(2)
        ]
        for out, vec, side, some in ((mine, own, 0, (up,)), (theirs, other, 1, other_up)):
            group = [conv[i : i + 1, side * half : (side + 1) * half] for i in range(3)]
            group += [vec[i : i + 1, :] for i in range(2)]
            group += [ref[:, j * half : (j + 1) * half] for ref in some for j in range(ref.shape[1] // half)]
            pad = [jnp.zeros((rows - 12 - len(group), half), F32)] if rows > 12 + len(group) else []
            out[...] = jnp.concatenate(shared + group + pad, 0)

    ins = (conv_vec, ffn_vec, in_vec, own_vec, other_vec, own_up, *other_ups)
    return call(body, [((rows, half), F32)] * 2, ins, (), 4, 0, 2e5, "pack_vectors")


def flat_permute(value, route, dp_size):
    pairs = []
    for d in range(dp_size):
        for t in range(2):
            d2, t2 = route(d, t)
            pairs.append((d * 2 + t, d2 * 2 + t2))
    return lax.ppermute(value, ("dp", "tensor"), pairs)


def over_x(d, t):
    return d, 1 - t


def over_core(d, t):
    return d ^ 1, t


def over_y(d, t):
    return d ^ 2, t


def over_z(flip):
    return lambda d, t: (d ^ (flip << 2), t)


def by_core(first, second):
    return lambda d, t: (second if d & 1 else first)(d, t)


def after(value, *others):
    others = [other for other in others if other is not None]
    return lax.optimization_barrier((value, *others))[0] if others else value


class Order:
    def __init__(self):
        self.last = None

    def __call__(self, step, *args):
        if self.last is not None:
            args = lax.optimization_barrier((args, self.last))[0]
        self.last = step(*args)
        return self.last


def split_sum(keep, got):
    size = keep.shape[0] // 2
    total = [(keep[at : at + size].astype(F32) + got[at : at + size].astype(F32)).astype(BF16) for at in (0, size)]
    return tuple(total)


class Reduction:
    def __init__(self, grid, order, blocks):
        self.grid, self.order = grid, order
        self.keep = blocks[0]
        self.stage = 0
        if grid.fast:
            self.got = grid.send(blocks[1], over_core)
        else:
            self.got = grid.send(blocks[1], over_x)

    def step(self):
        if not self.grid.fast:
            return
        route = (by_core(over_x, over_y), by_core(over_y, over_x), over_z(1), over_z(2))[self.stage]
        self.keep, out = self.order(split_sum, self.keep, self.got)
        self.got = self.grid.send(out, route)
        self.stage += 1

    def finish(self):
        if not self.grid.fast:
            total = self.keep.astype(F32) + self.got.astype(F32)
            total = total.reshape(-1, total.shape[-1])
            return lax.psum_scatter(total, "dp", scatter_dimension=0, tiled=True)
        return self.order(lambda keep, got: (keep.astype(F32) + got.astype(F32))[0], self.keep, self.got)


class Grid:
    def __init__(self):
        self.dp = lax.axis_size("dp")
        self.index = lax.axis_index("dp")
        self.side = lax.axis_index("tensor")
        self.fast = self.dp == 16

    def send(self, value, route):
        return flat_permute(value, route, self.dp)

    def hops(self, first, *again):
        if not self.fast:
            return [first]
        second = self.send(first, by_core(over_y, over_z(1)))
        return [first, second, self.send(first, over_core), self.send(after(second, *again), over_core)]


class VectorSum:
    def __init__(self, grid, order, packed):
        self.grid, self.order = grid, order
        self.routes = [over_core, over_y, over_z(1), over_z(2)] if grid.fast else []
        self.total, out = packed
        self.got = grid.send(out, over_x)

    def step(self):
        self.total = self.order(lambda total, got: total + got, self.total, self.got)
        if self.routes:
            self.got = self.grid.send(self.total, self.routes.pop(0))

    def finish(self):
        self.step()
        if not self.grid.fast:
            self.total = lax.psum(self.total, "dp")
        return self.total


def per_device(
    characters, first_gain, first_shift, query_weight, query_bias, key_weight, value_weight, value_bias,
    out_weight, out_bias, second_gain, second_shift, up_weight, up_bias, down_weight, down_bias,
    conv_weight, conv_bias, third_gain, third_shift, cotangent,
):
    _, length, width = characters.shape
    span = length // 2
    half = width // 2
    units = up_weight.shape[1]
    mols = span // STRIDE
    grid = Grid()
    side = grid.side

    order = Order()
    matrices = (query_weight, key_weight, value_weight, out_weight, up_weight, down_weight, conv_weight)
    x, *pieces, tail, wide, narrow = pick_pieces(
        characters[0],
        matrices,
        (first_gain, first_shift, out_bias, second_gain, second_shift, down_bias),
        (query_bias, value_bias, conv_bias, third_gain, third_shift, up_bias),
    )
    if not grid.fast:
        pieces = [
            jnp.concatenate(
                [
                    ref[first : first + count, column : column + half].reshape(PARTS, count // PARTS, half)
                    for ref, first, count, column in group
                ],
                1,
            )
            for group in piece_groups(*matrices)
        ]

    a, kept_own = own_attention(x, wide, narrow, query_weight, key_weight, value_weight)
    firsts = [grid.send(piece, over_x) for piece in pieces]
    firsts[0] = after(firsts[0], a)
    attention_parts = grid.hops(firsts[0])
    tail = attention_parts[0] if grid.fast else grid.send(tail, over_x)
    wqkv_other, wo_other, kept_other, narrow_other = other_attention(a, attention_parts, tail, half)
    middle, c = attention_output(x, kept_own, kept_other, out_weight, wo_other, wide)
    hid_own, slope_own, acc = own_feed_forward(c, middle, wide, narrow, up_weight, down_weight)
    if grid.fast:
        pair, acc = lax.optimization_barrier((firsts[1], acc))
        firsts[1:2] = [pair[:1], pair[1:]]
    ups, downs, hids, slopes = [up_weight], [down_weight], [hid_own], [slope_own]
    firsts[3] = after(firsts[3], acc)
    parts, more = [grid.hops(first, firsts[3]) for first in firsts[1:3]]
    for i in range(2):
        start = narrow.shape[1] - units + i * units // 2
        up, down, hid, slope, acc = other_feed_forward(
            c, acc, narrow_other, units // 2, start, parts, f"other_feed_forward_{i}"
        )
        if i == 0:
            parts, conv_parts = more, grid.hops(firsts[3], acc)
        for some, value in zip((ups, downs, hids, slopes), (up, down, hid, slope)):
            some.append(value)

    hs, dconv16, mol_own, mol_other, dh2, dh2_16, conv_vec = order(
        lambda *args: downsample(*args[:2], args[4:], *args[2:4], cotangent[0]),
        acc, conv_weight, narrow, narrow_other, *conv_parts,
    )
    theirs = grid.send(mol_other, over_x)

    def whole(which, array):
        return (which, array, 0, array.shape[1])

    conv_sum = Reduction(grid, order, order(conv_weight_grad, hs, dconv16))
    down_sum = Reduction(
        grid,
        order,
        order(
            lambda left, own, *others: weight_grad(
                (left,), [[whole(0, own)], [whole(0, v) for v in others]], "down_weight_grad"
            ),
            dh2_16, *hids,
        ),
    )
    conv_sum.step()
    du_own, up_vec_own, acc = order(
        lambda dh16, slope, up, down: feed_forward_backward(dh16, [slope], [up], [down], "own_feed_forward_backward"),
        dh2_16, slopes[0], ups[0], downs[0],
    )
    down_sum.step()
    theirs = order(lambda value: value, theirs)
    du_first, du_second, *up_vecs, dm, dm16, ffn_vec = order(
        lambda dh16, acc, *args: feed_forward_backward(
            dh16, args[3:5], args[5:7], args[7:9], "other_feed_forward_backward", acc, args[:3]
        ),
        dh2_16, acc, dh2, middle, wide, *slopes[1:], *ups[1:], *downs[1:],
    )
    conv_sum.step()
    down_sum.step()
    up_sum = Reduction(
        grid,
        order,
        order(
            lambda c, dm16, own, first, second, kept_own, kept_other: weight_grad(
                (c, dm16),
                [
                    [whole(0, own), (1, kept_own, 3 * half, half)],
                    [whole(0, first), whole(0, second), (1, kept_other, 3 * half, half)],
                ],
                "up_weight_grad",
            ),
            c, dm16, du_own, du_first, du_second, kept_own, kept_other,
        ),
    )
    dqkv_own, vec_own = order(
        functools.partial(attention_backward, name="own_attention_backward"), dm16, out_weight, kept_own
    )
    up_sum.step()
    conv_sum.step()
    down_sum.step()
    dqkv_other, vec_other = order(
        functools.partial(attention_backward, name="other_attention_backward"), dm16, wo_other, kept_other
    )
    conv_sum.step()
    attention_sum = Reduction(
        grid,
        order,
        order(
            lambda a, own, other: weight_grad((a,), [[whole(0, own)], [whole(0, other)]], "attention_weight_grad"),
            a, dqkv_own, dqkv_other,
        ),
    )
    up_sum.step()
    down_sum.step()
    sum_conv_weight = conv_sum.finish()
    input_rows, in_vec = order(
        lambda *args: input_backward(*args[:5], args[5:8], args[8]),
        dm, x, wide, dqkv_own, dqkv_other, query_weight, key_weight, value_weight, wqkv_other,
    )
    attention_sum.step()
    vectors = VectorSum(
        grid, order, order(pack_vectors, conv_vec, ffn_vec, in_vec, vec_own, vec_other, up_vec_own, *up_vecs)
    )
    up_sum.step()
    vectors.step()
    sum_down = down_sum.finish()
    attention_sum.step()
    vectors.step()
    up_sum.step()
    attention_sum.step()
    vectors.step()
    attention_sum.step()
    vectors.step()
    sum_up = up_sum.finish()
    vectors.finish()
    shared, own = vectors.total[:12], vectors.total[12:]
    sum_attention = attention_sum.finish()

    mine, theirs = mol_own[: mols + 1], theirs[: mols + 1]
    upper = jnp.where(side == 0, mine, theirs)
    lower = jnp.where(side == 0, theirs, mine)
    molecules = jnp.concatenate([upper, lower[1:mols]], 0)[None]

    shared = shared.reshape(-1, width)
    block = width // grid.dp
    shared = lax.dynamic_slice_in_dim(shared, grid.index * block, block, 1)
    return (
        molecules,
        input_rows[None],
        shared[4],
        shared[5],
        sum_attention[:, :half],
        own[3],
        sum_attention[:, half : 2 * half],
        sum_attention[:, 2 * half : 3 * half],
        own[4],
        sum_up[:, units:].T,
        shared[3],
        shared[1],
        shared[2],
        sum_up[:, :units],
        own[5 : 5 + units // half].reshape(-1),
        sum_down.T,
        shared[0],
        sum_conv_weight,
        own[2],
        own[0],
        own[1],
    )


def solution(mesh):
    return jax.shard_map(
        per_device,
        mesh=mesh,
        in_specs=(
            P("dp", None, None),
            P(),
            P(),
            P(None, "tensor"),
            P("tensor"),
            P(None, "tensor"),
            P(None, "tensor"),
            P("tensor"),
            P("tensor", None),
            P(),
            P(),
            P(),
            P(None, "tensor"),
            P("tensor"),
            P("tensor", None),
            P(),
            P(None, "tensor"),
            P("tensor"),
            P("tensor"),
            P("tensor"),
            P("dp", None, None),
        ),
        out_specs=(
            P("dp", None, "tensor"),
            P("dp", "tensor", None),
            P("dp"),
            P("dp"),
            P("dp", "tensor"),
            P("tensor"),
            P("dp", "tensor"),
            P("dp", "tensor"),
            P("tensor"),
            P("tensor", "dp"),
            P("dp"),
            P("dp"),
            P("dp"),
            P("dp", "tensor"),
            P("tensor"),
            P("tensor", "dp"),
            P("dp"),
            P("dp", "tensor"),
            P("tensor"),
            P("tensor"),
            P("tensor"),
        ),
        check_vma=False,
    )
```
